32 devices in a mesh: ens: 2 (over y), gx: 4 (over x, core), gy: 4 (over z).
Axes of the slice: x: 2, y: 2, z: 4, core: 2. Of those that a mesh axis runs over, the one named last changes fastest.
Arguments:
- log_conductivity: float32 [64, 64, 256], P(('ens', 'gx'), 'gy'), parts along dimension 0, may hold values from -3 to 3
- state: float32 [64, 64, 256], P(('ens', 'gx'), 'gy'), parts along dimension 0, may hold values from -6 to 6
- gradient: float32 [64, 64, 256], P(('ens', 'gx'), 'gy'), parts along dimension 0, may hold values from -60 to 60
- prior_sample: float32 [64, 64, 256], P(('ens', 'gx'), 'gy'), parts along dimension 0, may hold values from -6 to 6
- sensor_cells: int32 [16384], P(('ens', 'gx', 'gy')), parts along dimension 0, may hold values from 0 to 524287, as said below
- noise_precision: float32 [16384], P(('ens', 'gx', 'gy')), parts along dimension 0, may hold values from 20 to 200
Outputs:
- step_field: float32 [64, 64, 256], P(('ens', 'gx'), 'gy'), parts along dimension 0
- residual: float32 [64, 64, 256], P(('ens', 'gx'), 'gy'), parts along dimension 0
The draws below stay inside these ranges and needn't reach their ends.
There are 2 independent parts, one for each index of `ens`. The reference program is written for one: setup_inputs(seed, part) draws one part's arguments, and reference() takes and returns one part's arrays. A program takes and returns all parts, laid end to end along the dimension named above; each array names one. Nothing has to cross between parts.
Inputs may be any that keep to these rules, and one draw needn't show every extreme that they name: `sensor_cells`: sensors t * 512 to (t + 1) * 512 - 1 observe cells inside the block of cells held by the t-th device in the order gx, then gy (blocks of 8 x 16 x 256 cells); a cell may be observed by several sensors.
All inputs are finite; a program needn't handle non-finite values.
Results may differ from the reference program's by a relative error of at most 0.00015.
Values sent between devices are 32-bit elements; how exact they have to be, the bound alone decides.
No kernel may reach another device: no remote copies, remote signals or barrier semaphores. Data moves between devices by JAX's collectives and lax.ppermute only.
A program may use at most 128 MiB of HBM per device.

```python
import math
import jax
import jax.numpy as jnp

CX = 8
CY = 16
CZ = 256
SENS_DEV = 512
LEVELS = 3
SWEEPS = 1
COARSE_SWEEPS = 6
VCYCLES = 1
CG_ITERS = 2
NX = 32
NY = 64
NZ = 256
SENSORS = 8192


def draw_gradient(key, part):
    first_key, second_key = jax.random.split(jax.random.fold_in(key, 17))
    extent = (NX, NY, NZ)
    along_x = jnp.arange(NX, dtype=jnp.float32)[:, None, None] / (NX - 1)
    along_y = jnp.arange(NY, dtype=jnp.float32)[None, :, None] / (NY - 1)
    exponent = 0.5 * (along_x + along_y)
    random_part = jnp.clip(jax.random.normal(first_key, extent, jnp.float32), -4.0, 4.0)
    roughness = jnp.exp(jax.random.uniform(second_key, extent, jnp.float32, -0.35, 0.35))
    return random_part * roughness * jnp.power(10.0, exponent)


def draw_sensor_cells(key, part):
    keys = jax.random.split(jax.random.fold_in(key, 29), 3)
    slot_block = jnp.arange(SENSORS, dtype=jnp.int32) // SENS_DEV
    blocks_y = NY // CY
    row_index = slot_block // blocks_y * CX + jax.random.randint(keys[0], (SENSORS,), 0, CX, dtype=jnp.int32)
    column_index = slot_block % blocks_y * CY + jax.random.randint(keys[1], (SENSORS,), 0, CY, dtype=jnp.int32)
    depth_index = jax.random.randint(keys[2], (SENSORS,), 0, CZ, dtype=jnp.int32)
    return (row_index * NY + column_index) * NZ + depth_index


def shard_levels(rng, dims, shards, smallest, top_value):
    loudness, own = 1.0, jax.random.fold_in(rng, 6)
    for dim, blocks in shards:
        draws = jnp.exp(jax.random.uniform(jax.random.fold_in(own, dim), (blocks,), jnp.float32, smallest / len(shards), top_value / len(shards)))
        loudness = loudness * jnp.repeat(draws, dims[dim] // blocks).reshape([-1 if axis == dim else 1 for axis in range(len(dims))])
    return loudness


def scatter_about(rng, dims, scale, bound, pieces=(), held_as=jnp.bfloat16):
    values = scale * jax.random.normal(rng, dims, jnp.float32)
    if pieces:
        values = values * shard_levels(rng, dims, pieces, -0.22, 0.18)
    return jnp.clip(values, -bound, bound).astype(held_as)


def setup_inputs(seed: int = 0, part: int = 0) -> dict:
    splits = jax.random.split(jax.random.key(seed), 7)
    own_keys = jax.random.split(jax.random.fold_in(splits[6], part), 7)
    return {
        "log_conductivity": scatter_about(own_keys[0], (NX, NY, NZ), 0.7, 3.0, ((0, 4), (1, 4)), jnp.float32),
        "state": scatter_about(own_keys[1], (NX, NY, NZ), 1.0, 6.0, ((0, 4), (1, 4)), jnp.float32),
        "gradient": draw_gradient(jax.random.fold_in(jax.random.fold_in(splits[6], part), 71), part),
        "prior_sample": scatter_about(own_keys[3], (NX, NY, NZ), 1.0, 6.0, ((0, 4), (1, 4)), jnp.float32),
        "sensor_cells": draw_sensor_cells(jax.random.fold_in(jax.random.fold_in(splits[6], part), 71), part),
        "noise_precision": jnp.clip(jnp.exp(math.log(200.0) - 2.3025851 * jax.random.uniform(own_keys[5], (SENSORS,), jnp.float32) ** shard_levels(own_keys[5], (SENSORS,), ((0, 16),), -0.2, 0.2)), 20.0, 200.0),
    }


DAMPING = 0.8
PRIOR_MASS = 0.5
PRIOR_STIFF = 1.0


def coarsen_sum(values):
    extent_x, extent_y, extent_z = values.shape
    blocks = values.reshape(extent_x // 2, 2, extent_y // 2, 2, extent_z // 2, 2)
    return blocks.sum(axis=(1, 3, 5))


def refine(values):
    return jnp.repeat(jnp.repeat(jnp.repeat(values, 2, axis=0), 2, axis=1), 2, axis=2)


def neighbours(padded):
    centre = padded[1:-1, 1:-1, :]
    border = jnp.zeros_like(centre[:, :, :1])
    beside = (padded[:-2, 1:-1, :], padded[2:, 1:-1, :], padded[1:-1, :-2, :], padded[1:-1, 2:, :],
              jnp.concatenate([border, centre[:, :, :-1]], axis=2),
              jnp.concatenate([centre[:, :, 1:], border], axis=2))
    return beside, centre


def summed(entries):
    result = entries[0]
    for entry in entries[1:]:
        result = result + entry
    return result


def inside_flags(index_x, index_y, extent_x, extent_y, extent_z):
    index_z = jnp.arange(extent_z, dtype=jnp.int32)[None, None, :]
    return (index_x > 0, index_x < extent_x - 1, index_y > 0, index_y < extent_y - 1,
            index_z > 0, index_z < extent_z - 1)


def face_weights(cond_padded, level_scale, interior):
    beside, centre = neighbours(cond_padded)
    return tuple(level_scale * jnp.where(is_inner, 0.5 * (centre + neighbour), centre)
                 for is_inner, neighbour in zip(interior, beside))


def apply_operator(padded, couplings, diagonal):
    beside, centre = neighbours(padded)
    return diagonal * centre - summed([weight * neighbour for weight, neighbour in zip(couplings, beside)])


def prior_apply(padded):
    beside, centre = neighbours(padded)
    return PRIOR_MASS * centre + PRIOR_STIFF * (6.0 * centre - summed(list(beside)))


def sensitivity(cond_padded, state_padded, probe_padded, interior):
    cond_side, cond_mid = neighbours(cond_padded)
    state_side, state_mid = neighbours(state_padded)
    probe_side, probe_mid = neighbours(probe_padded)
    flux_mid = cond_mid * probe_mid
    return summed([jnp.where(is_inner, 0.5 * (flux_mid + cond_near * probe_near), flux_mid) * (state_mid - state_near)
                   for is_inner, cond_near, probe_near, state_near
                   in zip(interior, cond_side, probe_side, state_side)])


def misfit_gradient(cond_padded, state_padded, adjoint_padded, interior):
    cond_mid = neighbours(cond_padded)[1]
    state_side, state_mid = neighbours(state_padded)
    adjoint_side, adjoint_mid = neighbours(adjoint_padded)
    return cond_mid * summed([jnp.where(is_inner, 0.5, 1.0) * (state_mid - state_near) * (adjoint_mid - adjoint_near)
                              for is_inner, state_near, adjoint_near in zip(interior, state_side, adjoint_side)])


def smooth(iterate, source, couplings, diagonal, padder, sweeps):
    for sweep_index in range(sweeps):
        if iterate is None:
            iterate = DAMPING * source / diagonal
        else:
            iterate = iterate + DAMPING * (source - apply_operator(padder(iterate), couplings, diagonal)) / diagonal
    return iterate


def vcycle(source, depth_index, operators, padders, coarse_solve):
    if depth_index == len(operators):
        return coarse_solve(source)
    couplings, diagonal = operators[depth_index]
    iterate = smooth(None, source, couplings, diagonal, padders[depth_index], SWEEPS)
    defect = source - apply_operator(padders[depth_index](iterate), couplings, diagonal)
    iterate = iterate + refine(vcycle(coarsen_sum(defect), depth_index + 1, operators, padders, coarse_solve))
    return smooth(iterate, source, couplings, diagonal, padders[depth_index], SWEEPS)


def solve(source, operators, padders, coarse_solve):
    iterate = None
    for cycle_index in range(VCYCLES):
        if iterate is None:
            iterate = vcycle(source, 0, operators, padders, coarse_solve)
        else:
            couplings, diagonal = operators[0]
            defect = source - apply_operator(padders[0](iterate), couplings, diagonal)
            iterate = iterate + vcycle(defect, 0, operators, padders, coarse_solve)
    return iterate


def plain_pad(values):
    return jnp.pad(values, ((1, 1), (1, 1), (0, 0)))


def level_flags(values):
    extent_x, extent_y, extent_z = values.shape
    return inside_flags(jnp.arange(extent_x, dtype=jnp.int32)[:, None, None],
                        jnp.arange(extent_y, dtype=jnp.int32)[None, :, None], extent_x, extent_y, extent_z)


def reference(log_conductivity, state, gradient, prior_sample, sensor_cells, noise_precision):
    cond_levels = [jnp.exp(log_conductivity)]
    for depth_index in range(LEVELS - 1):
        cond_levels.append(coarsen_sum(cond_levels[-1]) / 8.0)
    operators = []
    for depth_index in range(LEVELS - 1):
        couplings = face_weights(plain_pad(cond_levels[depth_index]), float(2 ** depth_index),
                                 level_flags(cond_levels[depth_index]))
        operators.append((couplings, summed(list(couplings))))
    coarsest = LEVELS - 1
    coarse_couplings = face_weights(plain_pad(cond_levels[coarsest]), float(2 ** coarsest),
                                    level_flags(cond_levels[coarsest]))
    coarse_diagonal = summed(list(coarse_couplings))
    padders = [plain_pad] * (LEVELS - 1)

    def coarse_solve(source):
        return smooth(None, source, coarse_couplings, coarse_diagonal, plain_pad, COARSE_SWEEPS)

    fine_flags = level_flags(cond_levels[0])
    weight_field = jnp.zeros((NX * NY * NZ,), jnp.float32).at[sensor_cells].add(noise_precision).reshape(NX, NY, NZ)
    cond_padded = plain_pad(cond_levels[0])
    state_padded = plain_pad(state)

    def hessian_apply(direction):
        direction_padded = plain_pad(direction)
        change = solve(sensitivity(cond_padded, state_padded, direction_padded, fine_flags), operators, padders, coarse_solve)
        adjoint = solve(weight_field * change, operators, padders, coarse_solve)
        return misfit_gradient(cond_padded, state_padded, plain_pad(adjoint), fine_flags) + prior_apply(direction_padded)

    source = prior_apply(plain_pad(prior_sample)) - gradient
    step_field = jnp.zeros_like(source)
    residual = source
    direction = source
    norm_now = jnp.sum(residual * residual)
    for iteration in range(CG_ITERS):
        curved = hessian_apply(direction)
        step_length = norm_now / jnp.sum(direction * curved)
        step_field = step_field + step_length * direction
        residual = residual - step_length * curved
        norm_next = jnp.sum(residual * residual)
        direction = residual + (norm_next / norm_now) * direction
        norm_now = norm_next
    return step_field, residual
```

```python
import jax
import jax.numpy as jnp
from jax import lax
from jax.experimental import pallas as pl
from jax.experimental.pallas import tpu as pltpu
from jax.sharding import PartitionSpec as P

DAMPING = 0.8
KEPT = 0.2
PRIOR_MASS = 0.5
COARSE_SWEEPS = 6
HALO = 4
DEEP = 5
WIDE = 2
VMEM_LIMIT = 24 * 1024 * 1024
EXACT = lax.Precision.HIGHEST


def rotate(x, axis, shift):
    size = lax.axis_size(axis)
    return lax.ppermute(x, axis, [(i, (i + shift) % size) for i in range(size)])


def shifted(v, step, dim):
    size = v.shape[dim]
    return pltpu.roll(v, step % size, dim)


def dot(a, b):
    return lax.dot_general(
        a, b, (((1,), (0,)), ((), ())), precision=EXACT, preferred_element_type=jnp.float32
    )


def iota(shape, dim):
    return lax.broadcasted_iota(jnp.int32, shape, dim)


def total(tile):
    return jnp.sum(jnp.sum(tile, axis=1, keepdims=True), axis=0, keepdims=True)


def fold(plane):
    rows, lanes = plane.shape
    parts = [
        plane[r : r + 8, c : c + 128] for r in range(0, rows, 8) for c in range(0, lanes, 128)
    ]
    out = parts[0]
    for part in parts[1:]:
        out = out + part
    return out


def z_pairs(lanes):
    half = lanes // 2
    return (iota((lanes, half), 0) // 2 == iota((lanes, half), 1)).astype(jnp.float32)


def z_copies(lanes):
    return (iota((lanes, 2 * lanes), 0) == iota((lanes, 2 * lanes), 1) // 2).astype(jnp.float32)


def restrict_rows(planes, first_row, rows):
    extent = planes[0].shape[0]
    here = iota(planes[0].shape, 0)
    inside = (here >= first_row) & (here < first_row + rows)
    pick = (
        (iota((rows // 2, extent), 1) - first_row + 2) // 2 - 1 == iota((rows // 2, extent), 0)
    ).astype(jnp.float32)
    halves = []
    for x in range(0, len(planes), 2):
        pair = jnp.where(inside, planes[x] + planes[x + 1], 0.0)
        halves.append(dot(pick, pair))
    packed = dot(jnp.concatenate(halves, axis=0), z_pairs(planes[0].shape[1]))
    return packed.reshape(len(planes) // 2, rows // 2, packed.shape[1])


def swap_sum(v, dim, stride):
    even = (iota(v.shape, dim) // stride) % 2 == 0
    return v + jnp.where(even, shifted(v, -stride, dim), shifted(v, stride, dim))


def off_diagonal(v, low, high, fx, fx_high, fy, fz, step):
    out = fy * shifted(v, step, 0) + shifted(fy * v, -step, 0)
    out = out + (fz * shifted(v, step, 1) + shifted(fz * v, -step, 1))
    if low is not None:
        out = out + fx * low
    if high is not None:
        out = out + fx_high * high
    return out


def coefficients(planes, scale, step, x_mask, y_mask, z_mask, outside):
    count = len(planes)
    faces = [None] * count
    for x in range(count):
        low = planes[x] if x == 0 else planes[x - 1]
        faces[x] = (scale * x_mask(x)) * (0.5 * (planes[x] + low))
    out = []
    for x in range(count):
        k = planes[x]
        fy = (scale * y_mask) * (0.5 * (k + shifted(k, step, 0)))
        fz = (scale * z_mask) * (0.5 * (k + shifted(k, step, 1)))
        diag = (scale * outside(x)) * k + fy + shifted(fy, -step, 0) + fz + shifted(fz, -step, 1)
        diag = diag + faces[x]
        if x + 1 < count:
            diag = diag + faces[x + 1]
        out.append((faces[x], fy, fz, DAMPING / diag))
    return out


def flag(condition):
    return jnp.where(condition, 1.0, 0.0).astype(jnp.float32)


def place_blocks(refs, place, sizes, planes, rows, put):
    size_x, size_y = sizes
    for s in range(size_x):
        at_x = lax.rem(place[0] - s + size_x, size_x)
        for t in range(size_y):
            at_y = lax.rem(place[1] - t + size_y, size_y)
            put(at_x, at_y, refs[s], t)


def placed_whole(refs, place, sizes, planes, per, whole_ref):
    block_rows = whole_ref.shape[1] // sizes[1]

    def put(at_x, at_y, ref, t):
        row = pl.multiple_of(at_y * block_rows, block_rows)
        for x in range(planes):
            whole_ref[at_x * planes + x, pl.ds(row, block_rows), :] = ref[t * per + x]

    place_blocks(refs, place, sizes, planes, block_rows, put)


def summed_tiles(refs, sizes, per, index):
    tile = None
    for s in range(sizes[0]):
        for t in range(sizes[1]):
            part = refs[s][t * per + index]
            tile = part if tile is None else tile + part
    return total(tile)


def coarse_correction(source, mid, out, level1, level2):
    fx1, fy1, fz1, rd1 = level1
    fx2, fy2, fz2, rd2 = level2
    count = source.shape[0]

    def off1(ref, x):
        low = ref[x - 1] if x > 0 else None
        high = ref[x + 1] if x + 1 < count else None
        fx_high = fx1[x + 1] if x + 1 < count else None
        return off_diagonal(ref[x], low, high, fx1[x], fx_high, fy1[x], fz1[x], 1)

    for x in range(count):
        mid[x] = rd1[x] * source[x]
    coarse = []
    for x in range(0, count, 2):
        pair = KEPT * (source[x] + source[x + 1]) + (off1(mid, x) + off1(mid, x + 1))
        coarse.append(swap_sum(swap_sum(pair, 0, 1), 1, 1))
    half = count // 2
    iterate = [rd2[x] * coarse[x] for x in range(half)]
    for sweep in range(COARSE_SWEEPS - 1):
        new = []
        for x in range(half):
            low = iterate[x - 1] if x > 0 else None
            high = iterate[x + 1] if x + 1 < half else None
            fx_high = fx2[x + 1] if x + 1 < half else None
            off = off_diagonal(iterate[x], low, high, fx2[x], fx_high, fy2[x], fz2[x], 2)
            new.append(KEPT * iterate[x] + rd2[x] * (coarse[x] + off))
        iterate = new
    for x in range(count):
        mid[x] = mid[x] + iterate[x // 2]
    for x in range(count):
        out[x] = KEPT * mid[x] + rd1[x] * (source[x] + off1(mid, x))


def prolonged(whole_ref, place, planes, rows, pad):
    count, extent, lanes = whole_ref.shape
    own_x = planes - 2 * (pad // 2)
    own_y = (rows - 2 * pad) // 2
    first = place[1] * own_y - pad // 2
    pick = (iota((rows, extent), 1) == first + iota((rows, extent), 0) // 2).astype(jnp.float32)
    parts = []
    for x in range(planes):
        at = jnp.clip(place[0] * own_x - pad // 2 + x, 0, count - 1)
        parts.append(dot(pick, whole_ref[at]))
    wide = dot(jnp.concatenate(parts, axis=0), z_copies(lanes))
    return [wide[x * rows : (x + 1) * rows] for x in range(planes)]


def frame_masks(place, shape, pad, sizes):
    planes, rows, lanes = shape
    own_x, own_y = planes - 2 * pad, rows - 2 * pad
    all_x, all_y = own_x * sizes[0], own_y * sizes[1]
    base_x, base_y = place[0] * own_x - pad, place[1] * own_y - pad
    at_y = base_y + iota((rows, lanes), 0)
    at_z = iota((rows, lanes), 1)
    y_mask = flag((at_y >= 1) & (at_y < all_y))
    z_mask = flag(at_z >= 1)
    edges = flag(at_y == 0) + flag(at_y == all_y - 1) + flag(at_z == 0) + flag(at_z == lanes - 1)

    def x_mask(x):
        at = base_x + x
        return flag((at >= 1) & (at < all_x))

    def outside(x):
        at = base_x + x
        return edges + (flag(at == 0) + flag(at == all_x - 1))

    return x_mask, y_mask, z_mask, outside


def prior_rows(center, low, high, up, down, x_low, x_high, y_mask, z_mask, outside):
    rows, lanes = center.shape
    y_next = shifted(y_mask, -1, 0)
    z_next = shifted(z_mask, -1, 1)
    out = (PRIOR_MASS + outside) * center + x_low * (center - low) + x_high * (center - high)
    out = out + y_mask * (center - up) + y_next * (center - down)
    out = out + z_mask * (center - shifted(center, 1, 1))
    return out + z_next * (center - shifted(center, -1, 1))


def fine_restricted(base, fields, fx, fy, fz, out_ref, first, own):
    planes = []
    for x in range(first, first + own):
        off = off_diagonal(
            fields[x], fields[x - 1], fields[x + 1], fx[x], fx[x + 1], fy[x], fz[x], 1
        )
        planes.append(KEPT * base[x] + off)
    rows = planes[0].shape[0]
    coarse = restrict_rows(planes, first, rows - 2 * first)
    for x in range(coarse.shape[0]):
        out_ref[x] = coarse[x]


def sensitivity_planes(q, hux, huy, huz, nbu, first, last):
    faces = {x: hux[x] * (q(x) + q(x - 1)) for x in range(first, last + 1)}
    out = {}
    for x in range(first, last):
        mid = q(x)
        along_y = huy[x] * (mid + shifted(mid, 1, 0))
        along_z = huz[x] * (mid + shifted(mid, 1, 1))
        z = faces[x] - faces[x + 1] + nbu[x] * mid
        z = z + (along_y - shifted(along_y, -1, 0))
        out[x] = z + (along_z - shifted(along_z, -1, 1))
    return out


def first_residual_stage(z, fx, fy, fz, rd, z_ref, out_ref, planes):
    for x in z:
        z_ref[x] = z[x]
    iterate = {x: rd[x] * z[x] for x in range(HALO - 1, planes - HALO + 1)}
    fine_restricted(z, iterate, fx, fy, fz, out_ref, HALO, planes - 2 * HALO)


def call(kernel, outs, scratch, inputs, smem_first=True):
    vmem = pl.BlockSpec(memory_space=pltpu.VMEM)
    smem = pl.BlockSpec(memory_space=pltpu.SMEM)
    return pl.pallas_call(
        kernel,
        out_shape=[jax.ShapeDtypeStruct(shape, jnp.float32) for shape in outs],
        in_specs=[smem if smem_first and i == 0 else vmem for i in range(len(inputs))],
        out_specs=[vmem] * len(outs),
        scratch_shapes=[pltpu.VMEM(shape, jnp.float32) for shape in scratch],
        compiler_params=pltpu.CompilerParams(vmem_limit_bytes=VMEM_LIMIT),
    )(*inputs)


def own_coarse_conductivity(log_cond):
    def kernel(log_ref, out_ref):
        planes = [jnp.exp(log_ref[x]) for x in range(log_ref.shape[0])]
        coarse = restrict_rows(planes, 0, planes[0].shape[0])
        for x in range(coarse.shape[0]):
            out_ref[x] = coarse[x] * 0.125

    x, y, z = log_cond.shape
    return call(kernel, [(x // 2, y // 2, z // 2)], [], [log_cond], smem_first=False)[0]


def gathered(own):
    size_x, size_y = lax.axis_size("gx"), lax.axis_size("gy")
    row = jnp.concatenate([own] + [rotate(own, "gy", t) for t in range(1, size_y)], axis=0)
    return [row] + [rotate(row, "gx", s) for s in range(1, size_x)]


FIELD_DEPTHS = (DEEP, HALO, HALO, HALO, WIDE)


def setup_rows(own_x):
    starts, at = [], 0
    for depth in FIELD_DEPTHS:
        starts.append(at)
        at += (own_x + 2 * depth) * depth
    return starts, -(-at // 8) * 8


def field_plane(fields, low, high, index, x):
    depth = FIELD_DEPTHS[index]
    start = sum(FIELD_DEPTHS[:index])
    own = fields[index].shape[0]
    if x < depth:
        return low[start + x]
    if x < depth + own:
        return fields[index][x - depth]
    return high[start + x - depth - own]


def pack_setup_edges(fields, low, high):
    own_x, own_y, lanes = fields[0].shape
    starts, rows = setup_rows(own_x)
    number = len(fields)

    def kernel(*refs):
        fields = refs[:number]
        low, high, first_ref, last_ref = refs[number:]
        for index, depth in enumerate(FIELD_DEPTHS):
            for x in range(own_x + 2 * depth):
                plane = field_plane(fields, low, high, index, x)
                at = starts[index] + x * depth
                first_ref[at : at + depth, :] = plane[:depth]
                last_ref[at : at + depth, :] = plane[own_y - depth :]

    inputs = list(fields) + [low, high]
    return call(kernel, [(rows, lanes)] * 2, [], inputs, smem_first=False)


def setup(place, sizes, fields, low, high, before, after):
    own_x, own_y, lanes = fields[0].shape
    frame = (own_x + 2 * HALO, own_y + 2 * HALO, lanes)
    starts, _ = setup_rows(own_x)
    number = len(fields)
    coarse = (own_x // 2, own_y // 2, lanes // 2)

    def kernel(*refs):
        place = refs[0]
        fields = refs[1 : 1 + number]
        low, high, before, after = refs[1 + number : 5 + number]
        outs = refs[5 + number : 18 + number]
        cond, hux, huy, huz, nbu, fx, fy, fz, rd, weight, source, z_out, b1 = outs
        prior = refs[18 + number]
        state = refs[19 + number]
        grad = refs[20 + number]

        def assemble(index, ref, x_skip, first_row):
            depth = FIELD_DEPTHS[index]
            for x in range(own_x + 2 * depth):
                at = starts[index] + x * depth
                ref[x + x_skip, first_row : first_row + depth, :] = before[at : at + depth, :]
                ref[x + x_skip, first_row + depth : first_row + depth + own_y, :] = field_plane(
                    fields, low, high, index, x
                )
                end = first_row + depth + own_y
                ref[x + x_skip, end : end + depth, :] = after[at : at + depth, :]

        zero = jnp.zeros(frame[1:], jnp.float32)
        for x in range(frame[0]):
            weight[x] = zero
        assemble(0, prior, 0, 0)
        assemble(1, grad, 0, 0)
        assemble(2, cond, 0, 0)
        assemble(3, state, 0, 0)
        assemble(4, weight, HALO - WIDE, HALO - WIDE)
        x_mask, y_mask, z_mask, outside = frame_masks(place, frame, HALO, sizes)
        planes, rows = frame[:2]
        for x in range(planes):
            center = prior[x + 1, 1 : 1 + rows, :]
            value = prior_rows(
                center,
                prior[x, 1 : 1 + rows, :],
                prior[x + 2, 1 : 1 + rows, :],
                prior[x + 1, 0:rows, :],
                prior[x + 1, 2 : 2 + rows, :],
                x_mask(x),
                x_mask(x + 1),
                y_mask,
                z_mask,
                outside(x),
            )
            source[x] = value - grad[x]
        for x in range(planes):
            cond[x] = jnp.exp(cond[x])
        for x in range(planes):
            u = state[x]
            if x > 0:
                hux[x] = (0.5 * x_mask(x)) * (u - state[x - 1])
            else:
                hux[x] = zero
            huy[x] = (0.5 * y_mask) * (u - shifted(u, 1, 0))
            huz[x] = (0.5 * z_mask) * (u - shifted(u, 1, 1))
            nbu[x] = outside(x) * u
        found = coefficients(
            [cond[x] for x in range(planes)], 1.0, 1, x_mask, y_mask, z_mask, outside
        )
        for x in range(planes):
            fx[x], fy[x], fz[x], rd[x] = found[x]
        z = sensitivity_planes(
            lambda x: cond[x] * source[x], hux, huy, huz, nbu, 1, planes - 1
        )
        z_out[0] = zero
        z_out[planes - 1] = zero
        first_residual_stage(z, fx, fy, fz, rd, z_out, b1, planes)

    deep = (own_x + 2 * DEEP, -(-(own_y + 2 * DEEP) // 8) * 8, lanes)
    return call(
        kernel,
        [frame] * 12 + [coarse],
        [deep, frame, frame],
        [place] + list(fields) + [low, high, before, after],
    )


def coarse_setup(place, sizes, blocks, shape):
    planes, rows, lanes = shape
    whole = (planes * sizes[0], rows * sizes[1], lanes)
    half = (whole[0] // 2,) + whole[1:]

    def kernel(*refs):
        place = refs[0]
        blocks = refs[1 : 1 + sizes[0]]
        outs = refs[1 + sizes[0] : 9 + sizes[0]]
        cond = refs[9 + sizes[0]]
        placed_whole(blocks, place, sizes, planes, planes, cond)
        at_y = iota(whole[1:], 0)
        at_z = iota(whole[1:], 1)

        def level(values, scale, step, refs):
            count = len(values)
            y_mask = flag(at_y >= step)
            z_mask = flag(at_z >= step)
            edges = (
                flag(at_y < step)
                + flag(at_y >= whole[1] - step)
                + flag(at_z < step)
                + flag(at_z >= lanes - step)
            )

            def x_mask(x):
                return 1.0 if x > 0 else 0.0

            def outside(x):
                return edges + float((x == 0) + (x == count - 1))

            found = coefficients(values, scale, step, x_mask, y_mask, z_mask, outside)
            for x in range(count):
                for ref, value in zip(refs, found[x]):
                    ref[x] = value

        level([cond[x] for x in range(whole[0])], 2.0, 1, outs[:4])
        coarse = []
        for x in range(half[0]):
            pair = cond[2 * x] + cond[2 * x + 1]
            coarse.append(0.125 * swap_sum(swap_sum(pair, 0, 1), 1, 1))
        level(coarse, 4.0, 2, outs[4:])

    return call(kernel, [whole] * 4 + [half] * 4, [whole], [place] + list(blocks))


def middle(place, sizes, blocks, per, levels, fine, z, direction, weight, earlier):
    planes, rows, lanes = z.shape
    own_x = planes - 2 * HALO
    coarse = (own_x // 2, (rows - 2 * HALO) // 2, lanes // 2)
    whole = levels[0].shape
    first_time = earlier is None
    sums = 2 if first_time else 1
    extra = [] if first_time else [earlier[0], earlier[1], earlier[2]]
    inputs = [place] + list(blocks) + list(levels) + list(fine) + [z, direction, weight] + extra

    def kernel(*refs):
        at = 0

        def take(number):
            nonlocal at
            at += number
            return refs[at - number : at]

        (place,) = take(1)
        blocks = take(sizes[0])
        levels = take(8)
        fx, fy, fz, rd = take(4)
        z, direction, weight = take(3)
        old = take(len(extra))
        b1, second, curved, kept, combined, ratio_ref = take(6)
        whole_source, whole_mid, whole_out, mid = take(4)
        frame_rows = iota((rows, lanes), 0)
        own_rows = flag((frame_rows >= HALO) & (frame_rows < rows - HALO))
        placed_whole(blocks, place, sizes, coarse[0], per, whole_source)
        coarse_correction(whole_source, whole_mid, whole_out, levels[:4], levels[4:])
        correction = prolonged(whole_out, place, planes // 2, rows, HALO)
        if first_time:
            ratio = None
            for x in range(planes):
                combined[x] = direction[x]
            ratio_ref[...] = jnp.zeros((8, 128), jnp.float32)
        else:
            norm = summed_tiles(blocks, sizes, per, coarse[0])
            ratio = norm / old[2][0:1, 0:1]
            for x in range(planes):
                combined[x] = direction[x] + ratio * old[1][x]
            ratio_ref[...] = jnp.broadcast_to(norm, (8, 128))
        for x in range(1, planes - 1):
            mid[x] = rd[x] * z[x] + correction[x // 2]
        zero = jnp.zeros((rows, lanes), jnp.float32)
        forms = zero
        rights = {}
        for x in range(2, planes - 2):
            off = off_diagonal(mid[x], mid[x - 1], mid[x + 1], fx[x], fx[x + 1], fy[x], fz[x], 1)
            change = KEPT * mid[x] + rd[x] * (z[x] + off)
            if first_time:
                kept[x] = change
            else:
                change = change + ratio * old[0][x]
            right = weight[x] * change
            second[x] = right
            rights[x] = right
            if HALO <= x < planes - HALO:
                forms = forms + right * change
        for x in (0, 1, planes - 2, planes - 1):
            second[x] = zero
            if first_time:
                kept[x] = zero
        if not first_time:
            kept[...] = jnp.zeros(kept.shape, jnp.float32)
        x_mask, y_mask, z_mask, outside = frame_masks(place, (planes, rows, lanes), HALO, sizes)
        squares = zero
        for x in range(HALO, planes - HALO):
            center = combined[x]
            value = prior_rows(
                center,
                combined[x - 1],
                combined[x + 1],
                shifted(center, 1, 0),
                shifted(center, -1, 0),
                x_mask(x),
                x_mask(x + 1),
                y_mask,
                z_mask,
                outside(x),
            )
            curved[x - HALO] = value
            forms = forms + center * value
            if first_time:
                squares = squares + center * center
        iterate = {x: rd[x] * rights[x] for x in range(HALO - 1, planes - HALO + 1)}
        fine_restricted(rights, iterate, fx, fy, fz, b1, HALO, own_x)
        b1[coarse[0]] = fold(jnp.where(own_rows > 0, forms, 0.0))
        if first_time:
            b1[coarse[0] + 1] = fold(jnp.where(own_rows > 0, squares, 0.0))

    frame = (planes, rows, lanes)
    return call(
        kernel,
        [
            (coarse[0] + sums,) + coarse[1:],
            frame,
            (own_x, rows, lanes),
            frame if first_time else (8, 128),
            frame,
            (8, 128),
        ],
        [whole, whole, whole, frame],
        inputs,
    )


def image_planes(levels, fine, place, sizes, blocks, per, second, curved, cond, faces, scratch):
    fx, fy, fz, rd = fine
    hux, huy, huz, nbu = faces
    whole_source, whole_mid, whole_out, mid = scratch
    planes, rows, lanes = second.shape
    placed_whole(blocks, place, sizes, (planes - 2 * HALO) // 2, per, whole_source)
    coarse_correction(whole_source, whole_mid, whole_out, levels[:4], levels[4:])
    correction = prolonged(whole_out, place, planes // 2, rows, HALO)
    for x in range(2, planes - 2):
        mid[x] = rd[x] * second[x] + correction[x // 2]
    adjoint = {}
    for x in range(3, planes - 3):
        off = off_diagonal(mid[x], mid[x - 1], mid[x + 1], fx[x], fx[x + 1], fy[x], fz[x], 1)
        adjoint[x] = KEPT * mid[x] + rd[x] * (second[x] + off)
    out = {}
    along_x = {
        x: hux[x] * (adjoint[x] - adjoint[x - 1]) for x in range(HALO, planes - HALO + 1)
    }
    for x in range(HALO, planes - HALO):
        p = adjoint[x]
        along_y = huy[x] * (p - shifted(p, 1, 0))
        along_z = huz[x] * (p - shifted(p, 1, 1))
        value = along_x[x] + along_x[x + 1] + nbu[x] * p
        value = value + (along_y + shifted(along_y, -1, 0))
        value = value + (along_z + shifted(along_z, -1, 1))
        out[x] = cond[x] * value + curved[x - HALO]
    return out


def end_first(place, sizes, blocks, per, levels, fine, second, curved, cond, faces, source):
    planes, rows, lanes = second.shape
    own_x, own_y = planes - 2 * HALO, rows - 2 * HALO
    whole = levels[0].shape
    coarse = own_x // 2
    inputs = (
        [place] + list(blocks) + list(levels) + list(fine)
        + [second, curved, cond] + list(faces) + [source]
    )

    def kernel(*refs):
        place = refs[0]
        n = sizes[0]
        blocks = refs[1 : 1 + n]
        levels = refs[1 + n : 9 + n]
        fine = refs[9 + n : 13 + n]
        second, curved, cond = refs[13 + n : 16 + n]
        faces = refs[16 + n : 20 + n]
        source = refs[20 + n]
        first_ref, last_ref, own_ref, tile_ref, norm_ref, step_ref = refs[21 + n : 27 + n]
        *scratch, hold = refs[27 + n : 32 + n]
        image = image_planes(
            levels, fine, place, sizes, blocks, per, second, curved, cond, faces, scratch
        )
        form = summed_tiles(blocks, sizes, per, coarse)
        norm = summed_tiles(blocks, sizes, per, coarse + 1)
        step = norm / form
        norm_ref[...] = jnp.broadcast_to(norm, (8, 128))
        step_ref[...] = jnp.broadcast_to(step, (8, 128))
        squares = jnp.zeros((own_y, lanes), jnp.float32)
        for x in range(HALO, planes - HALO):
            hold[x - HALO] = source[x] - step * image[x]
        for x in range(own_x):
            value = hold[x, HALO : HALO + own_y, :]
            squares = squares + value * value
            own_ref[x] = value
            if x < HALO:
                first_ref[x] = value
            if x >= own_x - HALO:
                last_ref[x - own_x + HALO] = value
        tile_ref[0] = fold(squares)

    strip = (HALO, own_y, lanes)
    return call(
        kernel,
        [strip, strip, (own_x, own_y, lanes), (1, 8, 128), (8, 128), (8, 128)],
        [whole, whole, whole, (planes, rows, lanes), (own_x, rows, lanes)],
        inputs,
    )


def end_second(
    place, sizes, blocks, per, levels, fine, second, curved, cond, faces,
    source, remaining, combined, norm, step
):
    planes, rows, lanes = second.shape
    own_x, own_y = planes - 2 * HALO, rows - 2 * HALO
    whole = levels[0].shape
    coarse = own_x // 2
    inputs = (
        [place] + list(blocks) + list(levels) + list(fine)
        + [second, curved, cond] + list(faces) + [source, remaining, combined, norm, step]
    )

    def kernel(*refs):
        place = refs[0]
        n = sizes[0]
        blocks = refs[1 : 1 + n]
        levels = refs[1 + n : 9 + n]
        fine = refs[9 + n : 13 + n]
        second, curved, cond = refs[13 + n : 16 + n]
        faces = refs[16 + n : 20 + n]
        source, remaining, combined, norm, step = refs[20 + n : 25 + n]
        step_out, residual_out = refs[25 + n : 27 + n]
        *scratch, hold, hold_step = refs[27 + n : 33 + n]
        image = image_planes(
            levels, fine, place, sizes, blocks, per, second, curved, cond, faces, scratch
        )
        form = summed_tiles(blocks, sizes, per, coarse)
        now = norm[0:1, 0:1] / form
        before = step[0:1, 0:1]
        for x in range(HALO, planes - HALO):
            hold[x - HALO] = now * image[x]
            hold_step[x - HALO] = before * source[x] + now * combined[x]
        for x in range(own_x):
            residual_out[x] = remaining[x] - hold[x, HALO : HALO + own_y, :]
            step_out[x] = hold_step[x, HALO : HALO + own_y, :]

    own = (own_x, own_y, lanes)
    hold = (own_x, rows, lanes)
    return call(
        kernel,
        [own, own],
        [whole, whole, whole, (planes, rows, lanes), hold, hold],
        inputs,
    )


def pack_edges(own, low, high):
    own_x, own_y, lanes = own.shape
    planes = own_x + 2 * HALO

    def kernel(own, low, high, first_ref, last_ref):
        for x in range(planes):
            if x < HALO:
                ref, at = low, x
            elif x < HALO + own_x:
                ref, at = own, x - HALO
            else:
                ref, at = high, x - HALO - own_x
            first_ref[x] = ref[at, :HALO, :]
            last_ref[x] = ref[at, own_y - HALO :, :]

    strip = (planes, HALO, lanes)
    return call(kernel, [strip] * 2, [], [own, low, high], smem_first=False)


def begin(own, low, high, before, after, tile, cond, faces, fine):
    own_x, own_y, lanes = own.shape
    planes, rows = own_x + 2 * HALO, own_y + 2 * HALO
    frame = (planes, rows, lanes)
    coarse = (own_x // 2, own_y // 2, lanes // 2)

    def kernel(
        own, low, high, before, after, tile, cond, hux, huy, huz, nbu, fx, fy, fz, rd,
        direction, z_out, b1,
    ):
        for x in range(planes):
            if x < HALO:
                value = low[x]
            elif x < HALO + own_x:
                value = own[x - HALO]
            else:
                value = high[x - HALO - own_x]
            direction[x, HALO : HALO + own_y, :] = value
            direction[x, :HALO, :] = before[x]
            direction[x, HALO + own_y :, :] = after[x]
        z = sensitivity_planes(
            lambda x: cond[x] * direction[x], hux, huy, huz, nbu, 1, planes - 1
        )
        zero = jnp.zeros((rows, lanes), jnp.float32)
        z_out[0] = zero
        z_out[planes - 1] = zero
        first_residual_stage(z, fx, fy, fz, rd, z_out, b1, planes)
        b1[coarse[0]] = tile[0]

    return call(
        kernel,
        [frame, frame, (coarse[0] + 1,) + coarse[1:]],
        [],
        [own, low, high, before, after, tile, cond] + list(faces) + list(fine),
        smem_first=False,
    )


def on_device(log_conductivity, state, gradient, prior_sample, sensor_cells, noise_precision):
    sizes = (lax.axis_size("gx"), lax.axis_size("gy"))
    place_x = lax.axis_index("gx")
    place_y = lax.axis_index("gy")
    place = jnp.stack([place_x, place_y]).astype(jnp.int32)
    cells_x, cells_y, cells_z = log_conductivity.shape
    coarse = (cells_x // 2, cells_y // 2, cells_z // 2)

    cond_blocks = gathered(own_coarse_conductivity(log_conductivity))

    rows_all = cells_y * sizes[1]
    sensor_row = sensor_cells // (rows_all * cells_z)
    sensor_column = sensor_cells // cells_z % rows_all
    sensor_depth = sensor_cells % cells_z
    local_cell = (
        (sensor_row - place_x * cells_x) * cells_y + (sensor_column - place_y * cells_y)
    ) * cells_z + sensor_depth
    weight = (
        jnp.zeros((cells_x * cells_y * cells_z,), jnp.float32)
        .at[local_cell]
        .add(noise_precision)
        .reshape(cells_x, cells_y, cells_z)
    )

    fields = (prior_sample, gradient, log_conductivity, state, weight)
    first = jnp.concatenate([v[:d] for v, d in zip(fields, FIELD_DEPTHS)], axis=0)
    last = jnp.concatenate([v[cells_x - d :] for v, d in zip(fields, FIELD_DEPTHS)], axis=0)
    low, high = rotate(last, "gx", 1), rotate(first, "gx", -1)
    first, last = pack_setup_edges(fields, low, high)
    before, after = rotate(last, "gy", 1), rotate(first, "gy", -1)
    (cond, hux, huy, huz, nbu, fx, fy, fz, rd, weight, source, z, b1) = setup(
        place, sizes, fields, low, high, before, after
    )
    faces = (hux, huy, huz, nbu)
    fine = (fx, fy, fz, rd)
    levels = coarse_setup(place, sizes, cond_blocks, coarse)

    b1, second, curved, kept, _, _ = middle(
        place, sizes, gathered(b1), coarse[0], levels, fine, z, source, weight, None
    )
    first, last, remaining, tile, norm, step = end_first(
        place, sizes, gathered(b1), coarse[0] + 2, levels, fine, second, curved, cond, faces,
        source,
    )
    low, high = rotate(last, "gx", 1), rotate(first, "gx", -1)
    first, last = pack_edges(remaining, low, high)
    before, after = rotate(last, "gy", 1), rotate(first, "gy", -1)
    direction, z, b1 = begin(remaining, low, high, before, after, tile, cond, faces, fine)
    b1, second, curved, _, combined, norm = middle(
        place, sizes, gathered(b1), coarse[0] + 1, levels, fine, z, direction, weight,
        (kept, source, norm),
    )
    return tuple(
        end_second(
            place, sizes, gathered(b1), coarse[0] + 1, levels, fine, second, curved, cond,
            faces, source, remaining, combined, norm, step,
        )
    )


def solution(mesh):
    field = P(("ens", "gx"), "gy", None)
    sensors = P(("ens", "gx", "gy"))
    return jax.shard_map(
        on_device,
        mesh=mesh,
        in_specs=(field, field, field, field, sensors, sensors),
        out_specs=(field, field),
        check_vma=False,
    )
```

```python
import jax
import jax.numpy as jnp
from jax import lax
from jax.experimental import pallas as pl
from jax.experimental.pallas import tpu as pltpu
from jax.sharding import PartitionSpec as P

DAMPING = 0.8
KEPT = 0.2
PRIOR_MASS = 0.5
COARSE_SWEEPS = 6
HALO = 4
DEEP = 5
WIDE = 2
VMEM_LIMIT = 24 * 1024 * 1024
EXACT = lax.Precision.HIGHEST


def rotate(x, axis, shift):
    size = lax.axis_size(axis)
    return lax.ppermute(x, axis, [(i, (i + shift) % size) for i in range(size)])


def exchange(even_pairs, odd_pairs, axis):
    size = lax.axis_size(axis)
    inner = [(i, i) for i in (0, size - 1)]
    for i in range(1, size - 1, 2):
        inner += [(i, i + 1), (i + 1, i)]
    outer = [(i, i ^ 1) for i in range(size)]
    return lax.ppermute(even_pairs, axis, outer), lax.ppermute(odd_pairs, axis, inner)


def shifted(v, step, dim):
    size = v.shape[dim]
    return pltpu.roll(v, step % size, dim)


def dot(a, b):
    return lax.dot_general(
        a, b, (((1,), (0,)), ((), ())), precision=EXACT, preferred_element_type=jnp.float32
    )


def iota(shape, dim):
    return lax.broadcasted_iota(jnp.int32, shape, dim)


def total(tile):
    return jnp.sum(jnp.sum(tile, axis=1, keepdims=True), axis=0, keepdims=True)


def fold(plane):
    rows, lanes = plane.shape
    parts = [
        plane[r : r + 8, c : c + 128] for r in range(0, rows, 8) for c in range(0, lanes, 128)
    ]
    out = parts[0]
    for part in parts[1:]:
        out = out + part
    return out


def z_pairs(lanes):
    half = lanes // 2
    return (iota((lanes, half), 0) // 2 == iota((lanes, half), 1)).astype(jnp.float32)


def z_copies(lanes):
    return (iota((lanes, 2 * lanes), 0) == iota((lanes, 2 * lanes), 1) // 2).astype(jnp.float32)


def restrict_rows(planes, first_row, rows):
    extent = planes[0].shape[0]
    here = iota(planes[0].shape, 0)
    inside = (here >= first_row) & (here < first_row + rows)
    pick = (
        (iota((rows // 2, extent), 1) - first_row + 2) // 2 - 1 == iota((rows // 2, extent), 0)
    ).astype(jnp.float32)
    halves = []
    for x in range(0, len(planes), 2):
        pair = jnp.where(inside, planes[x] + planes[x + 1], 0.0)
        halves.append(dot(pick, pair))
    packed = dot(jnp.concatenate(halves, axis=0), z_pairs(planes[0].shape[1]))
    return packed.reshape(len(planes) // 2, rows // 2, packed.shape[1])


def swap_sum(v, dim, stride):
    even = (iota(v.shape, dim) // stride) % 2 == 0
    return v + jnp.where(even, shifted(v, -stride, dim), shifted(v, stride, dim))


def off_diagonal(v, low, high, fx, fx_high, fy, fz, step):
    out = fy * shifted(v, step, 0) + shifted(fy * v, -step, 0)
    out = out + (fz * shifted(v, step, 1) + shifted(fz * v, -step, 1))
    if low is not None:
        out = out + fx * low
    if high is not None:
        out = out + fx_high * high
    return out


def coefficients(planes, scale, step, x_mask, y_mask, z_mask, outside):
    count = len(planes)
    faces = [None] * count
    for x in range(count):
        low = planes[x] if x == 0 else planes[x - 1]
        faces[x] = (scale * x_mask(x)) * (0.5 * (planes[x] + low))
    out = []
    for x in range(count):
        k = planes[x]
        fy = (scale * y_mask) * (0.5 * (k + shifted(k, step, 0)))
        fz = (scale * z_mask) * (0.5 * (k + shifted(k, step, 1)))
        diag = (scale * outside(x)) * k + fy + shifted(fy, -step, 0) + fz + shifted(fz, -step, 1)
        diag = diag + faces[x]
        if x + 1 < count:
            diag = diag + faces[x + 1]
        out.append((faces[x], fy, fz, DAMPING / diag))
    return out


def flag(condition):
    return jnp.where(condition, 1.0, 0.0).astype(jnp.float32)


def place_blocks(refs, place, sizes, planes, rows, put):
    size_x, size_y = sizes
    for s in range(size_x):
        at_x = lax.rem(place[0] - s + size_x, size_x)
        for t in range(size_y):
            at_y = lax.rem(place[1] - t + size_y, size_y)
            put(at_x, at_y, refs[s], t)


def placed_whole(refs, place, sizes, planes, per, whole_ref):
    block_rows = whole_ref.shape[1] // sizes[1]

    def put(at_x, at_y, ref, t):
        row = pl.multiple_of(at_y * block_rows, block_rows)
        for x in range(planes):
            whole_ref[at_x * planes + x, pl.ds(row, block_rows), :] = ref[t * per + x]

    place_blocks(refs, place, sizes, planes, block_rows, put)


def summed_tiles(refs, sizes, per, index):
    tile = None
    for s in range(sizes[0]):
        for t in range(sizes[1]):
            part = refs[s][t * per + index]
            tile = part if tile is None else tile + part
    return tile


def halved(one, two):
    lower = iota(one.shape, 1) < one.shape[1] // 2
    middle = one.shape[1] // 2
    return jnp.where(lower, one + shifted(one, middle, 1), two + shifted(two, middle, 1))


def coarse_correction(source, mid, out, level1, level2):
    fx1, fy1, fz1, rd1 = level1
    fx2, fy2, fz2, rd2 = level2
    count = source.shape[0]

    def off1(ref, x):
        low = ref[x - 1] if x > 0 else None
        high = ref[x + 1] if x + 1 < count else None
        fx_high = fx1[x + 1] if x + 1 < count else None
        return off_diagonal(ref[x], low, high, fx1[x], fx_high, fy1[x], fz1[x], 1)

    for x in range(count):
        mid[x] = rd1[x] * source[x]
    coarse = []
    for x in range(0, count, 2):
        pair = KEPT * (source[x] + source[x + 1]) + (off1(mid, x) + off1(mid, x + 1))
        coarse.append(swap_sum(swap_sum(pair, 0, 1), 1, 1))
    half = count // 2
    iterate = [rd2[x] * coarse[x] for x in range(half)]
    for sweep in range(COARSE_SWEEPS - 1):
        new = []
        for x in range(half):
            low = iterate[x - 1] if x > 0 else None
            high = iterate[x + 1] if x + 1 < half else None
            fx_high = fx2[x + 1] if x + 1 < half else None
            off = off_diagonal(iterate[x], low, high, fx2[x], fx_high, fy2[x], fz2[x], 2)
            new.append(KEPT * iterate[x] + rd2[x] * (coarse[x] + off))
        iterate = new
    for x in range(count):
        mid[x] = mid[x] + iterate[x // 2]
    for x in range(count):
        out[x] = KEPT * mid[x] + rd1[x] * (source[x] + off1(mid, x))


def prolonged(whole_ref, place, planes, rows, pad):
    count, extent, lanes = whole_ref.shape
    own_x = planes - 2 * (pad // 2)
    own_y = (rows - 2 * pad) // 2
    first = place[1] * own_y - pad // 2
    pick = (iota((rows, extent), 1) == first + iota((rows, extent), 0) // 2).astype(jnp.float32)
    parts = []
    for x in range(planes):
        at = jnp.clip(place[0] * own_x - pad // 2 + x, 0, count - 1)
        parts.append(dot(pick, whole_ref[at]))
    wide = dot(jnp.concatenate(parts, axis=0), z_copies(lanes))
    return [wide[x * rows : (x + 1) * rows] for x in range(planes)]


def frame_masks(place, shape, pad, sizes):
    planes, rows, lanes = shape
    own_x, own_y = planes - 2 * pad, rows - 2 * pad
    all_x, all_y = own_x * sizes[0], own_y * sizes[1]
    base_x, base_y = place[0] * own_x - pad, place[1] * own_y - pad
    at_y = base_y + iota((rows, lanes), 0)
    at_z = iota((rows, lanes), 1)
    y_mask = flag((at_y >= 1) & (at_y < all_y))
    z_mask = flag(at_z >= 1)
    edges = flag(at_y == 0) + flag(at_y == all_y - 1) + flag(at_z == 0) + flag(at_z == lanes - 1)

    def x_mask(x):
        at = base_x + x
        return flag((at >= 1) & (at < all_x))

    def outside(x):
        at = base_x + x
        return edges + (flag(at == 0) + flag(at == all_x - 1))

    return x_mask, y_mask, z_mask, outside


def prior_rows(center, low, high, up, down, x_low, x_high, y_mask, z_mask, outside):
    rows, lanes = center.shape
    y_next = shifted(y_mask, -1, 0)
    z_next = shifted(z_mask, -1, 1)
    out = (PRIOR_MASS + outside) * center + x_low * (center - low) + x_high * (center - high)
    out = out + y_mask * (center - up) + y_next * (center - down)
    out = out + z_mask * (center - shifted(center, 1, 1))
    return out + z_next * (center - shifted(center, -1, 1))


def fine_restricted(base, fields, fx, fy, fz, out_ref, first, own):
    planes = []
    for x in range(first, first + own):
        off = off_diagonal(
            fields[x], fields[x - 1], fields[x + 1], fx[x], fx[x + 1], fy[x], fz[x], 1
        )
        planes.append(KEPT * base[x] + off)
    rows = planes[0].shape[0]
    coarse = restrict_rows(planes, first, rows - 2 * first)
    for x in range(coarse.shape[0]):
        out_ref[x] = coarse[x]


def sensitivity_planes(q, hux, huy, huz, nbu, first, last):
    faces = {x: hux[x] * (q(x) + q(x - 1)) for x in range(first, last + 1)}
    out = {}
    for x in range(first, last):
        mid = q(x)
        along_y = huy[x] * (mid + shifted(mid, 1, 0))
        along_z = huz[x] * (mid + shifted(mid, 1, 1))
        z = faces[x] - faces[x + 1] + nbu[x] * mid
        z = z + (along_y - shifted(along_y, -1, 0))
        out[x] = z + (along_z - shifted(along_z, -1, 1))
    return out


def first_residual_stage(z, fx, fy, fz, rd, z_ref, out_ref, planes):
    for x in z:
        z_ref[x] = z[x]
    iterate = {x: rd[x] * z[x] for x in range(HALO - 1, planes - HALO + 1)}
    fine_restricted(z, iterate, fx, fy, fz, out_ref, HALO, planes - 2 * HALO)


def call(kernel, outs, scratch, inputs, smem_first=True):
    vmem = pl.BlockSpec(memory_space=pltpu.VMEM)
    smem = pl.BlockSpec(memory_space=pltpu.SMEM)
    return pl.pallas_call(
        kernel,
        out_shape=[jax.ShapeDtypeStruct(shape, jnp.float32) for shape in outs],
        in_specs=[smem if smem_first and i == 0 else vmem for i in range(len(inputs))],
        out_specs=[vmem] * len(outs),
        scratch_shapes=[pltpu.VMEM(shape, jnp.float32) for shape in scratch],
        compiler_params=pltpu.CompilerParams(vmem_limit_bytes=VMEM_LIMIT),
    )(*inputs)


def prepare(place, sizes, fields, cells, precision):
    own_x, own_y, lanes = fields[0].shape
    number = len(fields)
    all_rows = own_y * sizes[1]
    depths = FIELD_DEPTHS

    def kernel(*refs):
        place = refs[0]
        fields = refs[1 : 1 + number]
        cells, precision = refs[1 + number : 3 + number]
        coarse_ref, weight_ref, even_ref, odd_ref = refs[3 + number :]
        cell = cells[...]
        column = lax.div(cell, lanes)
        at_z = cell - column * lanes
        at_x = lax.div(column, all_rows)
        at_y = column - at_x * all_rows
        row = (at_x - place[0] * own_x) * own_y + (at_y - place[1] * own_y)
        count = cell.shape[1]
        picks = flag(iota((own_x * own_y, count), 0) == row)
        values = jnp.where(iota((lanes, count), 0) == at_z, precision[...], 0.0)
        weight = lax.dot_general(
            picks, values, (((1,), (1,)), ((), ())),
            precision=EXACT, preferred_element_type=jnp.float32,
        )
        for x in range(own_x):
            weight_ref[x] = weight[x * own_y : (x + 1) * own_y]
        even = lax.rem(place[0], 2) == 0
        at = 0
        for index, depth in enumerate(depths):
            ref = weight_ref if index == number else fields[index]
            start = own_x - depth
            even_start = jnp.where(even, start, 0)
            odd_start = jnp.where(even, 0, start)
            for x in range(depth):
                even_ref[at + x] = ref[even_start + x]
                odd_ref[at + x] = ref[odd_start + x]
            at += depth
        planes = [jnp.exp(fields[2][x]) for x in range(own_x)]
        coarse = restrict_rows(planes, 0, own_y)
        for x in range(coarse.shape[0]):
            coarse_ref[x] = coarse[x] * 0.125

    edge = (sum(depths), own_y, lanes)
    return call(
        kernel,
        [(own_x // 2, own_y // 2, lanes // 2), fields[0].shape, edge, edge],
        [],
        [place] + list(fields) + [cells, precision],
    )


def gathered(own):
    size_x, size_y = lax.axis_size("gx"), lax.axis_size("gy")
    row = jnp.concatenate([own] + [rotate(own, "gy", t) for t in range(1, size_y)], axis=0)
    return [row] + [rotate(row, "gx", s) for s in range(1, size_x)]


FIELD_DEPTHS = (DEEP, HALO, HALO, HALO, WIDE)


def reach(depth, own_x, x):
    return depth - max(0, depth - x, x - depth - own_x + 1)


def setup_rows(own_x):
    starts, at = [], 0
    for depth in FIELD_DEPTHS:
        starts.append([])
        for x in range(own_x + 2 * depth):
            starts[-1].append(at)
            at += reach(depth, own_x, x)
    return starts, -(-at // 8) * 8


def field_plane(fields, even_edge, odd_edge, even, index, x):
    depth = FIELD_DEPTHS[index]
    start = sum(FIELD_DEPTHS[:index])
    own = fields[index].shape[0]
    if x < depth:
        return jnp.where(even, odd_edge[start + x], even_edge[start + x])
    if x < depth + own:
        return fields[index][x - depth]
    at = start + x - depth - own
    return jnp.where(even, even_edge[at], odd_edge[at])


def pack_setup_edges(place, fields, even_edge, odd_edge):
    own_x, own_y, lanes = fields[0].shape
    starts, rows = setup_rows(own_x)
    number = len(fields)

    def kernel(*refs):
        place = refs[0]
        fields = refs[1 : 1 + number]
        even_edge, odd_edge, even_ref, odd_ref = refs[1 + number :]
        even_x = lax.rem(place[0], 2) == 0
        even_y = lax.rem(place[1], 2) == 0
        for index, depth in enumerate(FIELD_DEPTHS):
            for x in range(own_x + 2 * depth):
                here = reach(depth, own_x, x)
                if here == 0:
                    continue
                plane = field_plane(fields, even_edge, odd_edge, even_x, index, x)
                at = starts[index][x]
                first, last = plane[:here], plane[own_y - here :]
                even_ref[at : at + here, :] = jnp.where(even_y, last, first)
                odd_ref[at : at + here, :] = jnp.where(even_y, first, last)

    inputs = [place] + list(fields) + [even_edge, odd_edge]
    return call(kernel, [(rows, lanes)] * 2, [], inputs)


def setup(place, sizes, fields, x_edges, y_edges):
    own_x, own_y, lanes = fields[0].shape
    frame = (own_x + 2 * HALO, own_y + 2 * HALO, lanes)
    starts, _ = setup_rows(own_x)
    number = len(fields)
    coarse = (own_x // 2, own_y // 2, lanes // 2)

    def kernel(*refs):
        place = refs[0]
        fields = refs[1 : 1 + number]
        even_edge, odd_edge, even_rows, odd_rows = refs[1 + number : 5 + number]
        even_x = lax.rem(place[0], 2) == 0
        even_y = lax.rem(place[1], 2) == 0
        outs = refs[5 + number : 18 + number]
        cond, hux, huy, huz, nbu, fx, fy, fz, rd, weight, source, z_out, b1 = outs
        prior = refs[18 + number]
        state = refs[19 + number]
        grad = refs[20 + number]

        def assemble(index, ref, x_skip, first_row):
            depth = FIELD_DEPTHS[index]
            for x in range(own_x + 2 * depth):
                here = reach(depth, own_x, x)
                at = starts[index][x]
                own_row = first_row + depth
                if here < depth or x_skip:
                    ref[x + x_skip] = jnp.zeros(ref.shape[1:], jnp.float32)
                ref[x + x_skip, own_row : own_row + own_y, :] = field_plane(
                    fields, even_edge, odd_edge, even_x, index, x
                )
                if here == 0:
                    continue
                even_part, odd_part = even_rows[at : at + here, :], odd_rows[at : at + here, :]
                ref[x + x_skip, own_row - here : own_row, :] = jnp.where(
                    even_y, odd_part, even_part
                )
                end = own_row + own_y
                ref[x + x_skip, end : end + here, :] = jnp.where(even_y, even_part, odd_part)

        zero = jnp.zeros(frame[1:], jnp.float32)
        for x in range(HALO - WIDE):
            weight[x] = zero
            weight[frame[0] - 1 - x] = zero
        assemble(0, prior, 0, 0)
        assemble(1, grad, 0, 0)
        assemble(2, cond, 0, 0)
        assemble(3, state, 0, 0)
        assemble(4, weight, HALO - WIDE, HALO - WIDE)
        x_mask, y_mask, z_mask, outside = frame_masks(place, frame, HALO, sizes)
        planes, rows = frame[:2]
        for x in range(planes):
            center = prior[x + 1, 1 : 1 + rows, :]
            value = prior_rows(
                center,
                prior[x, 1 : 1 + rows, :],
                prior[x + 2, 1 : 1 + rows, :],
                prior[x + 1, 0:rows, :],
                prior[x + 1, 2 : 2 + rows, :],
                x_mask(x),
                x_mask(x + 1),
                y_mask,
                z_mask,
                outside(x),
            )
            source[x] = value - grad[x]
        for x in range(planes):
            cond[x] = jnp.exp(cond[x])
        for x in range(planes):
            u = state[x]
            if x > 0:
                hux[x] = (0.5 * x_mask(x)) * (u - state[x - 1])
            else:
                hux[x] = zero
            huy[x] = (0.5 * y_mask) * (u - shifted(u, 1, 0))
            huz[x] = (0.5 * z_mask) * (u - shifted(u, 1, 1))
            nbu[x] = outside(x) * u
        found = coefficients(
            [cond[x] for x in range(planes)], 1.0, 1, x_mask, y_mask, z_mask, outside
        )
        for x in range(planes):
            fx[x], fy[x], fz[x], rd[x] = found[x]
        z = sensitivity_planes(
            lambda x: cond[x] * source[x], hux, huy, huz, nbu, 1, planes - 1
        )
        z_out[0] = zero
        z_out[planes - 1] = zero
        first_residual_stage(z, fx, fy, fz, rd, z_out, b1, planes)

    deep = (own_x + 2 * DEEP, -(-(own_y + 2 * DEEP) // 8) * 8, lanes)
    return call(
        kernel,
        [frame] * 12 + [coarse],
        [deep, frame, frame],
        [place] + list(fields) + list(x_edges) + list(y_edges),
    )


def coarse_setup(place, sizes, blocks, shape):
    planes, rows, lanes = shape
    whole = (planes * sizes[0], rows * sizes[1], lanes)
    half = (whole[0] // 2,) + whole[1:]

    def kernel(*refs):
        place = refs[0]
        blocks = refs[1 : 1 + sizes[0]]
        outs = refs[1 + sizes[0] : 9 + sizes[0]]
        cond = refs[9 + sizes[0]]
        placed_whole(blocks, place, sizes, planes, planes, cond)
        at_y = iota(whole[1:], 0)
        at_z = iota(whole[1:], 1)

        def level(values, scale, step, refs):
            count = len(values)
            y_mask = flag(at_y >= step)
            z_mask = flag(at_z >= step)
            edges = (
                flag(at_y < step)
                + flag(at_y >= whole[1] - step)
                + flag(at_z < step)
                + flag(at_z >= lanes - step)
            )

            def x_mask(x):
                return 1.0 if x > 0 else 0.0

            def outside(x):
                return edges + float((x == 0) + (x == count - 1))

            found = coefficients(values, scale, step, x_mask, y_mask, z_mask, outside)
            for x in range(count):
                for ref, value in zip(refs, found[x]):
                    ref[x] = value

        level([cond[x] for x in range(whole[0])], 2.0, 1, outs[:4])
        coarse = []
        for x in range(half[0]):
            pair = cond[2 * x] + cond[2 * x + 1]
            coarse.append(0.125 * swap_sum(swap_sum(pair, 0, 1), 1, 1))
        level(coarse, 4.0, 2, outs[4:])

    return call(kernel, [whole] * 4 + [half] * 4, [whole], [place] + list(blocks))


def middle(place, sizes, blocks, per, levels, fine, z, direction, weight, earlier):
    planes, rows, lanes = z.shape
    own_x = planes - 2 * HALO
    coarse = (own_x // 2, (rows - 2 * HALO) // 2, lanes // 2)
    whole = levels[0].shape
    first_time = earlier is None
    extra = [] if first_time else [earlier[0], earlier[1], earlier[2]]
    inputs = [place] + list(blocks) + list(levels) + list(fine) + [z, direction, weight] + extra

    def kernel(*refs):
        at = 0

        def take(number):
            nonlocal at
            at += number
            return refs[at - number : at]

        (place,) = take(1)
        blocks = take(sizes[0])
        levels = take(8)
        fx, fy, fz, rd = take(4)
        z, direction, weight = take(3)
        old = take(len(extra))
        b1, second, curved = take(3)
        if first_time:
            (kept,) = take(1)
            combined = direction
        else:
            combined, norm_ref = take(2)
        whole_source, whole_mid, whole_out, mid = take(4)
        frame_rows = iota((rows, lanes), 0)
        own_rows = flag((frame_rows >= HALO) & (frame_rows < rows - HALO))
        placed_whole(blocks, place, sizes, coarse[0], per, whole_source)
        coarse_correction(whole_source, whole_mid, whole_out, levels[:4], levels[4:])
        correction = prolonged(whole_out, place, planes // 2, rows, HALO)
        if first_time:
            ratio = None
        else:
            norm = total(summed_tiles(blocks, sizes, per, coarse[0]))
            ratio = norm / old[2][0:1, 0:1]
            for x in range(planes):
                combined[x] = direction[x] + ratio * old[1][x]
            norm_ref[...] = jnp.broadcast_to(norm, (8, 128))
        for x in range(1, planes - 1):
            mid[x] = rd[x] * z[x] + correction[x // 2]
        zero = jnp.zeros((rows, lanes), jnp.float32)
        forms = zero
        rights = {}
        for x in range(2, planes - 2):
            off = off_diagonal(mid[x], mid[x - 1], mid[x + 1], fx[x], fx[x + 1], fy[x], fz[x], 1)
            change = KEPT * mid[x] + rd[x] * (z[x] + off)
            if first_time:
                kept[x] = change
            else:
                change = change + ratio * old[0][x]
            right = weight[x] * change
            second[x] = right
            rights[x] = right
            if HALO <= x < planes - HALO:
                forms = forms + right * change
        for x in (0, 1, planes - 2, planes - 1):
            second[x] = zero
            if first_time:
                kept[x] = zero
        x_mask, y_mask, z_mask, outside = frame_masks(place, (planes, rows, lanes), HALO, sizes)
        squares = zero
        for x in range(HALO, planes - HALO):
            center = combined[x]
            value = prior_rows(
                center,
                combined[x - 1],
                combined[x + 1],
                shifted(center, 1, 0),
                shifted(center, -1, 0),
                x_mask(x),
                x_mask(x + 1),
                y_mask,
                z_mask,
                outside(x),
            )
            curved[x - HALO] = value
            forms = forms + center * value
            if first_time:
                squares = squares + center * center
        iterate = {x: rd[x] * rights[x] for x in range(HALO - 1, planes - HALO + 1)}
        fine_restricted(rights, iterate, fx, fy, fz, b1, HALO, own_x)
        tile = fold(jnp.where(own_rows > 0, forms, 0.0))
        if first_time:
            tile = halved(tile, fold(jnp.where(own_rows > 0, squares, 0.0)))
        b1[coarse[0]] = tile

    frame = (planes, rows, lanes)
    return call(
        kernel,
        [
            (coarse[0] + 1,) + coarse[1:],
            frame,
            (own_x, rows, lanes),
            frame,
        ]
        + ([] if first_time else [(8, 128)]),
        [whole, whole, whole, frame],
        inputs,
    )


def image_planes(levels, fine, place, sizes, blocks, per, second, curved, cond, faces, scratch):
    fx, fy, fz, rd = fine
    hux, huy, huz, nbu = faces
    whole_source, whole_mid, whole_out, mid = scratch
    planes, rows, lanes = second.shape
    placed_whole(blocks, place, sizes, (planes - 2 * HALO) // 2, per, whole_source)
    coarse_correction(whole_source, whole_mid, whole_out, levels[:4], levels[4:])
    correction = prolonged(whole_out, place, planes // 2, rows, HALO)
    for x in range(2, planes - 2):
        mid[x] = rd[x] * second[x] + correction[x // 2]
    adjoint = {}
    for x in range(3, planes - 3):
        off = off_diagonal(mid[x], mid[x - 1], mid[x + 1], fx[x], fx[x + 1], fy[x], fz[x], 1)
        adjoint[x] = KEPT * mid[x] + rd[x] * (second[x] + off)
    out = {}
    along_x = {
        x: hux[x] * (adjoint[x] - adjoint[x - 1]) for x in range(HALO, planes - HALO + 1)
    }
    for x in range(HALO, planes - HALO):
        p = adjoint[x]
        along_y = huy[x] * (p - shifted(p, 1, 0))
        along_z = huz[x] * (p - shifted(p, 1, 1))
        value = along_x[x] + along_x[x + 1] + nbu[x] * p
        value = value + (along_y + shifted(along_y, -1, 0))
        value = value + (along_z + shifted(along_z, -1, 1))
        out[x] = cond[x] * value + curved[x - HALO]
    return out


def end_first(place, sizes, blocks, per, levels, fine, second, curved, cond, faces, source):
    planes, rows, lanes = second.shape
    own_x, own_y = planes - 2 * HALO, rows - 2 * HALO
    whole = levels[0].shape
    coarse = own_x // 2
    inputs = (
        [place] + list(blocks) + list(levels) + list(fine)
        + [second, curved, cond] + list(faces) + [source]
    )

    def kernel(*refs):
        place = refs[0]
        n = sizes[0]
        blocks = refs[1 : 1 + n]
        levels = refs[1 + n : 9 + n]
        fine = refs[9 + n : 13 + n]
        second, curved, cond = refs[13 + n : 16 + n]
        faces = refs[16 + n : 20 + n]
        source = refs[20 + n]
        first_ref, last_ref, own_ref, tile_ref, norm_ref, step_ref = refs[21 + n : 27 + n]
        *scratch, hold = refs[27 + n : 32 + n]
        image = image_planes(
            levels, fine, place, sizes, blocks, per, second, curved, cond, faces, scratch
        )
        tile = summed_tiles(blocks, sizes, per, coarse)
        lower = iota(tile.shape, 1) < tile.shape[1] // 2
        form = total(jnp.where(lower, tile, 0.0))
        norm = total(jnp.where(lower, 0.0, tile))
        step = norm / form
        norm_ref[...] = jnp.broadcast_to(norm, (8, 128))
        step_ref[...] = jnp.broadcast_to(step, (8, 128))
        squares = jnp.zeros((own_y, lanes), jnp.float32)
        for x in range(HALO, planes - HALO):
            hold[x - HALO] = source[x] - step * image[x]
        for x in range(own_x):
            value = hold[x, HALO : HALO + own_y, :]
            squares = squares + value * value
            own_ref[x] = value
            if x < HALO:
                first_ref[x] = value
            if x >= own_x - HALO:
                last_ref[x - own_x + HALO] = value
        tile_ref[0] = fold(squares)

    strip = (HALO, own_y, lanes)
    return call(
        kernel,
        [strip, strip, (own_x, own_y, lanes), (1, 8, 128), (8, 128), (8, 128)],
        [whole, whole, whole, (planes, rows, lanes), (own_x, rows, lanes)],
        inputs,
    )


def end_second(
    place, sizes, blocks, per, levels, fine, second, curved, cond, faces,
    source, remaining, combined, norm, step
):
    planes, rows, lanes = second.shape
    own_x, own_y = planes - 2 * HALO, rows - 2 * HALO
    whole = levels[0].shape
    coarse = own_x // 2
    inputs = (
        [place] + list(blocks) + list(levels) + list(fine)
        + [second, curved, cond] + list(faces) + [source, remaining, combined, norm, step]
    )

    def kernel(*refs):
        place = refs[0]
        n = sizes[0]
        blocks = refs[1 : 1 + n]
        levels = refs[1 + n : 9 + n]
        fine = refs[9 + n : 13 + n]
        second, curved, cond = refs[13 + n : 16 + n]
        faces = refs[16 + n : 20 + n]
        source, remaining, combined, norm, step = refs[20 + n : 25 + n]
        step_out, residual_out = refs[25 + n : 27 + n]
        *scratch, hold, hold_step = refs[27 + n : 33 + n]
        image = image_planes(
            levels, fine, place, sizes, blocks, per, second, curved, cond, faces, scratch
        )
        form = total(summed_tiles(blocks, sizes, per, coarse))
        now = norm[0:1, 0:1] / form
        before = step[0:1, 0:1]
        for x in range(HALO, planes - HALO):
            hold[x - HALO] = now * image[x]
            hold_step[x - HALO] = before * source[x] + now * combined[x]
        for x in range(own_x):
            residual_out[x] = remaining[x] - hold[x, HALO : HALO + own_y, :]
            step_out[x] = hold_step[x, HALO : HALO + own_y, :]

    own = (own_x, own_y, lanes)
    hold = (own_x, rows, lanes)
    return call(
        kernel,
        [own, own],
        [whole, whole, whole, (planes, rows, lanes), hold, hold],
        inputs,
    )


def edge_rows(own_x):
    starts, at = [], 0
    for x in range(own_x + 2 * HALO):
        starts.append(at)
        at += reach(HALO, own_x, x)
    return starts, -(-at // 8) * 8


def pack_edges(own, low, high):
    own_x, own_y, lanes = own.shape
    planes = own_x + 2 * HALO
    starts, rows = edge_rows(own_x)

    def kernel(own, low, high, first_ref, last_ref):
        for x in range(planes):
            here = reach(HALO, own_x, x)
            if here == 0:
                continue
            if x < HALO:
                ref, at = low, x
            elif x < HALO + own_x:
                ref, at = own, x - HALO
            else:
                ref, at = high, x - HALO - own_x
            row = starts[x]
            first_ref[row : row + here, :] = ref[at, :here, :]
            last_ref[row : row + here, :] = ref[at, own_y - here :, :]

    return call(kernel, [(rows, lanes)] * 2, [], [own, low, high], smem_first=False)


def begin(own, low, high, before, after, tile, cond, faces, fine):
    own_x, own_y, lanes = own.shape
    planes, rows = own_x + 2 * HALO, own_y + 2 * HALO
    frame = (planes, rows, lanes)
    coarse = (own_x // 2, own_y // 2, lanes // 2)
    starts, _ = edge_rows(own_x)

    def kernel(
        own, low, high, before, after, tile, cond, hux, huy, huz, nbu, fx, fy, fz, rd,
        direction, z_out, b1,
    ):
        for x in range(planes):
            if x < HALO:
                value = low[x]
            elif x < HALO + own_x:
                value = own[x - HALO]
            else:
                value = high[x - HALO - own_x]
            here = reach(HALO, own_x, x)
            if here < HALO:
                direction[x] = jnp.zeros((rows, lanes), jnp.float32)
            direction[x, HALO : HALO + own_y, :] = value
            if here:
                row = starts[x]
                direction[x, HALO - here : HALO, :] = before[row : row + here, :]
                end = HALO + own_y
                direction[x, end : end + here, :] = after[row : row + here, :]
        z = sensitivity_planes(
            lambda x: cond[x] * direction[x], hux, huy, huz, nbu, 1, planes - 1
        )
        zero = jnp.zeros((rows, lanes), jnp.float32)
        z_out[0] = zero
        z_out[planes - 1] = zero
        first_residual_stage(z, fx, fy, fz, rd, z_out, b1, planes)
        b1[coarse[0]] = tile[0]

    return call(
        kernel,
        [frame, frame, (coarse[0] + 1,) + coarse[1:]],
        [],
        [own, low, high, before, after, tile, cond] + list(faces) + list(fine),
        smem_first=False,
    )


def on_device(log_conductivity, state, gradient, prior_sample, sensor_cells, noise_precision):
    sizes = (lax.axis_size("gx"), lax.axis_size("gy"))
    place_x = lax.axis_index("gx")
    place_y = lax.axis_index("gy")
    place = jnp.stack([place_x, place_y]).astype(jnp.int32)
    cells_x, cells_y, cells_z = log_conductivity.shape
    coarse = (cells_x // 2, cells_y // 2, cells_z // 2)

    fields = (prior_sample, gradient, log_conductivity, state)
    own_cond, weight, *x_edges = prepare(
        place, sizes, fields, sensor_cells[None], noise_precision[None]
    )
    fields = fields + (weight,)
    x_edges = exchange(*x_edges, "gx")
    cond_blocks = gathered(own_cond)
    y_edges = exchange(*pack_setup_edges(place, fields, *x_edges), "gy")
    (cond, hux, huy, huz, nbu, fx, fy, fz, rd, weight, source, z, b1) = setup(
        place, sizes, fields, x_edges, y_edges
    )
    faces = (hux, huy, huz, nbu)
    fine = (fx, fy, fz, rd)
    levels = coarse_setup(place, sizes, cond_blocks, coarse)

    b1, second, curved, kept = middle(
        place, sizes, gathered(b1), coarse[0], levels, fine, z, source, weight, None
    )
    first, last, remaining, tile, norm, step = end_first(
        place, sizes, gathered(b1), coarse[0] + 1, levels, fine, second, curved, cond, faces,
        source,
    )
    low, high = rotate(last, "gx", 1), rotate(first, "gx", -1)
    first, last = pack_edges(remaining, low, high)
    before, after = rotate(last, "gy", 1), rotate(first, "gy", -1)
    direction, z, b1 = begin(remaining, low, high, before, after, tile, cond, faces, fine)
    b1, second, curved, combined, norm = middle(
        place, sizes, gathered(b1), coarse[0] + 1, levels, fine, z, direction, weight,
        (kept, source, norm),
    )
    return tuple(
        end_second(
            place, sizes, gathered(b1), coarse[0] + 1, levels, fine, second, curved, cond,
            faces, source, remaining, combined, norm, step,
        )
    )


def solution(mesh):
    field = P(("ens", "gx"), "gy", None)
    sensors = P(("ens", "gx", "gy"))
    return jax.shard_map(
        on_device,
        mesh=mesh,
        in_specs=(field, field, field, field, sensors, sensors),
        out_specs=(field, field),
        check_vma=False,
    )
```

```python
import jax
import jax.numpy as jnp
from jax import lax
from jax.experimental import pallas as pl
from jax.experimental.pallas import tpu as pltpu
from jax.sharding import PartitionSpec as P

DAMPING = 0.8
KEPT = 0.2
PRIOR_MASS = 0.5
COARSE_SWEEPS = 6
HALO = 4
DEEP = 5
WIDE = 2
VMEM_LIMIT = 24 * 1024 * 1024
PREPARE_LIMIT = 65_600_000
EXACT = lax.Precision.HIGHEST


def rotate(x, axis, shift):
    size = lax.axis_size(axis)
    return lax.ppermute(x, axis, [(i, (i + shift) % size) for i in range(size)])


def exchange(even_pairs, odd_pairs, axis):
    size = lax.axis_size(axis)
    inner = [(i, i) for i in (0, size - 1)]
    for i in range(1, size - 1, 2):
        inner += [(i, i + 1), (i + 1, i)]
    outer = [(i, i ^ 1) for i in range(size)]
    return lax.ppermute(even_pairs, axis, outer), lax.ppermute(odd_pairs, axis, inner)


def here():
    return lax.axis_index("gx"), lax.axis_index("gy")


def shifted(v, step, dim):
    size = v.shape[dim]
    return pltpu.roll(v, step % size, dim)


def dot(a, b):
    return lax.dot_general(
        a, b, (((1,), (0,)), ((), ())), precision=EXACT, preferred_element_type=jnp.float32
    )


def iota(shape, dim):
    return lax.broadcasted_iota(jnp.int32, shape, dim)


def total(tile):
    return jnp.sum(jnp.sum(tile, axis=1, keepdims=True), axis=0, keepdims=True)


def fold(plane):
    rows, lanes = plane.shape
    parts = [
        plane[r : r + 8, c : c + 128] for r in range(0, rows, 8) for c in range(0, lanes, 128)
    ]
    out = parts[0]
    for part in parts[1:]:
        out = out + part
    return out


def z_pairs(lanes):
    half = lanes // 2
    return (iota((lanes, half), 0) // 2 == iota((lanes, half), 1)).astype(jnp.float32)


def z_copies(lanes):
    return (iota((lanes, 2 * lanes), 0) == iota((lanes, 2 * lanes), 1) // 2).astype(jnp.float32)


def restrict_rows(planes, first_row, rows):
    extent = planes[0].shape[0]
    here = iota(planes[0].shape, 0)
    inside = (here >= first_row) & (here < first_row + rows)
    pick = (
        (iota((rows // 2, extent), 1) - first_row + 2) // 2 - 1 == iota((rows // 2, extent), 0)
    ).astype(jnp.float32)
    halves = []
    for x in range(0, len(planes), 2):
        pair = jnp.where(inside, planes[x] + planes[x + 1], 0.0)
        halves.append(dot(pick, pair))
    packed = dot(jnp.concatenate(halves, axis=0), z_pairs(planes[0].shape[1]))
    return packed.reshape(len(planes) // 2, rows // 2, packed.shape[1])


def swap_sum(v, dim, stride):
    even = (iota(v.shape, dim) // stride) % 2 == 0
    return v + jnp.where(even, shifted(v, -stride, dim), shifted(v, stride, dim))


def off_diagonal(v, low, high, fx, fx_high, fy, fz, step=1):
    out = fy * shifted(v, 1, 0) + shifted(fy * v, -1, 0)
    out = out + (fz * shifted(v, step, 1) + shifted(fz * v, -step, 1))
    if low is not None:
        out = out + fx * low
    if high is not None:
        out = out + fx_high * high
    return out


def coefficients(planes, scale, step, x_mask, y_mask, z_mask, outside):
    count = len(planes)
    faces = [None] * count
    for x in range(count):
        low = planes[x] if x == 0 else planes[x - 1]
        faces[x] = (scale * x_mask(x)) * (0.5 * (planes[x] + low))
    out = []
    for x in range(count):
        k = planes[x]
        fy = (scale * y_mask) * (0.5 * (k + shifted(k, 1, 0)))
        fz = (scale * z_mask) * (0.5 * (k + shifted(k, step, 1)))
        diag = (scale * outside(x)) * k + fy + shifted(fy, -1, 0) + fz + shifted(fz, -step, 1)
        diag = diag + faces[x]
        if x + 1 < count:
            diag = diag + faces[x + 1]
        out.append((faces[x], fy, fz, DAMPING / diag))
    return out


def flag(condition):
    return jnp.where(condition, 1.0, 0.0).astype(jnp.float32)


def placed_whole(refs, place, sizes, shape, per, first, whole_ref):
    planes, block_rows, _ = shape
    for s in range(sizes[0]):
        at_x = lax.rem(place[0] - s + sizes[0], sizes[0]) * planes
        for t in range(sizes[1]):
            at_y = lax.rem(place[1] - t + sizes[1], sizes[1])
            row = pl.multiple_of(at_y * block_rows, block_rows)
            for x in range(planes):
                block = refs[s][t * per + first + x]
                whole_ref[at_x + x, pl.ds(row, block_rows), :] = block


def summed_tiles(refs, sizes, per, index):
    tile = None
    for s in range(sizes[0]):
        for t in range(sizes[1]):
            part = refs[s][t * per + index]
            tile = part if tile is None else tile + part
    return tile


def halved(one, two):
    lower = iota(one.shape, 1) < one.shape[1] // 2
    middle = one.shape[1] // 2
    return jnp.where(lower, one + shifted(one, middle, 1), two + shifted(two, middle, 1))


def row_pairs(ref, x, rows):
    return ref[x, pl.ds(0, rows // 2, stride=2), :] + ref[x, pl.ds(1, rows // 2, stride=2), :]


def coarse_correction(place, own, source, mid, pairs, level1, level2):
    fx1, fy1, fz1, rd1 = level1
    fx2, fy2, fz2, rd2 = level2
    planes, own_rows, lanes = own
    count = source.shape[0]
    rows = source.shape[1] - own_rows
    half = count // 2
    blank = jnp.zeros((own_rows, lanes), jnp.float32)
    for x in range(count):
        source[x, rows:, :] = blank
        mid[x, rows:, :] = blank
        mid[x, :rows, :] = rd1[x, :rows, :] * source[x, :rows, :]

    def off1(x):
        low = mid[x - 1, :rows, :] if x > 0 else None
        high = mid[x + 1, :rows, :] if x + 1 < count else None
        fx_high = fx1[x + 1, :rows, :] if x + 1 < count else None
        return off_diagonal(
            mid[x, :rows, :], low, high, fx1[x, :rows, :], fx_high,
            fy1[x, :rows, :], fz1[x, :rows, :],
        )

    for x in range(half):
        pair = KEPT * (source[2 * x, :rows, :] + source[2 * x + 1, :rows, :])
        pairs[x, :rows, :] = swap_sum(pair + (off1(2 * x) + off1(2 * x + 1)), 1, 1)
    coarse = [row_pairs(pairs, x, rows) for x in range(half)]
    iterate = [rd2[x] * coarse[x] for x in range(half)]
    for sweep in range(COARSE_SWEEPS - 1):
        new = []
        for x in range(half):
            low = iterate[x - 1] if x > 0 else None
            high = iterate[x + 1] if x + 1 < half else None
            fx_high = fx2[x + 1] if x + 1 < half else None
            off = off_diagonal(iterate[x], low, high, fx2[x], fx_high, fy2[x], fz2[x], 2)
            new.append(KEPT * iterate[x] + rd2[x] * (coarse[x] + off))
        iterate = new
    for x in range(half):
        pairs[x, rows:, :] = blank
        pairs[x, pl.ds(0, rows // 2, stride=2), :] = iterate[x]
        pairs[x, pl.ds(1, rows // 2, stride=2), :] = iterate[x]

    start = jnp.clip((place[1] - 1) * own_rows, 0, max(rows - 2 * own_rows, 0))
    window = pl.ds(pl.multiple_of(start, own_rows), min(3 * own_rows, rows + own_rows))
    ends = HALO // 2
    at = [
        jnp.clip(place[0] * planes - ends + x, 0, count - 1) for x in range(-1, planes + 2 * ends + 1)
    ]
    value = [mid[a, window, :] + pairs[lax.div(a, 2), window, :] for a in at]
    first = place[1] * own_rows - ends - start
    frame_rows = 2 * (own_rows + 2 * ends)
    extent = value[0].shape[0]
    pick = flag(
        iota((frame_rows, extent), 1) == first + iota((frame_rows, extent), 0) // 2
    )
    parts = []
    for x in range(1, len(at) - 1):
        a = at[x]
        off = off_diagonal(
            value[x], value[x - 1], value[x + 1], fx1[a, window, :], fx1[a + 1, window, :],
            fy1[a, window, :], fz1[a, window, :],
        )
        smooth = KEPT * value[x] + rd1[a, window, :] * (source[a, window, :] + off)
        parts.append(dot(pick, smooth))
    wide = dot(jnp.concatenate(parts, axis=0), z_copies(lanes))
    return [wide[x * frame_rows : (x + 1) * frame_rows] for x in range(len(parts))]


def coarse_scratch(own, sizes):
    whole = (own[0] * sizes[0], own[1] * (sizes[1] + 1), own[2])
    return [whole, whole, (whole[0] // 2,) + whole[1:]]


def frame_masks(place, shape, pad, sizes):
    planes, rows, lanes = shape
    own_x, own_y = planes - 2 * pad, rows - 2 * pad
    all_x, all_y = own_x * sizes[0], own_y * sizes[1]
    base_x, base_y = place[0] * own_x - pad, place[1] * own_y - pad
    at_y = base_y + iota((rows, lanes), 0)
    at_z = iota((rows, lanes), 1)
    y_mask = flag((at_y >= 1) & (at_y < all_y))
    z_mask = flag(at_z >= 1)
    edges = flag(at_y == 0) + flag(at_y == all_y - 1) + flag(at_z == 0) + flag(at_z == lanes - 1)

    def x_mask(x):
        at = base_x + x
        return flag((at >= 1) & (at < all_x))

    def outside(x):
        at = base_x + x
        return edges + (flag(at == 0) + flag(at == all_x - 1))

    return x_mask, y_mask, z_mask, outside


def prior_rows(center, low, high, up, down, x_low, x_high, y_mask, z_mask, outside):
    rows, lanes = center.shape
    y_next = shifted(y_mask, -1, 0)
    z_next = shifted(z_mask, -1, 1)
    out = (PRIOR_MASS + outside) * center + x_low * (center - low) + x_high * (center - high)
    out = out + y_mask * (center - up) + y_next * (center - down)
    out = out + z_mask * (center - shifted(center, 1, 1))
    return out + z_next * (center - shifted(center, -1, 1))


def fine_restricted(base, fields, fx, fy, fz, out_ref, first, own):
    planes = []
    for x in range(first, first + own):
        off = off_diagonal(
            fields[x], fields[x - 1], fields[x + 1], fx[x], fx[x + 1], fy[x], fz[x]
        )
        planes.append(KEPT * base[x] + off)
    rows = planes[0].shape[0]
    coarse = restrict_rows(planes, first, rows - 2 * first)
    for x in range(coarse.shape[0]):
        out_ref[x] = coarse[x]


def sensitivity_planes(q, hux, huy, huz, nbu, first, last):
    faces = {x: hux[x] * (q(x) + q(x - 1)) for x in range(first, last + 1)}
    out = {}
    for x in range(first, last):
        mid = q(x)
        along_y = huy[x] * (mid + shifted(mid, 1, 0))
        along_z = huz[x] * (mid + shifted(mid, 1, 1))
        z = faces[x] - faces[x + 1] + nbu[x] * mid
        z = z + (along_y - shifted(along_y, -1, 0))
        out[x] = z + (along_z - shifted(along_z, -1, 1))
    return out


def first_residual_stage(z, fx, fy, fz, rd, z_ref, out_ref, planes):
    for x in z:
        z_ref[x] = z[x]
    iterate = {x: rd[x] * z[x] for x in range(HALO - 1, planes - HALO + 1)}
    fine_restricted(z, iterate, fx, fy, fz, out_ref, HALO, planes - 2 * HALO)


def call(kernel, outs, scratch, inputs, limit=VMEM_LIMIT, cost=None):
    vmem = pl.BlockSpec(memory_space=pltpu.VMEM)
    return pl.pallas_call(
        kernel,
        out_shape=[jax.ShapeDtypeStruct(shape, jnp.float32) for shape in outs],
        in_specs=[vmem] * len(inputs),
        out_specs=[vmem] * len(outs),
        scratch_shapes=[pltpu.VMEM(shape, jnp.float32) for shape in scratch],
        compiler_params=pltpu.CompilerParams(vmem_limit_bytes=limit),
        cost_estimate=cost,
    )(*inputs)


def prepare(sizes, fields, cells, precision):
    own_x, own_y, lanes = fields[0].shape
    number = len(fields)
    all_rows = own_y * sizes[1]
    depths = FIELD_DEPTHS

    def kernel(*refs):
        place = here()
        fields = refs[:number]
        cells, precision = refs[number : 2 + number]
        coarse_ref, weight_ref, even_ref, odd_ref = refs[2 + number :]
        cell = cells[...]
        column = lax.div(cell, lanes)
        at_z = cell - column * lanes
        at_x = lax.div(column, all_rows)
        at_y = column - at_x * all_rows
        row = (at_x - place[0] * own_x) * own_y + (at_y - place[1] * own_y)
        count = cell.shape[1]
        picks = flag(iota((own_x * own_y, count), 0) == row)
        values = jnp.where(iota((lanes, count), 0) == at_z, precision[...], 0.0)
        weight = lax.dot_general(
            picks, values, (((1,), (1,)), ((), ())),
            precision=EXACT, preferred_element_type=jnp.float32,
        )
        for x in range(own_x):
            weight_ref[x] = weight[x * own_y : (x + 1) * own_y]
        even = lax.rem(place[0], 2) == 0
        at = 0
        for index, depth in enumerate(depths):
            ref = weight_ref if index == number else fields[index]
            start = own_x - depth
            even_start = jnp.where(even, start, 0)
            odd_start = jnp.where(even, 0, start)
            for x in range(depth):
                even_ref[at + x] = ref[even_start + x]
                odd_ref[at + x] = ref[odd_start + x]
            at += depth
        planes = [jnp.exp(fields[2][x]) for x in range(own_x)]
        coarse = restrict_rows(planes, 0, own_y)
        for x in range(coarse.shape[0]):
            coarse_ref[x] = coarse[x] * 0.125

    edge = (sum(depths), own_y, lanes)
    return call(
        kernel,
        [(own_x // 2, own_y // 2, lanes // 2), fields[0].shape, edge, edge],
        [],
        list(fields) + [cells, precision],
        limit=PREPARE_LIMIT,
    )


def gathered(own):
    size_x, size_y = lax.axis_size("gx"), lax.axis_size("gy")
    row = jnp.concatenate([own] + [rotate(own, "gy", t) for t in range(1, size_y)], axis=0)
    return [row] + [rotate(row, "gx", s) for s in range(1, size_x)]


FIELD_DEPTHS = (DEEP, HALO, HALO, HALO, WIDE)


def reach(depth, own_x, x):
    return depth - max(0, depth - x, x - depth - own_x + 1)


def setup_rows(own_x):
    starts, at = [], 0
    for depth in FIELD_DEPTHS:
        starts.append([])
        for x in range(own_x + 2 * depth):
            starts[-1].append(at)
            at += reach(depth, own_x, x)
    return starts, -(-at // 8) * 8


def field_plane(fields, even_edge, odd_edge, even, index, x):
    depth = FIELD_DEPTHS[index]
    start = sum(FIELD_DEPTHS[:index])
    own = fields[index].shape[0]
    if x < depth:
        return jnp.where(even, odd_edge[start + x], even_edge[start + x])
    if x < depth + own:
        return fields[index][x - depth]
    at = start + x - depth - own
    return jnp.where(even, even_edge[at], odd_edge[at])


def pack_setup_edges(fields, even_edge, odd_edge):
    own_x, own_y, lanes = fields[0].shape
    starts, rows = setup_rows(own_x)
    number = len(fields)

    def kernel(*refs):
        place = here()
        fields = refs[:number]
        even_edge, odd_edge, even_ref, odd_ref = refs[number:]
        even_x = lax.rem(place[0], 2) == 0
        even_y = lax.rem(place[1], 2) == 0
        for index, depth in enumerate(FIELD_DEPTHS):
            for x in range(own_x + 2 * depth):
                near = reach(depth, own_x, x)
                if near == 0:
                    continue
                plane = field_plane(fields, even_edge, odd_edge, even_x, index, x)
                at = starts[index][x]
                first, last = plane[:near], plane[own_y - near :]
                even_ref[at : at + near, :] = jnp.where(even_y, last, first)
                odd_ref[at : at + near, :] = jnp.where(even_y, first, last)

    inputs = list(fields) + [even_edge, odd_edge]
    return call(kernel, [(rows, lanes)] * 2, [], inputs)


def setup(sizes, fields, x_edges, y_edges, own_cond):
    own_x, own_y, lanes = fields[0].shape
    frame = (own_x + 2 * HALO, own_y + 2 * HALO, lanes)
    starts, _ = setup_rows(own_x)
    number = len(fields)
    coarse = (own_x // 2, own_y // 2, lanes // 2)

    def kernel(*refs):
        place = here()
        fields = refs[:number]
        even_edge, odd_edge, even_rows, odd_rows, own_cond = refs[number : 5 + number]
        even_x = lax.rem(place[0], 2) == 0
        even_y = lax.rem(place[1], 2) == 0
        outs = refs[5 + number : 18 + number]
        cond, hux, huy, huz, nbu, fx, fy, fz, rd, weight, source, z_out, b1 = outs
        prior = refs[18 + number]
        state = refs[19 + number]
        grad = refs[20 + number]

        def assemble(index, ref, x_skip, first_row):
            depth = FIELD_DEPTHS[index]
            for x in range(own_x + 2 * depth):
                near = reach(depth, own_x, x)
                at = starts[index][x]
                own_row = first_row + depth
                if near < depth or x_skip:
                    ref[x + x_skip] = jnp.zeros(ref.shape[1:], jnp.float32)
                ref[x + x_skip, own_row : own_row + own_y, :] = field_plane(
                    fields, even_edge, odd_edge, even_x, index, x
                )
                if near == 0:
                    continue
                even_part, odd_part = even_rows[at : at + near, :], odd_rows[at : at + near, :]
                ref[x + x_skip, own_row - near : own_row, :] = jnp.where(
                    even_y, odd_part, even_part
                )
                end = own_row + own_y
                ref[x + x_skip, end : end + near, :] = jnp.where(even_y, even_part, odd_part)

        zero = jnp.zeros(frame[1:], jnp.float32)
        for x in range(HALO - WIDE):
            weight[x] = zero
            weight[frame[0] - 1 - x] = zero
        assemble(0, prior, 0, 0)
        assemble(1, grad, 0, 0)
        assemble(2, cond, 0, 0)
        assemble(3, state, 0, 0)
        assemble(4, weight, HALO - WIDE, HALO - WIDE)
        x_mask, y_mask, z_mask, outside = frame_masks(place, frame, HALO, sizes)
        planes, rows = frame[:2]
        for x in range(planes):
            center = prior[x + 1, 1 : 1 + rows, :]
            value = prior_rows(
                center,
                prior[x, 1 : 1 + rows, :],
                prior[x + 2, 1 : 1 + rows, :],
                prior[x + 1, 0:rows, :],
                prior[x + 1, 2 : 2 + rows, :],
                x_mask(x),
                x_mask(x + 1),
                y_mask,
                z_mask,
                outside(x),
            )
            source[x] = value - grad[x]
        for x in range(planes):
            cond[x] = jnp.exp(cond[x])
        for x in range(planes):
            u = state[x]
            if x > 0:
                hux[x] = (0.5 * x_mask(x)) * (u - state[x - 1])
            else:
                hux[x] = zero
            huy[x] = (0.5 * y_mask) * (u - shifted(u, 1, 0))
            huz[x] = (0.5 * z_mask) * (u - shifted(u, 1, 1))
            nbu[x] = outside(x) * u
        found = coefficients(
            [cond[x] for x in range(planes)], 1.0, 1, x_mask, y_mask, z_mask, outside
        )
        for x in range(planes):
            fx[x], fy[x], fz[x], rd[x] = found[x]
        z = sensitivity_planes(
            lambda x: cond[x] * source[x], hux, huy, huz, nbu, 1, planes - 1
        )
        z_out[0] = zero
        z_out[planes - 1] = zero
        first_residual_stage(z, fx, fy, fz, rd, z_out, b1, planes)
        for x in range(coarse[0]):
            b1[coarse[0] + x] = own_cond[x]

    deep = (own_x + 2 * DEEP, -(-(own_y + 2 * DEEP) // 8) * 8, lanes)
    return call(
        kernel,
        [frame] * 12 + [(2 * coarse[0],) + coarse[1:]],
        [deep, frame, frame],
        list(fields) + list(x_edges) + list(y_edges) + [own_cond],
    )


def coarse_setup(sizes, blocks, shape):
    planes, own_rows, lanes = shape
    count, rows = planes * sizes[0], own_rows * sizes[1]
    half = count // 2

    def kernel(*refs):
        blocks = refs[: sizes[0]]
        outs = refs[sizes[0] : 8 + sizes[0]]
        cond, pairs = refs[8 + sizes[0] :]
        placed_whole(blocks, here(), sizes, shape, 2 * planes, planes, cond)

        def level(values, scale, step, refs):
            number, extent = len(values), values[0].shape[0]
            at_y = iota((extent, lanes), 0)
            at_z = iota((extent, lanes), 1)
            edges = (
                flag(at_y == 0) + flag(at_y == extent - 1)
                + flag(at_z < step) + flag(at_z >= lanes - step)
            )

            def x_mask(x):
                return 1.0 if x > 0 else 0.0

            def outside(x):
                return edges + float((x == 0) + (x == number - 1))

            found = coefficients(
                values, scale, step, x_mask, flag(at_y >= 1), flag(at_z >= step), outside
            )
            for x in range(number):
                for ref, value in zip(refs, found[x]):
                    ref[x, :extent, :] = value

        level([cond[x] for x in range(count)], 2.0, 1, outs[:4])
        blank = jnp.zeros((own_rows, lanes), jnp.float32)
        for x in range(count):
            for ref in outs[:4]:
                ref[x, rows:, :] = blank
        outs[0][count] = jnp.zeros((rows + own_rows, lanes), jnp.float32)
        for x in range(half):
            pairs[x] = swap_sum(cond[2 * x] + cond[2 * x + 1], 1, 1)
        coarse = [0.125 * row_pairs(pairs, x, rows) for x in range(half)]
        level(coarse, 4.0, 2, outs[4:])

    padded = (count, rows + own_rows, lanes)
    return call(
        kernel,
        [(count + 1,) + padded[1:]] + [padded] * 3 + [(half, rows // 2, lanes)] * 4,
        [(count, rows, lanes), (half, rows, lanes)],
        list(blocks),
    )


def prior_part(sizes, direction):
    planes, rows, lanes = direction.shape

    def kernel(direction, out_ref):
        x_mask, y_mask, z_mask, outside = frame_masks(here(), direction.shape, HALO, sizes)
        for x in range(HALO, planes - HALO):
            center = direction[x]
            out_ref[x - HALO] = prior_rows(
                center,
                direction[x - 1],
                direction[x + 1],
                shifted(center, 1, 0),
                shifted(center, -1, 0),
                x_mask(x),
                x_mask(x + 1),
                y_mask,
                z_mask,
                outside(x),
            )

    size = planes * rows * lanes
    return call(
        kernel, [(planes - 2 * HALO, rows, lanes)], [], [direction],
        cost=pl.CostEstimate(flops=20 * size, bytes_accessed=8 * size, transcendentals=0),
    )[0]


def middle(sizes, blocks, per, levels, fine, z, direction, curved, weight, earlier):
    planes, rows, lanes = z.shape
    own_x = planes - 2 * HALO
    coarse = (own_x // 2, (rows - 2 * HALO) // 2, lanes // 2)
    first_time = earlier is None
    extra = [] if first_time else list(earlier)
    inputs = list(blocks) + list(levels) + list(fine) + [z, direction, curved, weight] + extra

    def kernel(*refs):
        at = 0

        def take(number):
            nonlocal at
            at += number
            return refs[at - number : at]

        place = here()
        blocks = take(sizes[0])
        levels = take(8)
        fx, fy, fz, rd = take(4)
        z, direction, curved, weight = take(4)
        old = take(len(extra))
        b1, second = take(2)
        if first_time:
            (kept,) = take(1)
        else:
            combined, curved_out, norm_ref = take(3)
        source, whole_mid, pairs, mid = take(4)
        frame_rows = iota((rows, lanes), 0)
        own_rows = (frame_rows >= HALO) & (frame_rows < rows - HALO)
        placed_whole(blocks, place, sizes, coarse, per, 0, source)
        correction = coarse_correction(
            place, coarse, source, whole_mid, pairs, levels[:4], levels[4:]
        )
        zero = jnp.zeros((rows, lanes), jnp.float32)
        forms = zero
        squares = zero
        if first_time:
            for x in range(own_x):
                d = direction[x + HALO]
                forms = forms + d * curved[x]
                squares = squares + d * d
        else:
            norm = total(summed_tiles(blocks, sizes, per, coarse[0]))
            ratio = norm / old[2][0:1, 0:1]
            for x in range(own_x):
                d = direction[x + HALO] + ratio * old[1][x + HALO]
                image = curved[x] + ratio * old[3][x]
                combined[x] = d
                curved_out[x] = image
                forms = forms + d * image
            norm_ref[...] = jnp.broadcast_to(norm, (8, 128))
        for x in range(1, planes - 1):
            mid[x] = rd[x] * z[x] + correction[x // 2]
        rights = {}
        for x in range(2, planes - 2):
            off = off_diagonal(mid[x], mid[x - 1], mid[x + 1], fx[x], fx[x + 1], fy[x], fz[x])
            change = KEPT * mid[x] + rd[x] * (z[x] + off)
            if first_time:
                kept[x] = change
            else:
                change = change + ratio * old[0][x]
            right = weight[x] * change
            second[x] = right
            rights[x] = right
            if HALO <= x < planes - HALO:
                forms = forms + right * change
        for x in (0, 1, planes - 2, planes - 1):
            second[x] = zero
            if first_time:
                kept[x] = zero
        iterate = {x: rd[x] * rights[x] for x in range(HALO - 1, planes - HALO + 1)}
        fine_restricted(rights, iterate, fx, fy, fz, b1, HALO, own_x)
        tile = fold(jnp.where(own_rows, forms, 0.0))
        if first_time:
            tile = halved(tile, fold(jnp.where(own_rows, squares, 0.0)))
        b1[coarse[0]] = tile

    frame = (planes, rows, lanes)
    own = (own_x, rows, lanes)
    return call(
        kernel,
        [(coarse[0] + 1,) + coarse[1:], frame] + ([frame] if first_time else [own, own, (8, 128)]),
        coarse_scratch(coarse, sizes) + [frame],
        inputs,
    )


def image_planes(levels, fine, sizes, blocks, per, second, curved, cond, faces, scratch):
    fx, fy, fz, rd = fine
    hux, huy, huz, nbu = faces
    source, whole_mid, pairs, mid = scratch
    place = here()
    planes, rows, lanes = second.shape
    own = ((planes - 2 * HALO) // 2, (rows - 2 * HALO) // 2, lanes // 2)
    placed_whole(blocks, place, sizes, own, per, 0, source)
    correction = coarse_correction(
        place, own, source, whole_mid, pairs, levels[:4], levels[4:]
    )
    for x in range(2, planes - 2):
        mid[x] = rd[x] * second[x] + correction[x // 2]
    adjoint = {}
    for x in range(3, planes - 3):
        off = off_diagonal(mid[x], mid[x - 1], mid[x + 1], fx[x], fx[x + 1], fy[x], fz[x])
        adjoint[x] = KEPT * mid[x] + rd[x] * (second[x] + off)
    out = {}
    along_x = {
        x: hux[x] * (adjoint[x] - adjoint[x - 1]) for x in range(HALO, planes - HALO + 1)
    }
    for x in range(HALO, planes - HALO):
        p = adjoint[x]
        along_y = huy[x] * (p - shifted(p, 1, 0))
        along_z = huz[x] * (p - shifted(p, 1, 1))
        value = along_x[x] + along_x[x + 1] + nbu[x] * p
        value = value + (along_y + shifted(along_y, -1, 0))
        value = value + (along_z + shifted(along_z, -1, 1))
        out[x] = cond[x] * value + curved[x - HALO]
    return out


def end_first(sizes, blocks, per, levels, fine, second, curved, cond, faces, source):
    planes, rows, lanes = second.shape
    own_x, own_y = planes - 2 * HALO, rows - 2 * HALO
    coarse = own_x // 2
    scratch_shapes = coarse_scratch((coarse, own_y // 2, lanes // 2), sizes)
    inputs = (
        list(blocks) + list(levels) + list(fine)
        + [second, curved, cond] + list(faces) + [source]
    )

    def kernel(*refs):
        n = sizes[0]
        blocks = refs[:n]
        levels = refs[n : 8 + n]
        fine = refs[8 + n : 12 + n]
        second, curved, cond = refs[12 + n : 15 + n]
        faces = refs[15 + n : 19 + n]
        source = refs[19 + n]
        first_ref, last_ref, own_ref, tile_ref, norm_ref, step_ref = refs[20 + n : 26 + n]
        *scratch, hold = refs[26 + n :]
        image = image_planes(
            levels, fine, sizes, blocks, per, second, curved, cond, faces, scratch
        )
        tile = summed_tiles(blocks, sizes, per, coarse)
        lower = iota(tile.shape, 1) < tile.shape[1] // 2
        form = total(jnp.where(lower, tile, 0.0))
        norm = total(jnp.where(lower, 0.0, tile))
        step = norm / form
        norm_ref[...] = jnp.broadcast_to(norm, (8, 128))
        step_ref[...] = jnp.broadcast_to(step, (8, 128))
        squares = jnp.zeros((own_y, lanes), jnp.float32)
        for x in range(HALO, planes - HALO):
            hold[x - HALO] = source[x] - step * image[x]
        for x in range(own_x):
            value = hold[x, HALO : HALO + own_y, :]
            squares = squares + value * value
            own_ref[x] = value
            if x < HALO:
                first_ref[x] = value
            if x >= own_x - HALO:
                last_ref[x - own_x + HALO] = value
        tile_ref[0] = fold(squares)

    strip = (HALO, own_y, lanes)
    return call(
        kernel,
        [strip, strip, (own_x, own_y, lanes), (1, 8, 128), (8, 128), (8, 128)],
        scratch_shapes + [(planes, rows, lanes), (own_x, rows, lanes)],
        inputs,
    )


def end_second(
    sizes, blocks, per, levels, fine, second, curved, cond, faces,
    source, remaining, combined, norm, step
):
    planes, rows, lanes = second.shape
    own_x, own_y = planes - 2 * HALO, rows - 2 * HALO
    coarse = own_x // 2
    scratch_shapes = coarse_scratch((coarse, own_y // 2, lanes // 2), sizes)
    inputs = (
        list(blocks) + list(levels) + list(fine)
        + [second, curved, cond] + list(faces) + [source, remaining, combined, norm, step]
    )

    def kernel(*refs):
        n = sizes[0]
        blocks = refs[:n]
        levels = refs[n : 8 + n]
        fine = refs[8 + n : 12 + n]
        second, curved, cond = refs[12 + n : 15 + n]
        faces = refs[15 + n : 19 + n]
        source, remaining, combined, norm, step = refs[19 + n : 24 + n]
        step_out, residual_out = refs[24 + n : 26 + n]
        *scratch, hold, hold_step = refs[26 + n :]
        image = image_planes(
            levels, fine, sizes, blocks, per, second, curved, cond, faces, scratch
        )
        form = total(summed_tiles(blocks, sizes, per, coarse))
        now = norm[0:1, 0:1] / form
        before = step[0:1, 0:1]
        for x in range(HALO, planes - HALO):
            hold[x - HALO] = now * image[x]
            hold_step[x - HALO] = before * source[x] + now * combined[x - HALO]
        for x in range(own_x):
            residual_out[x] = remaining[x] - hold[x, HALO : HALO + own_y, :]
            step_out[x] = hold_step[x, HALO : HALO + own_y, :]

    own = (own_x, own_y, lanes)
    hold = (own_x, rows, lanes)
    return call(
        kernel,
        [own, own],
        scratch_shapes + [(planes, rows, lanes), hold, hold],
        inputs,
    )


def edge_rows(own_x):
    starts, at = [], 0
    for x in range(own_x + 2 * HALO):
        starts.append(at)
        at += reach(HALO, own_x, x)
    return starts, -(-at // 8) * 8


def pack_edges(own, low, high):
    own_x, own_y, lanes = own.shape
    planes = own_x + 2 * HALO
    starts, rows = edge_rows(own_x)

    def kernel(own, low, high, first_ref, last_ref):
        for x in range(planes):
            near = reach(HALO, own_x, x)
            if near == 0:
                continue
            if x < HALO:
                ref, at = low, x
            elif x < HALO + own_x:
                ref, at = own, x - HALO
            else:
                ref, at = high, x - HALO - own_x
            row = starts[x]
            first_ref[row : row + near, :] = ref[at, :near, :]
            last_ref[row : row + near, :] = ref[at, own_y - near :, :]

    return call(kernel, [(rows, lanes)] * 2, [], [own, low, high])


def begin(own, low, high, before, after, tile, cond, faces, fine):
    own_x, own_y, lanes = own.shape
    planes, rows = own_x + 2 * HALO, own_y + 2 * HALO
    frame = (planes, rows, lanes)
    coarse = (own_x // 2, own_y // 2, lanes // 2)
    starts, _ = edge_rows(own_x)

    def kernel(
        own, low, high, before, after, tile, cond, hux, huy, huz, nbu, fx, fy, fz, rd,
        direction, z_out, b1,
    ):
        for x in range(planes):
            if x < HALO:
                value = low[x]
            elif x < HALO + own_x:
                value = own[x - HALO]
            else:
                value = high[x - HALO - own_x]
            near = reach(HALO, own_x, x)
            if near < HALO:
                direction[x] = jnp.zeros((rows, lanes), jnp.float32)
            direction[x, HALO : HALO + own_y, :] = value
            if near:
                row = starts[x]
                direction[x, HALO - near : HALO, :] = before[row : row + near, :]
                end = HALO + own_y
                direction[x, end : end + near, :] = after[row : row + near, :]
        z = sensitivity_planes(
            lambda x: cond[x] * direction[x], hux, huy, huz, nbu, 1, planes - 1
        )
        zero = jnp.zeros((rows, lanes), jnp.float32)
        z_out[0] = zero
        z_out[planes - 1] = zero
        first_residual_stage(z, fx, fy, fz, rd, z_out, b1, planes)
        b1[coarse[0]] = tile[0]

    return call(
        kernel,
        [frame, frame, (coarse[0] + 1,) + coarse[1:]],
        [],
        [own, low, high, before, after, tile, cond] + list(faces) + list(fine),
    )


def on_device(log_conductivity, state, gradient, prior_sample, sensor_cells, noise_precision):
    sizes = (lax.axis_size("gx"), lax.axis_size("gy"))
    cells_x, cells_y, cells_z = log_conductivity.shape
    coarse = (cells_x // 2, cells_y // 2, cells_z // 2)
    per = coarse[0] + 1

    fields = (prior_sample, gradient, log_conductivity, state)
    own_cond, weight, *x_edges = prepare(
        sizes, fields, sensor_cells[None], noise_precision[None]
    )
    fields = fields + (weight,)
    x_edges = exchange(*x_edges, "gx")
    y_edges = exchange(*pack_setup_edges(fields, *x_edges), "gy")
    (cond, hux, huy, huz, nbu, fx, fy, fz, rd, weight, source, z, b1) = setup(
        sizes, fields, x_edges, y_edges, own_cond
    )
    faces = (hux, huy, huz, nbu)
    fine = (fx, fy, fz, rd)

    blocks = gathered(b1)
    curved = prior_part(sizes, source)
    levels = coarse_setup(sizes, blocks, coarse)
    b1, second, kept = middle(
        sizes, blocks, 2 * coarse[0], levels, fine, z, source, curved, weight, None
    )
    first, last, remaining, tile, norm, step = end_first(
        sizes, gathered(b1), per, levels, fine, second, curved, cond, faces, source
    )
    low, high = rotate(last, "gx", 1), rotate(first, "gx", -1)
    first, last = pack_edges(remaining, low, high)
    before, after = rotate(last, "gy", 1), rotate(first, "gy", -1)
    direction, z, b1 = begin(remaining, low, high, before, after, tile, cond, faces, fine)
    blocks = gathered(b1)
    b1, second, combined, curved, norm = middle(
        sizes, blocks, per, levels, fine, z, direction, prior_part(sizes, direction), weight,
        (kept, source, norm, curved),
    )
    return tuple(
        end_second(
            sizes, gathered(b1), per, levels, fine, second, curved, cond,
            faces, source, remaining, combined, norm, step,
        )
    )


def solution(mesh):
    field = P(("ens", "gx"), "gy", None)
    sensors = P(("ens", "gx", "gy"))
    return jax.shard_map(
        on_device,
        mesh=mesh,
        in_specs=(field, field, field, field, sensors, sensors),
        out_specs=(field, field),
        check_vma=False,
    )
```

```python
import jax
import jax.numpy as jnp
from jax import lax
from jax.experimental import pallas as pl
from jax.experimental.pallas import tpu as pltpu
from jax.sharding import PartitionSpec as P

DAMPING = 0.8
KEPT = 0.2
PRIOR_MASS = 0.5
COARSE_SWEEPS = 6
HALO = 4
DEEP = 5
WIDE = 2
VMEM_LIMIT = 24 * 1024 * 1024
PREPARE_LIMIT = 65_600_000
EXACT = lax.Precision.HIGHEST


def rotate(x, axis, shift):
    size = lax.axis_size(axis)
    return lax.ppermute(x, axis, [(i, (i + shift) % size) for i in range(size)])


def exchange(even_pairs, odd_pairs, axis):
    size = lax.axis_size(axis)
    inner = [(i, i) for i in (0, size - 1)]
    for i in range(1, size - 1, 2):
        inner += [(i, i + 1), (i + 1, i)]
    outer = [(i, i ^ 1) for i in range(size)]
    return lax.ppermute(even_pairs, axis, outer), lax.ppermute(odd_pairs, axis, inner)


def here():
    return lax.axis_index("gx"), lax.axis_index("gy")


def shifted(v, step, dim):
    size = v.shape[dim]
    return pltpu.roll(v, step % size, dim)


def dot(a, b):
    return lax.dot_general(
        a, b, (((1,), (0,)), ((), ())), precision=EXACT, preferred_element_type=jnp.float32
    )


def iota(shape, dim):
    return lax.broadcasted_iota(jnp.int32, shape, dim)


def total(tile):
    return jnp.sum(jnp.sum(tile, axis=1, keepdims=True), axis=0, keepdims=True)


def fold(plane):
    rows, lanes = plane.shape
    parts = [
        plane[r : r + 8, c : c + 128] for r in range(0, rows, 8) for c in range(0, lanes, 128)
    ]
    out = parts[0]
    for part in parts[1:]:
        out = out + part
    return out


def z_pairs(lanes):
    half = lanes // 2
    return (iota((lanes, half), 0) // 2 == iota((lanes, half), 1)).astype(jnp.float32)


def z_copies(lanes):
    return (iota((lanes, 2 * lanes), 0) == iota((lanes, 2 * lanes), 1) // 2).astype(jnp.float32)


def restrict_rows(planes, first_row, rows):
    extent = planes[0].shape[0]
    here = iota(planes[0].shape, 0)
    inside = (here >= first_row) & (here < first_row + rows)
    pick = (
        (iota((rows // 2, extent), 1) - first_row + 2) // 2 - 1 == iota((rows // 2, extent), 0)
    ).astype(jnp.float32)
    halves = []
    for x in range(0, len(planes), 2):
        pair = jnp.where(inside, planes[x] + planes[x + 1], 0.0)
        halves.append(dot(pick, pair))
    packed = dot(jnp.concatenate(halves, axis=0), z_pairs(planes[0].shape[1]))
    return packed.reshape(len(planes) // 2, rows // 2, packed.shape[1])


def swap_sum(v, dim, stride):
    even = (iota(v.shape, dim) // stride) % 2 == 0
    return v + jnp.where(even, shifted(v, -stride, dim), shifted(v, stride, dim))


def off_diagonal(v, low, high, fx, fx_high, fy, fz, step=1):
    out = fy * shifted(v, 1, 0) + shifted(fy * v, -1, 0)
    out = out + (fz * shifted(v, step, 1) + shifted(fz * v, -step, 1))
    if low is not None:
        out = out + fx * low
    if high is not None:
        out = out + fx_high * high
    return out


def coefficients(planes, scale, step, x_mask, y_mask, z_mask, outside):
    count = len(planes)
    faces = [None] * count
    for x in range(count):
        low = planes[x] if x == 0 else planes[x - 1]
        faces[x] = (scale * x_mask(x)) * (0.5 * (planes[x] + low))
    out = []
    for x in range(count):
        k = planes[x]
        fy = (scale * y_mask) * (0.5 * (k + shifted(k, 1, 0)))
        fz = (scale * z_mask) * (0.5 * (k + shifted(k, step, 1)))
        diag = (scale * outside(x)) * k + fy + shifted(fy, -1, 0) + fz + shifted(fz, -step, 1)
        diag = diag + faces[x]
        if x + 1 < count:
            diag = diag + faces[x + 1]
        out.append((faces[x], fy, fz, DAMPING / diag))
    return out


def flag(condition):
    return jnp.where(condition, 1.0, 0.0).astype(jnp.float32)


def placed_whole(refs, place, sizes, shape, per, first, whole_ref):
    planes, block_rows, _ = shape
    for s in range(sizes[0]):
        at_x = lax.rem(place[0] - s + sizes[0], sizes[0]) * planes
        for t in range(sizes[1]):
            at_y = lax.rem(place[1] - t + sizes[1], sizes[1])
            row = pl.multiple_of(at_y * block_rows, block_rows)
            for x in range(planes):
                block = refs[s][t * per + first + x]
                whole_ref[at_x + x, pl.ds(row, block_rows), :] = block


def placed_overlapping(refs, place, sizes, shape, per, room, whole_ref):
    planes, block_rows, lanes = shape
    sub = iota((block_rows, lanes), 0)
    last, first = sub == block_rows - 1, sub == 0

    def spots():
        for s in range(sizes[0]):
            at_x = lax.rem(place[0] - s + sizes[0], sizes[0]) * planes
            for t in range(sizes[1]):
                at_y = lax.rem(place[1] - t + sizes[1], sizes[1])
                row = pl.multiple_of(at_y * block_rows, block_rows)
                yield refs[s], t * per, at_x, row

    for ref, tile, at_x, row in spots():
        for x in range(planes):
            room[at_x + x + 1, pl.ds(row + block_rows, block_rows), :] = ref[tile + x]
    for ref, tile, at_x, row in spots():
        adds = [(0, 1, ref[tile + planes]), (planes + 1, 1, ref[tile + planes + 1])]
        pairs = [(x + 1, ref[tile + planes + 2], 2 * x) for x in range(planes)]
        pairs += [(0, ref[tile + planes + 3], 0), (planes + 1, ref[tile + planes + 3], 2)]
        for x, borders, at in pairs:
            before = shifted(borders, block_rows - 1 - at, 0)
            after = shifted(borders, -(at + 1), 0)
            adds.append((x, 0, jnp.where(last, before, 0.0)))
            adds.append((x, 2, jnp.where(first, after, 0.0)))
        spans = [
            (at_x + x, pl.ds(row + step * block_rows, block_rows)) for x, step, _ in adds
        ]
        values = [room[x, span, :] + add for (x, span), (_, _, add) in zip(spans, adds)]
        for (x, span), value in zip(spans, values):
            room[x, span, :] = value
    rows = block_rows * sizes[1]
    for x in range(planes * sizes[0]):
        whole_ref[x, :rows, :] = room[x + 1, block_rows : block_rows + rows, :]


def summed_tiles(refs, sizes, per, index):
    tile = None
    for s in range(sizes[0]):
        for t in range(sizes[1]):
            part = refs[s][t * per + index]
            tile = part if tile is None else tile + part
    return tile


def halved(one, two):
    lower = iota(one.shape, 1) < one.shape[1] // 2
    middle = one.shape[1] // 2
    return jnp.where(lower, one + shifted(one, middle, 1), two + shifted(two, middle, 1))


def row_pairs(ref, x, rows):
    return ref[x, pl.ds(0, rows // 2, stride=2), :] + ref[x, pl.ds(1, rows // 2, stride=2), :]


def coarse_correction(place, own, source, mid, pairs, level1, level2):
    fx1, fy1, fz1, rd1 = level1
    fx2, fy2, fz2, rd2 = level2
    planes, own_rows, lanes = own
    count = source.shape[0]
    rows = source.shape[1] - own_rows
    half = count // 2
    blank = jnp.zeros((own_rows, lanes), jnp.float32)
    for x in range(count):
        source[x, rows:, :] = blank
        mid[x, rows:, :] = blank
        mid[x, :rows, :] = rd1[x, :rows, :] * source[x, :rows, :]

    def off1(x):
        low = mid[x - 1, :rows, :] if x > 0 else None
        high = mid[x + 1, :rows, :] if x + 1 < count else None
        fx_high = fx1[x + 1, :rows, :] if x + 1 < count else None
        return off_diagonal(
            mid[x, :rows, :], low, high, fx1[x, :rows, :], fx_high,
            fy1[x, :rows, :], fz1[x, :rows, :],
        )

    for x in range(half):
        pair = KEPT * (source[2 * x, :rows, :] + source[2 * x + 1, :rows, :])
        pairs[x, :rows, :] = swap_sum(pair + (off1(2 * x) + off1(2 * x + 1)), 1, 1)
    coarse = [row_pairs(pairs, x, rows) for x in range(half)]
    iterate = [rd2[x] * coarse[x] for x in range(half)]
    for sweep in range(COARSE_SWEEPS - 1):
        new = []
        for x in range(half):
            low = iterate[x - 1] if x > 0 else None
            high = iterate[x + 1] if x + 1 < half else None
            fx_high = fx2[x + 1] if x + 1 < half else None
            off = off_diagonal(iterate[x], low, high, fx2[x], fx_high, fy2[x], fz2[x], 2)
            new.append(KEPT * iterate[x] + rd2[x] * (coarse[x] + off))
        iterate = new
    for x in range(half):
        pairs[x, rows:, :] = blank
        pairs[x, pl.ds(0, rows // 2, stride=2), :] = iterate[x]
        pairs[x, pl.ds(1, rows // 2, stride=2), :] = iterate[x]

    start = jnp.clip((place[1] - 1) * own_rows, 0, max(rows - 2 * own_rows, 0))
    window = pl.ds(pl.multiple_of(start, own_rows), min(3 * own_rows, rows + own_rows))
    ends = HALO // 2
    at = [
        jnp.clip(place[0] * planes - ends + x, 0, count - 1) for x in range(-1, planes + 2 * ends + 1)
    ]
    value = [mid[a, window, :] + pairs[lax.div(a, 2), window, :] for a in at]
    first = place[1] * own_rows - ends - start
    frame_rows = 2 * (own_rows + 2 * ends)
    extent = value[0].shape[0]
    pick = flag(
        iota((frame_rows, extent), 1) == first + iota((frame_rows, extent), 0) // 2
    )
    parts = []
    for x in range(1, len(at) - 1):
        a = at[x]
        off = off_diagonal(
            value[x], value[x - 1], value[x + 1], fx1[a, window, :], fx1[a + 1, window, :],
            fy1[a, window, :], fz1[a, window, :],
        )
        smooth = KEPT * value[x] + rd1[a, window, :] * (source[a, window, :] + off)
        parts.append(dot(pick, smooth))
    wide = dot(jnp.concatenate(parts, axis=0), z_copies(lanes))
    return [wide[x * frame_rows : (x + 1) * frame_rows] for x in range(len(parts))]


def coarse_scratch(own, sizes):
    whole = (own[0] * sizes[0], own[1] * (sizes[1] + 1), own[2])
    return [whole, whole, (whole[0] // 2,) + whole[1:]]


def frame_masks(place, shape, pad, sizes):
    planes, rows, lanes = shape
    own_x, own_y = planes - 2 * pad, rows - 2 * pad
    all_x, all_y = own_x * sizes[0], own_y * sizes[1]
    base_x, base_y = place[0] * own_x - pad, place[1] * own_y - pad
    at_y = base_y + iota((rows, lanes), 0)
    at_z = iota((rows, lanes), 1)
    y_mask = flag((at_y >= 1) & (at_y < all_y))
    z_mask = flag(at_z >= 1)
    edges = flag(at_y == 0) + flag(at_y == all_y - 1) + flag(at_z == 0) + flag(at_z == lanes - 1)

    def x_mask(x):
        at = base_x + x
        return flag((at >= 1) & (at < all_x))

    def outside(x):
        at = base_x + x
        return edges + (flag(at == 0) + flag(at == all_x - 1))

    return x_mask, y_mask, z_mask, outside


def prior_rows(center, low, high, up, down, x_low, x_high, y_mask, z_mask, outside):
    rows, lanes = center.shape
    y_next = shifted(y_mask, -1, 0)
    z_next = shifted(z_mask, -1, 1)
    out = (PRIOR_MASS + outside) * center + x_low * (center - low) + x_high * (center - high)
    out = out + y_mask * (center - up) + y_next * (center - down)
    out = out + z_mask * (center - shifted(center, 1, 1))
    return out + z_next * (center - shifted(center, -1, 1))


def fine_restricted(base, fields, fx, fy, fz, out_ref, first, own):
    planes = []
    for x in range(first, first + own):
        off = off_diagonal(
            fields[x], fields[x - 1], fields[x + 1], fx[x], fx[x + 1], fy[x], fz[x]
        )
        planes.append(KEPT * base[x] + off)
    rows = planes[0].shape[0]
    coarse = restrict_rows(planes, first, rows - 2 * first)
    for x in range(coarse.shape[0]):
        out_ref[x] = coarse[x]


def sensitivity_planes(q, hux, huy, huz, nbu, first, last):
    faces = {x: hux[x] * (q(x) + q(x - 1)) for x in range(first, last + 1)}
    out = {}
    for x in range(first, last):
        mid = q(x)
        along_y = huy[x] * (mid + shifted(mid, 1, 0))
        along_z = huz[x] * (mid + shifted(mid, 1, 1))
        z = faces[x] - faces[x + 1] + nbu[x] * mid
        z = z + (along_y - shifted(along_y, -1, 0))
        out[x] = z + (along_z - shifted(along_z, -1, 1))
    return out


def first_residual_stage(z, fx, fy, fz, rd, z_ref, out_ref, planes):
    for x in z:
        z_ref[x] = z[x]
    iterate = {x: rd[x] * z[x] for x in range(HALO - 1, planes - HALO + 1)}
    fine_restricted(z, iterate, fx, fy, fz, out_ref, HALO, planes - 2 * HALO)


def call(kernel, outs, scratch, inputs, limit=VMEM_LIMIT, cost=None):
    vmem = pl.BlockSpec(memory_space=pltpu.VMEM)
    return pl.pallas_call(
        kernel,
        out_shape=[jax.ShapeDtypeStruct(shape, jnp.float32) for shape in outs],
        in_specs=[vmem] * len(inputs),
        out_specs=[vmem] * len(outs),
        scratch_shapes=[pltpu.VMEM(shape, jnp.float32) for shape in scratch],
        compiler_params=pltpu.CompilerParams(vmem_limit_bytes=limit),
        cost_estimate=cost,
    )(*inputs)


def prepare(sizes, fields, cells, precision):
    own_x, own_y, lanes = fields[0].shape
    number = len(fields)
    all_rows = own_y * sizes[1]
    depths = FIELD_DEPTHS

    def kernel(*refs):
        place = here()
        fields = refs[:number]
        cells, precision = refs[number : 2 + number]
        coarse_ref, weight_ref, even_ref, odd_ref = refs[2 + number :]
        cell = cells[...]
        column = lax.div(cell, lanes)
        at_z = cell - column * lanes
        at_x = lax.div(column, all_rows)
        at_y = column - at_x * all_rows
        row = (at_x - place[0] * own_x) * own_y + (at_y - place[1] * own_y)
        count = cell.shape[1]
        picks = flag(iota((own_x * own_y, count), 0) == row)
        values = jnp.where(iota((lanes, count), 0) == at_z, precision[...], 0.0)
        weight = lax.dot_general(
            picks, values, (((1,), (1,)), ((), ())),
            precision=EXACT, preferred_element_type=jnp.float32,
        )
        for x in range(own_x):
            weight_ref[x] = weight[x * own_y : (x + 1) * own_y]
        even = lax.rem(place[0], 2) == 0
        at = 0
        for index, depth in enumerate(depths):
            ref = weight_ref if index == number else fields[index]
            start = own_x - depth
            even_start = jnp.where(even, start, 0)
            odd_start = jnp.where(even, 0, start)
            for x in range(depth):
                even_ref[at + x] = ref[even_start + x]
                odd_ref[at + x] = ref[odd_start + x]
            at += depth
        planes = [jnp.exp(fields[2][x]) for x in range(own_x)]
        coarse = restrict_rows(planes, 0, own_y)
        for x in range(coarse.shape[0]):
            coarse_ref[x] = coarse[x] * 0.125

    edge = (sum(depths), own_y, lanes)
    return call(
        kernel,
        [(own_x // 2, own_y // 2, lanes // 2), fields[0].shape, edge, edge],
        [],
        list(fields) + [cells, precision],
        limit=PREPARE_LIMIT,
    )


def gathered_row(own):
    size = lax.axis_size("gy")
    return jnp.concatenate([own] + [rotate(own, "gy", t) for t in range(1, size)], axis=0)


def gathered_rows(row):
    return [row] + [rotate(row, "gx", s) for s in range(1, lax.axis_size("gx"))]


def gathered(own):
    return gathered_rows(gathered_row(own))


FIELD_DEPTHS = (DEEP, HALO, HALO, HALO, WIDE)


def reach(depth, own_x, x):
    return depth - max(0, depth - x, x - depth - own_x + 1)


def setup_rows(own_x):
    starts, at = [], 0
    for depth in FIELD_DEPTHS:
        starts.append([])
        for x in range(own_x + 2 * depth):
            starts[-1].append(at)
            at += reach(depth, own_x, x)
    return starts, -(-at // 8) * 8


def field_plane(fields, even_edge, odd_edge, even, index, x):
    depth = FIELD_DEPTHS[index]
    start = sum(FIELD_DEPTHS[:index])
    own = fields[index].shape[0]
    if x < depth:
        return jnp.where(even, odd_edge[start + x], even_edge[start + x])
    if x < depth + own:
        return fields[index][x - depth]
    at = start + x - depth - own
    return jnp.where(even, even_edge[at], odd_edge[at])


def pack_setup_edges(fields, even_edge, odd_edge):
    own_x, own_y, lanes = fields[0].shape
    starts, rows = setup_rows(own_x)
    number = len(fields)

    def kernel(*refs):
        place = here()
        fields = refs[:number]
        even_edge, odd_edge, even_ref, odd_ref = refs[number:]
        even_x = lax.rem(place[0], 2) == 0
        even_y = lax.rem(place[1], 2) == 0
        for index, depth in enumerate(FIELD_DEPTHS):
            for x in range(own_x + 2 * depth):
                near = reach(depth, own_x, x)
                if near == 0:
                    continue
                plane = field_plane(fields, even_edge, odd_edge, even_x, index, x)
                at = starts[index][x]
                first, last = plane[:near], plane[own_y - near :]
                even_ref[at : at + near, :] = jnp.where(even_y, last, first)
                odd_ref[at : at + near, :] = jnp.where(even_y, first, last)

    inputs = list(fields) + [even_edge, odd_edge]
    return call(kernel, [(rows, lanes)] * 2, [], inputs)


def setup(sizes, fields, x_edges, y_edges, own_cond):
    own_x, own_y, lanes = fields[0].shape
    frame = (own_x + 2 * HALO, own_y + 2 * HALO, lanes)
    starts, _ = setup_rows(own_x)
    number = len(fields)
    coarse = (own_x // 2, own_y // 2, lanes // 2)

    def kernel(*refs):
        place = here()
        fields = refs[:number]
        even_edge, odd_edge, even_rows, odd_rows, own_cond = refs[number : 5 + number]
        even_x = lax.rem(place[0], 2) == 0
        even_y = lax.rem(place[1], 2) == 0
        outs = refs[5 + number : 18 + number]
        cond, hux, huy, huz, nbu, fx, fy, fz, rd, weight, source, z_out, b1 = outs
        prior = refs[18 + number]
        state = refs[19 + number]
        grad = refs[20 + number]

        def assemble(index, ref, x_skip, first_row):
            depth = FIELD_DEPTHS[index]
            for x in range(own_x + 2 * depth):
                near = reach(depth, own_x, x)
                at = starts[index][x]
                own_row = first_row + depth
                if near < depth or x_skip:
                    ref[x + x_skip] = jnp.zeros(ref.shape[1:], jnp.float32)
                ref[x + x_skip, own_row : own_row + own_y, :] = field_plane(
                    fields, even_edge, odd_edge, even_x, index, x
                )
                if near == 0:
                    continue
                even_part, odd_part = even_rows[at : at + near, :], odd_rows[at : at + near, :]
                ref[x + x_skip, own_row - near : own_row, :] = jnp.where(
                    even_y, odd_part, even_part
                )
                end = own_row + own_y
                ref[x + x_skip, end : end + near, :] = jnp.where(even_y, even_part, odd_part)

        zero = jnp.zeros(frame[1:], jnp.float32)
        for x in range(HALO - WIDE):
            weight[x] = zero
            weight[frame[0] - 1 - x] = zero
        assemble(0, prior, 0, 0)
        assemble(1, grad, 0, 0)
        assemble(2, cond, 0, 0)
        assemble(3, state, 0, 0)
        assemble(4, weight, HALO - WIDE, HALO - WIDE)
        x_mask, y_mask, z_mask, outside = frame_masks(place, frame, HALO, sizes)
        planes, rows = frame[:2]
        for x in range(planes):
            center = prior[x + 1, 1 : 1 + rows, :]
            value = prior_rows(
                center,
                prior[x, 1 : 1 + rows, :],
                prior[x + 2, 1 : 1 + rows, :],
                prior[x + 1, 0:rows, :],
                prior[x + 1, 2 : 2 + rows, :],
                x_mask(x),
                x_mask(x + 1),
                y_mask,
                z_mask,
                outside(x),
            )
            source[x] = value - grad[x]
        for x in range(planes):
            cond[x] = jnp.exp(cond[x])
        for x in range(planes):
            u = state[x]
            if x > 0:
                hux[x] = (0.5 * x_mask(x)) * (u - state[x - 1])
            else:
                hux[x] = zero
            huy[x] = (0.5 * y_mask) * (u - shifted(u, 1, 0))
            huz[x] = (0.5 * z_mask) * (u - shifted(u, 1, 1))
            nbu[x] = outside(x) * u
        found = coefficients(
            [cond[x] for x in range(planes)], 1.0, 1, x_mask, y_mask, z_mask, outside
        )
        for x in range(planes):
            fx[x], fy[x], fz[x], rd[x] = found[x]
        z = sensitivity_planes(
            lambda x: cond[x] * source[x], hux, huy, huz, nbu, 1, planes - 1
        )
        z_out[0] = zero
        z_out[planes - 1] = zero
        first_residual_stage(z, fx, fy, fz, rd, z_out, b1, planes)
        for x in range(coarse[0]):
            b1[coarse[0] + x] = own_cond[x]

    deep = (own_x + 2 * DEEP, -(-(own_y + 2 * DEEP) // 8) * 8, lanes)
    return call(
        kernel,
        [frame] * 12 + [(2 * coarse[0],) + coarse[1:]],
        [deep, frame, frame],
        list(fields) + list(x_edges) + list(y_edges) + [own_cond],
    )


def coarse_setup(sizes, blocks, shape):
    planes, own_rows, lanes = shape
    count, rows = planes * sizes[0], own_rows * sizes[1]
    half = count // 2

    def kernel(*refs):
        blocks = refs[: sizes[0]]
        outs = refs[sizes[0] : 8 + sizes[0]]
        cond, pairs = refs[8 + sizes[0] :]
        placed_whole(blocks, here(), sizes, shape, 2 * planes, planes, cond)

        def level(values, scale, step, refs):
            number, extent = len(values), values[0].shape[0]
            at_y = iota((extent, lanes), 0)
            at_z = iota((extent, lanes), 1)
            edges = (
                flag(at_y == 0) + flag(at_y == extent - 1)
                + flag(at_z < step) + flag(at_z >= lanes - step)
            )

            def x_mask(x):
                return 1.0 if x > 0 else 0.0

            def outside(x):
                return edges + float((x == 0) + (x == number - 1))

            found = coefficients(
                values, scale, step, x_mask, flag(at_y >= 1), flag(at_z >= step), outside
            )
            for x in range(number):
                for ref, value in zip(refs, found[x]):
                    ref[x, :extent, :] = value

        level([cond[x] for x in range(count)], 2.0, 1, outs[:4])
        blank = jnp.zeros((own_rows, lanes), jnp.float32)
        for x in range(count):
            for ref in outs[:4]:
                ref[x, rows:, :] = blank
        outs[0][count] = jnp.zeros((rows + own_rows, lanes), jnp.float32)
        for x in range(half):
            pairs[x] = swap_sum(cond[2 * x] + cond[2 * x + 1], 1, 1)
        coarse = [0.125 * row_pairs(pairs, x, rows) for x in range(half)]
        level(coarse, 4.0, 2, outs[4:])

    padded = (count, rows + own_rows, lanes)
    return call(
        kernel,
        [(count + 1,) + padded[1:]] + [padded] * 3 + [(half, rows // 2, lanes)] * 4,
        [(count, rows, lanes), (half, rows, lanes)],
        list(blocks),
    )


def prior_part(sizes, direction):
    planes, rows, lanes = direction.shape

    def kernel(direction, out_ref):
        x_mask, y_mask, z_mask, outside = frame_masks(here(), direction.shape, HALO, sizes)
        for x in range(HALO, planes - HALO):
            center = direction[x]
            out_ref[x - HALO] = prior_rows(
                center,
                direction[x - 1],
                direction[x + 1],
                shifted(center, 1, 0),
                shifted(center, -1, 0),
                x_mask(x),
                x_mask(x + 1),
                y_mask,
                z_mask,
                outside(x),
            )

    size = planes * rows * lanes
    return call(
        kernel, [(planes - 2 * HALO, rows, lanes)], [], [direction],
        cost=pl.CostEstimate(flops=20 * size, bytes_accessed=8 * size, transcendentals=0),
    )[0]


def middle(sizes, blocks, per, levels, fine, z, direction, curved, weight, earlier):
    planes, rows, lanes = z.shape
    own_x = planes - 2 * HALO
    coarse = (own_x // 2, (rows - 2 * HALO) // 2, lanes // 2)
    first_time = earlier is None
    extra = [] if first_time else list(earlier)
    inputs = list(blocks) + list(levels) + list(fine) + [z, direction, curved, weight] + extra

    def kernel(*refs):
        at = 0

        def take(number):
            nonlocal at
            at += number
            return refs[at - number : at]

        place = here()
        blocks = take(sizes[0])
        levels = take(8)
        fx, fy, fz, rd = take(4)
        z, direction, curved, weight = take(4)
        old = take(len(extra))
        b1, second = take(2)
        if first_time:
            (kept,) = take(1)
        else:
            combined, curved_out, norm_ref = take(3)
        source, whole_mid, pairs, mid, *room = refs[at:]
        frame_rows = iota((rows, lanes), 0)
        own_rows = (frame_rows >= HALO) & (frame_rows < rows - HALO)
        if first_time:
            placed_whole(blocks, place, sizes, coarse, per, 0, source)
        else:
            placed_overlapping(blocks, place, sizes, coarse, per, room[0], source)
        correction = coarse_correction(
            place, coarse, source, whole_mid, pairs, levels[:4], levels[4:]
        )
        zero = jnp.zeros((rows, lanes), jnp.float32)
        forms = zero
        squares = zero
        if first_time:
            for x in range(own_x):
                d = direction[x + HALO]
                forms = forms + d * curved[x]
                squares = squares + d * d
        else:
            tile = summed_tiles(blocks, sizes, per, per - 1)
            norm = total(jnp.where(iota(tile.shape, 0) >= 4, tile, 0.0))
            ratio = norm / old[2][0:1, 0:1]
            for x in range(own_x):
                d = direction[x + HALO] + ratio * old[1][x + HALO]
                image = curved[x] + ratio * old[3][x]
                combined[x] = d
                curved_out[x] = image
                forms = forms + d * image
            norm_ref[...] = jnp.broadcast_to(norm, (8, 128))
        for x in range(1, planes - 1):
            mid[x] = rd[x] * z[x] + correction[x // 2]
        rights = {}
        for x in range(2, planes - 2):
            off = off_diagonal(mid[x], mid[x - 1], mid[x + 1], fx[x], fx[x + 1], fy[x], fz[x])
            change = KEPT * mid[x] + rd[x] * (z[x] + off)
            if first_time:
                kept[x] = change
            else:
                change = change + ratio * old[0][x]
            right = weight[x] * change
            second[x] = right
            rights[x] = right
            if HALO <= x < planes - HALO:
                forms = forms + right * change
        for x in (0, 1, planes - 2, planes - 1):
            second[x] = zero
            if first_time:
                kept[x] = zero
        iterate = {x: rd[x] * rights[x] for x in range(HALO - 1, planes - HALO + 1)}
        fine_restricted(rights, iterate, fx, fy, fz, b1, HALO, own_x)
        tile = fold(jnp.where(own_rows, forms, 0.0))
        if first_time:
            tile = halved(tile, fold(jnp.where(own_rows, squares, 0.0)))
        b1[coarse[0]] = tile

    frame = (planes, rows, lanes)
    own = (own_x, rows, lanes)
    margin = (coarse[0] * sizes[0] + 2, coarse[1] * (sizes[1] + 2), coarse[2])
    return call(
        kernel,
        [(coarse[0] + 1,) + coarse[1:], frame] + ([frame] if first_time else [own, own, (8, 128)]),
        coarse_scratch(coarse, sizes) + [frame] + ([] if first_time else [margin]),
        inputs,
    )


def image_planes(levels, fine, sizes, blocks, per, second, curved, cond, faces, scratch):
    fx, fy, fz, rd = fine
    hux, huy, huz, nbu = faces
    source, whole_mid, pairs, mid = scratch
    place = here()
    planes, rows, lanes = second.shape
    own = ((planes - 2 * HALO) // 2, (rows - 2 * HALO) // 2, lanes // 2)
    placed_whole(blocks, place, sizes, own, per, 0, source)
    correction = coarse_correction(
        place, own, source, whole_mid, pairs, levels[:4], levels[4:]
    )
    for x in range(2, planes - 2):
        mid[x] = rd[x] * second[x] + correction[x // 2]
    adjoint = {}
    for x in range(3, planes - 3):
        off = off_diagonal(mid[x], mid[x - 1], mid[x + 1], fx[x], fx[x + 1], fy[x], fz[x])
        adjoint[x] = KEPT * mid[x] + rd[x] * (second[x] + off)
    out = {}
    along_x = {
        x: hux[x] * (adjoint[x] - adjoint[x - 1]) for x in range(HALO, planes - HALO + 1)
    }
    for x in range(HALO, planes - HALO):
        p = adjoint[x]
        along_y = huy[x] * (p - shifted(p, 1, 0))
        along_z = huz[x] * (p - shifted(p, 1, 1))
        value = along_x[x] + along_x[x + 1] + nbu[x] * p
        value = value + (along_y + shifted(along_y, -1, 0))
        value = value + (along_z + shifted(along_z, -1, 1))
        out[x] = cond[x] * value + curved[x - HALO]
    return out


def own_restricted(direction, cond, faces, fine, squares, out_ref):
    fx, fy, fz, rd = fine
    hux, huy, huz, nbu = faces
    first, last = min(direction), max(direction)
    own_x = last - first + 1
    rows, lanes = direction[first].shape
    q = {x: cond[x] * direction[x] for x in direction}
    along_x = {first: hux[first] * q[first], last + 1: hux[last + 1] * q[last]}
    for x in range(first + 1, last + 1):
        along_x[x] = hux[x] * (q[x] + q[x - 1])
    z = {first - 1: -along_x[first], last + 1: along_x[last + 1]}
    for x in direction:
        mid = q[x]
        along_y = huy[x] * (mid + shifted(mid, 1, 0))
        along_z = huz[x] * (mid + shifted(mid, 1, 1))
        value = along_x[x] - along_x[x + 1] + nbu[x] * mid
        value = value + (along_y - shifted(along_y, -1, 0))
        z[x] = value + (along_z - shifted(along_z, -1, 1))
    iterate = {x: rd[x] * z[x] for x in z}
    planes = [fx[first - 1] * iterate[first - 1]]
    for x in range(first - 1, last + 2):
        off = off_diagonal(
            iterate[x], iterate.get(x - 1), iterate.get(x + 1),
            fx[x], fx[x + 1], fy[x], fz[x],
        )
        planes.append(KEPT * z[x] + off)
    planes[0] = fx[first - 1] * iterate[first - 1]
    planes.append(fx[last + 2] * iterate[last + 1])
    margin = HALO - 2
    block_rows = (rows - 2 * HALO) // 2
    target = iota((2 * block_rows, rows), 0)
    home = jnp.where(target < block_rows, target + 1, jnp.where(target == block_rows, 0, -9))
    home = jnp.where(target == block_rows + 1, block_rows + 1, home)
    here_row = iota((2 * block_rows, rows), 1)
    pick = flag((here_row >= margin + 2 * home) & (here_row < margin + 2 * home + 2))
    frame_rows = iota((rows, lanes), 0)
    inside = (frame_rows >= margin) & (frame_rows < rows - margin)
    halves = [
        dot(pick, jnp.where(inside, planes[x] + planes[x + 1], 0.0))
        for x in range(0, len(planes), 2)
    ]
    packed = dot(jnp.concatenate(halves, axis=0), z_pairs(lanes))
    tops, borders = [], []
    for x in range(len(halves)):
        at = 2 * block_rows * x
        tops.append(packed[at : at + block_rows])
        borders.append(packed[at + block_rows : at + 2 * block_rows])
    number = own_x // 2
    for x in range(number):
        out_ref[x] = tops[x + 1]
    out_ref[number] = tops[0]
    out_ref[number + 1] = tops[-1]
    pairs = borders[1]
    for x in range(1, number):
        pairs = pairs + shifted(borders[x + 1], 2 * x, 0)
    out_ref[number + 2] = pairs
    tile = fold(squares)
    tile = tile + shifted(tile, 4, 0)
    corners = borders[0] + shifted(borders[-1], 2, 0)
    out_ref[number + 3] = jnp.where(iota(tile.shape, 0) >= 4, tile, corners)


def end_first(sizes, blocks, per, levels, fine, second, curved, cond, faces, source):
    planes, rows, lanes = second.shape
    own_x, own_y = planes - 2 * HALO, rows - 2 * HALO
    coarse = own_x // 2
    scratch_shapes = coarse_scratch((coarse, own_y // 2, lanes // 2), sizes)
    inputs = (
        list(blocks) + list(levels) + list(fine)
        + [second, curved, cond] + list(faces) + [source]
    )

    def kernel(*refs):
        n = sizes[0]
        blocks = refs[:n]
        levels = refs[n : 8 + n]
        fine = refs[8 + n : 12 + n]
        second, curved, cond = refs[12 + n : 15 + n]
        faces = refs[15 + n : 19 + n]
        source = refs[19 + n]
        first_ref, last_ref, own_ref, b1, norm_ref, step_ref = refs[20 + n : 26 + n]
        *scratch, hold = refs[26 + n :]
        image = image_planes(
            levels, fine, sizes, blocks, per, second, curved, cond, faces, scratch
        )
        tile = summed_tiles(blocks, sizes, per, coarse)
        lower = iota(tile.shape, 1) < tile.shape[1] // 2
        form = total(jnp.where(lower, tile, 0.0))
        norm = total(jnp.where(lower, 0.0, tile))
        step = norm / form
        norm_ref[...] = jnp.broadcast_to(norm, (8, 128))
        step_ref[...] = jnp.broadcast_to(step, (8, 128))
        frame_rows = iota((rows, lanes), 0)
        own_rows = (frame_rows >= HALO) & (frame_rows < rows - HALO)
        squares = jnp.zeros((rows, lanes), jnp.float32)
        remaining = {}
        for x in range(HALO, planes - HALO):
            value = jnp.where(own_rows, source[x] - step * image[x], 0.0)
            hold[x - HALO] = value
            remaining[x] = value
            squares = squares + value * value
        own_restricted(remaining, cond, faces, fine, squares, b1)
        for x in range(own_x):
            value = hold[x, HALO : HALO + own_y, :]
            own_ref[x] = value
            if x < HALO:
                first_ref[x] = value
            if x >= own_x - HALO:
                last_ref[x - own_x + HALO] = value

    strip = (HALO, own_y, lanes)
    return call(
        kernel,
        [strip, strip, (own_x, own_y, lanes), (coarse + 4, own_y // 2, lanes // 2)]
        + [(8, 128), (8, 128)],
        scratch_shapes + [(planes, rows, lanes), (own_x, rows, lanes)],
        inputs,
    )


def end_second(
    sizes, blocks, per, levels, fine, second, curved, cond, faces,
    source, remaining, combined, norm, step
):
    planes, rows, lanes = second.shape
    own_x, own_y = planes - 2 * HALO, rows - 2 * HALO
    coarse = own_x // 2
    scratch_shapes = coarse_scratch((coarse, own_y // 2, lanes // 2), sizes)
    inputs = (
        list(blocks) + list(levels) + list(fine)
        + [second, curved, cond] + list(faces) + [source, remaining, combined, norm, step]
    )

    def kernel(*refs):
        n = sizes[0]
        blocks = refs[:n]
        levels = refs[n : 8 + n]
        fine = refs[8 + n : 12 + n]
        second, curved, cond = refs[12 + n : 15 + n]
        faces = refs[15 + n : 19 + n]
        source, remaining, combined, norm, step = refs[19 + n : 24 + n]
        step_out, residual_out = refs[24 + n : 26 + n]
        *scratch, hold, hold_step = refs[26 + n :]
        image = image_planes(
            levels, fine, sizes, blocks, per, second, curved, cond, faces, scratch
        )
        form = total(summed_tiles(blocks, sizes, per, coarse))
        now = norm[0:1, 0:1] / form
        before = step[0:1, 0:1]
        for x in range(HALO, planes - HALO):
            hold[x - HALO] = now * image[x]
            hold_step[x - HALO] = before * source[x] + now * combined[x - HALO]
        for x in range(own_x):
            residual_out[x] = remaining[x] - hold[x, HALO : HALO + own_y, :]
            step_out[x] = hold_step[x, HALO : HALO + own_y, :]

    own = (own_x, own_y, lanes)
    hold = (own_x, rows, lanes)
    return call(
        kernel,
        [own, own],
        scratch_shapes + [(planes, rows, lanes), hold, hold],
        inputs,
    )


def edge_rows(own_x):
    starts, at = [], 0
    for x in range(own_x + 2 * HALO):
        starts.append(at)
        at += reach(HALO, own_x, x)
    return starts, -(-at // 8) * 8


def pack_edges(own, low, high):
    own_x, own_y, lanes = own.shape
    planes = own_x + 2 * HALO
    starts, rows = edge_rows(own_x)

    def kernel(own, low, high, first_ref, last_ref):
        for x in range(planes):
            near = reach(HALO, own_x, x)
            if near == 0:
                continue
            if x < HALO:
                ref, at = low, x
            elif x < HALO + own_x:
                ref, at = own, x - HALO
            else:
                ref, at = high, x - HALO - own_x
            row = starts[x]
            first_ref[row : row + near, :] = ref[at, :near, :]
            last_ref[row : row + near, :] = ref[at, own_y - near :, :]

    return call(kernel, [(rows, lanes)] * 2, [], [own, low, high])


def begin(own, low, high, before, after, cond, faces):
    own_x, own_y, lanes = own.shape
    planes, rows = own_x + 2 * HALO, own_y + 2 * HALO
    frame = (planes, rows, lanes)
    starts, _ = edge_rows(own_x)

    def kernel(
        own, low, high, before, after, cond, hux, huy, huz, nbu, direction, z_out
    ):
        for x in range(planes):
            if x < HALO:
                value = low[x]
            elif x < HALO + own_x:
                value = own[x - HALO]
            else:
                value = high[x - HALO - own_x]
            near = reach(HALO, own_x, x)
            if near < HALO:
                direction[x] = jnp.zeros((rows, lanes), jnp.float32)
            direction[x, HALO : HALO + own_y, :] = value
            if near:
                row = starts[x]
                direction[x, HALO - near : HALO, :] = before[row : row + near, :]
                end = HALO + own_y
                direction[x, end : end + near, :] = after[row : row + near, :]
        z = sensitivity_planes(
            lambda x: cond[x] * direction[x], hux, huy, huz, nbu, 1, planes - 1
        )
        zero = jnp.zeros((rows, lanes), jnp.float32)
        z_out[0] = zero
        z_out[planes - 1] = zero
        for x in z:
            z_out[x] = z[x]

    size = planes * rows * lanes
    return call(
        kernel,
        [frame, frame],
        [],
        [own, low, high, before, after, cond] + list(faces),
        cost=pl.CostEstimate(flops=20 * size, bytes_accessed=28 * size, transcendentals=0),
    )


def on_device(log_conductivity, state, gradient, prior_sample, sensor_cells, noise_precision):
    sizes = (lax.axis_size("gx"), lax.axis_size("gy"))
    cells_x, cells_y, cells_z = log_conductivity.shape
    coarse = (cells_x // 2, cells_y // 2, cells_z // 2)
    per = coarse[0] + 1

    fields = (prior_sample, gradient, log_conductivity, state)
    own_cond, weight, *x_edges = prepare(
        sizes, fields, sensor_cells[None], noise_precision[None]
    )
    fields = fields + (weight,)
    x_edges = exchange(*x_edges, "gx")
    y_edges = exchange(*pack_setup_edges(fields, *x_edges), "gy")
    (cond, hux, huy, huz, nbu, fx, fy, fz, rd, weight, source, z, b1) = setup(
        sizes, fields, x_edges, y_edges, own_cond
    )
    faces = (hux, huy, huz, nbu)
    fine = (fx, fy, fz, rd)

    blocks = gathered(b1)
    curved = prior_part(sizes, source)
    levels = coarse_setup(sizes, blocks, coarse)
    b1, second, kept = middle(
        sizes, blocks, 2 * coarse[0], levels, fine, z, source, curved, weight, None
    )
    first, last, remaining, b1, norm, step = end_first(
        sizes, gathered(b1), per, levels, fine, second, curved, cond, faces, source
    )
    row = gathered_row(b1)
    low, high = rotate(last, "gx", 1), rotate(first, "gx", -1)
    first, last = pack_edges(remaining, low, high)
    row, first, last = lax.optimization_barrier((row, first, last))
    blocks = gathered_rows(row)
    before, after = rotate(last, "gy", 1), rotate(first, "gy", -1)
    direction, z = begin(remaining, low, high, before, after, cond, faces)
    b1, second, combined, curved, norm = middle(
        sizes, blocks, per + 3, levels, fine, z, direction, prior_part(sizes, direction), weight,
        (kept, source, norm, curved),
    )
    return tuple(
        end_second(
            sizes, gathered(b1), per, levels, fine, second, curved, cond,
            faces, source, remaining, combined, norm, step,
        )
    )


def solution(mesh):
    field = P(("ens", "gx"), "gy", None)
    sensors = P(("ens", "gx", "gy"))
    return jax.shard_map(
        on_device,
        mesh=mesh,
        in_specs=(field, field, field, field, sensors, sensors),
        out_specs=(field, field),
        check_vma=False,
    )
```

```python
import jax
import jax.numpy as jnp
from jax import lax
from jax.experimental import pallas as pl
from jax.experimental.pallas import tpu as pltpu
from jax.sharding import PartitionSpec as P

DAMPING = 0.8
KEPT = 0.2
PRIOR_MASS = 0.5
COARSE_SWEEPS = 6
HALO = 4
DEEP = 5
WIDE = 2
VMEM_LIMIT = 24 * 1024 * 1024
EXACT = lax.Precision.HIGHEST


def rotate(x, axis, shift):
    size = lax.axis_size(axis)
    return lax.ppermute(x, axis, [(i, (i + shift) % size) for i in range(size)])


def exchange(even_pairs, odd_pairs, axis):
    size = lax.axis_size(axis)
    inner = [(i, i) for i in (0, size - 1)]
    for i in range(1, size - 1, 2):
        inner += [(i, i + 1), (i + 1, i)]
    outer = [(i, i ^ 1) for i in range(size)]
    return lax.ppermute(even_pairs, axis, outer), lax.ppermute(odd_pairs, axis, inner)


def here():
    return lax.axis_index("gx"), lax.axis_index("gy")


def shifted(v, step, dim):
    size = v.shape[dim]
    return pltpu.roll(v, step % size, dim)


def dot(a, b):
    return lax.dot_general(
        a, b, (((1,), (0,)), ((), ())), precision=EXACT, preferred_element_type=jnp.float32
    )


def iota(shape, dim):
    return lax.broadcasted_iota(jnp.int32, shape, dim)


def total(tile):
    return jnp.sum(jnp.sum(tile, axis=1, keepdims=True), axis=0, keepdims=True)


def fold(plane):
    rows, lanes = plane.shape
    parts = [
        plane[r : r + 8, c : c + 128] for r in range(0, rows, 8) for c in range(0, lanes, 128)
    ]
    out = parts[0]
    for part in parts[1:]:
        out = out + part
    return out


def z_pairs(lanes):
    half = lanes // 2
    return (iota((lanes, half), 0) // 2 == iota((lanes, half), 1)).astype(jnp.float32)


def z_copies(lanes):
    return (iota((lanes, 2 * lanes), 0) == iota((lanes, 2 * lanes), 1) // 2).astype(jnp.float32)


def restrict_rows(planes, first_row, rows):
    extent = planes[0].shape[0]
    here = iota(planes[0].shape, 0)
    inside = (here >= first_row) & (here < first_row + rows)
    pick = (
        (iota((rows // 2, extent), 1) - first_row + 2) // 2 - 1 == iota((rows // 2, extent), 0)
    ).astype(jnp.float32)
    halves = []
    for x in range(0, len(planes), 2):
        pair = jnp.where(inside, planes[x] + planes[x + 1], 0.0)
        halves.append(dot(pick, pair))
    packed = dot(jnp.concatenate(halves, axis=0), z_pairs(planes[0].shape[1]))
    return packed.reshape(len(planes) // 2, rows // 2, packed.shape[1])


def swap_sum(v, dim, stride):
    even = (iota(v.shape, dim) // stride) % 2 == 0
    return v + jnp.where(even, shifted(v, -stride, dim), shifted(v, stride, dim))


def off_diagonal(v, low, high, fx, fx_high, fy, fz, step=1):
    out = fy * shifted(v, 1, 0) + shifted(fy * v, -1, 0)
    out = out + (fz * shifted(v, step, 1) + shifted(fz * v, -step, 1))
    if low is not None:
        out = out + fx * low
    if high is not None:
        out = out + fx_high * high
    return out


def coefficients(planes, scale, step, x_mask, y_mask, z_mask, outside):
    count = len(planes)
    faces = [None] * count
    for x in range(count):
        low = planes[x] if x == 0 else planes[x - 1]
        faces[x] = (scale * x_mask(x)) * (0.5 * (planes[x] + low))
    out = []
    for x in range(count):
        k = planes[x]
        fy = (scale * y_mask) * (0.5 * (k + shifted(k, 1, 0)))
        fz = (scale * z_mask) * (0.5 * (k + shifted(k, step, 1)))
        diag = (scale * outside(x)) * k + fy + shifted(fy, -1, 0) + fz + shifted(fz, -step, 1)
        diag = diag + faces[x]
        if x + 1 < count:
            diag = diag + faces[x + 1]
        out.append((faces[x], fy, fz, DAMPING / diag))
    return out


def flag(condition):
    return jnp.where(condition, 1.0, 0.0).astype(jnp.float32)


def placed_whole(refs, place, sizes, shape, per, first, whole_ref):
    planes, block_rows, _ = shape
    for s in range(sizes[0]):
        at_x = lax.rem(place[0] - s + sizes[0], sizes[0]) * planes
        for t in range(sizes[1]):
            at_y = lax.rem(place[1] - t + sizes[1], sizes[1])
            row = pl.multiple_of(at_y * block_rows, block_rows)
            for x in range(planes):
                block = refs[s][t * per + first + x]
                whole_ref[at_x + x, pl.ds(row, block_rows), :] = block


def placed_overlapping(refs, place, sizes, shape, per, room, whole_ref):
    planes, block_rows, lanes = shape
    sub = iota((block_rows, lanes), 0)
    last, first = sub == block_rows - 1, sub == 0

    def spots():
        for s in range(sizes[0]):
            at_x = lax.rem(place[0] - s + sizes[0], sizes[0]) * planes
            for t in range(sizes[1]):
                at_y = lax.rem(place[1] - t + sizes[1], sizes[1])
                row = pl.multiple_of(at_y * block_rows, block_rows)
                yield refs[s], t * per, at_x, row

    for ref, tile, at_x, row in spots():
        for x in range(planes):
            room[at_x + x + 1, pl.ds(row + block_rows, block_rows), :] = ref[tile + x]
    for ref, tile, at_x, row in spots():
        adds = [(0, 1, ref[tile + planes]), (planes + 1, 1, ref[tile + planes + 1])]
        pairs = [(x + 1, ref[tile + planes + 2], 2 * x) for x in range(planes)]
        pairs += [(0, ref[tile + planes + 3], 0), (planes + 1, ref[tile + planes + 3], 2)]
        for x, borders, at in pairs:
            before = shifted(borders, block_rows - 1 - at, 0)
            after = shifted(borders, -(at + 1), 0)
            adds.append((x, 0, jnp.where(last, before, 0.0)))
            adds.append((x, 2, jnp.where(first, after, 0.0)))
        spans = [
            (at_x + x, pl.ds(row + step * block_rows, block_rows)) for x, step, _ in adds
        ]
        values = [room[x, span, :] + add for (x, span), (_, _, add) in zip(spans, adds)]
        for (x, span), value in zip(spans, values):
            room[x, span, :] = value
    rows = block_rows * sizes[1]
    for x in range(planes * sizes[0]):
        whole_ref[x, :rows, :] = room[x + 1, block_rows : block_rows + rows, :]


def summed_tiles(refs, sizes, per, index):
    tile = None
    for s in range(sizes[0]):
        for t in range(sizes[1]):
            part = refs[s][t * per + index]
            tile = part if tile is None else tile + part
    return tile


def halved(one, two):
    lower = iota(one.shape, 1) < one.shape[1] // 2
    middle = one.shape[1] // 2
    return jnp.where(lower, one + shifted(one, middle, 1), two + shifted(two, middle, 1))


def row_pairs(ref, x, rows):
    return ref[x, pl.ds(0, rows // 2, stride=2), :] + ref[x, pl.ds(1, rows // 2, stride=2), :]


def coarse_correction(place, own, source, mid, pairs, level1, level2):
    fx1, fy1, fz1, rd1 = level1
    fx2, fy2, fz2, rd2 = level2
    planes, own_rows, lanes = own
    count = source.shape[0]
    rows = source.shape[1] - own_rows
    half = count // 2
    blank = jnp.zeros((own_rows, lanes), jnp.float32)
    for x in range(count):
        source[x, rows:, :] = blank
        mid[x, rows:, :] = blank
        mid[x, :rows, :] = rd1[x, :rows, :] * source[x, :rows, :]

    def off1(x):
        low = mid[x - 1, :rows, :] if x > 0 else None
        high = mid[x + 1, :rows, :] if x + 1 < count else None
        fx_high = fx1[x + 1, :rows, :] if x + 1 < count else None
        return off_diagonal(
            mid[x, :rows, :], low, high, fx1[x, :rows, :], fx_high,
            fy1[x, :rows, :], fz1[x, :rows, :],
        )

    for x in range(half):
        pair = KEPT * (source[2 * x, :rows, :] + source[2 * x + 1, :rows, :])
        pairs[x, :rows, :] = swap_sum(pair + (off1(2 * x) + off1(2 * x + 1)), 1, 1)
    coarse = [row_pairs(pairs, x, rows) for x in range(half)]
    iterate = [rd2[x] * coarse[x] for x in range(half)]
    for sweep in range(COARSE_SWEEPS - 1):
        new = []
        for x in range(half):
            low = iterate[x - 1] if x > 0 else None
            high = iterate[x + 1] if x + 1 < half else None
            fx_high = fx2[x + 1] if x + 1 < half else None
            off = off_diagonal(iterate[x], low, high, fx2[x], fx_high, fy2[x], fz2[x], 2)
            new.append(KEPT * iterate[x] + rd2[x] * (coarse[x] + off))
        iterate = new
    for x in range(half):
        pairs[x, rows:, :] = blank
        pairs[x, pl.ds(0, rows // 2, stride=2), :] = iterate[x]
        pairs[x, pl.ds(1, rows // 2, stride=2), :] = iterate[x]

    start = jnp.clip((place[1] - 1) * own_rows, 0, max(rows - 2 * own_rows, 0))
    window = pl.ds(pl.multiple_of(start, own_rows), min(3 * own_rows, rows + own_rows))
    ends = HALO // 2
    at = [
        jnp.clip(place[0] * planes - ends + x, 0, count - 1) for x in range(-1, planes + 2 * ends + 1)
    ]
    value = [mid[a, window, :] + pairs[lax.div(a, 2), window, :] for a in at]
    first = place[1] * own_rows - ends - start
    frame_rows = 2 * (own_rows + 2 * ends)
    extent = value[0].shape[0]
    pick = flag(
        iota((frame_rows, extent), 1) == first + iota((frame_rows, extent), 0) // 2
    )
    parts = []
    for x in range(1, len(at) - 1):
        a = at[x]
        off = off_diagonal(
            value[x], value[x - 1], value[x + 1], fx1[a, window, :], fx1[a + 1, window, :],
            fy1[a, window, :], fz1[a, window, :],
        )
        smooth = KEPT * value[x] + rd1[a, window, :] * (source[a, window, :] + off)
        parts.append(dot(pick, smooth))
    wide = dot(jnp.concatenate(parts, axis=0), z_copies(lanes))
    return [wide[x * frame_rows : (x + 1) * frame_rows] for x in range(len(parts))]


def coarse_scratch(own, sizes):
    whole = (own[0] * sizes[0], own[1] * (sizes[1] + 1), own[2])
    return [whole, whole, (whole[0] // 2,) + whole[1:]]


def frame_masks(place, shape, pad, sizes):
    planes, rows, lanes = shape
    own_x, own_y = planes - 2 * pad, rows - 2 * pad
    all_x, all_y = own_x * sizes[0], own_y * sizes[1]
    base_x, base_y = place[0] * own_x - pad, place[1] * own_y - pad
    at_y = base_y + iota((rows, lanes), 0)
    at_z = iota((rows, lanes), 1)
    y_mask = flag((at_y >= 1) & (at_y < all_y))
    z_mask = flag(at_z >= 1)
    edges = flag(at_y == 0) + flag(at_y == all_y - 1) + flag(at_z == 0) + flag(at_z == lanes - 1)

    def x_mask(x):
        at = base_x + x
        return flag((at >= 1) & (at < all_x))

    def outside(x):
        at = base_x + x
        return edges + (flag(at == 0) + flag(at == all_x - 1))

    return x_mask, y_mask, z_mask, outside


def prior_rows(center, low, high, up, down, x_low, x_high, y_mask, z_mask, outside):
    rows, lanes = center.shape
    y_next = shifted(y_mask, -1, 0)
    z_next = shifted(z_mask, -1, 1)
    out = (PRIOR_MASS + outside) * center + x_low * (center - low) + x_high * (center - high)
    out = out + y_mask * (center - up) + y_next * (center - down)
    out = out + z_mask * (center - shifted(center, 1, 1))
    return out + z_next * (center - shifted(center, -1, 1))


def fine_restricted(base, fields, fx, fy, fz, out_ref, first, own):
    planes = []
    for x in range(first, first + own):
        off = off_diagonal(
            fields[x], fields[x - 1], fields[x + 1], fx[x], fx[x + 1], fy[x], fz[x]
        )
        planes.append(KEPT * base[x] + off)
    rows = planes[0].shape[0]
    coarse = restrict_rows(planes, first, rows - 2 * first)
    for x in range(coarse.shape[0]):
        out_ref[x] = coarse[x]


def sensitivity_planes(q, hux, huy, huz, nbu, first, last):
    faces = {x: hux[x] * (q(x) + q(x - 1)) for x in range(first, last + 1)}
    out = {}
    for x in range(first, last):
        mid = q(x)
        along_y = huy[x] * (mid + shifted(mid, 1, 0))
        along_z = huz[x] * (mid + shifted(mid, 1, 1))
        z = faces[x] - faces[x + 1] + nbu[x] * mid
        z = z + (along_y - shifted(along_y, -1, 0))
        out[x] = z + (along_z - shifted(along_z, -1, 1))
    return out


def first_residual_stage(z, fx, fy, fz, rd, z_ref, out_ref, planes):
    for x in z:
        z_ref[x] = z[x]
    iterate = {x: rd[x] * z[x] for x in range(HALO - 1, planes - HALO + 1)}
    fine_restricted(z, iterate, fx, fy, fz, out_ref, HALO, planes - 2 * HALO)


def call(kernel, outs, scratch, inputs, limit=VMEM_LIMIT, cost=None):
    vmem = pl.BlockSpec(memory_space=pltpu.VMEM)
    return pl.pallas_call(
        kernel,
        out_shape=[jax.ShapeDtypeStruct(shape, jnp.float32) for shape in outs],
        in_specs=[vmem] * len(inputs),
        out_specs=[vmem] * len(outs),
        scratch_shapes=[pltpu.VMEM(shape, jnp.float32) for shape in scratch],
        compiler_params=pltpu.CompilerParams(vmem_limit_bytes=limit),
        cost_estimate=cost,
    )(*inputs)


def scattered(sizes, shape, cells, precision):
    own_x, own_y, lanes = shape
    all_rows = own_y * sizes[1]

    def kernel(cells, precision, out_ref):
        place = here()
        cell = cells[...]
        column = lax.div(cell, lanes)
        at_z = cell - column * lanes
        at_x = lax.div(column, all_rows)
        at_y = column - at_x * all_rows
        row = (at_x - place[0] * own_x) * own_y + (at_y - place[1] * own_y)
        count = cell.shape[1]
        picks = flag(iota((own_x * own_y, count), 0) == row)
        values = jnp.where(iota((lanes, count), 0) == at_z, precision[...], 0.0)
        weight = lax.dot_general(
            picks, values, (((1,), (1,)), ((), ())),
            precision=EXACT, preferred_element_type=jnp.float32,
        )
        for x in range(own_x):
            out_ref[x] = weight[x * own_y : (x + 1) * own_y]

    cost = pl.CostEstimate(flops=10**9, bytes_accessed=4096, transcendentals=0)
    return call(kernel, [shape], [], [cells, precision], cost=cost)[0]


def prepare(fields):
    own_x, own_y, lanes = fields[0].shape
    number = len(fields)
    starts, rows = setup_rows(own_x, True)

    def kernel(*refs):
        place = here()
        fields = refs[:number]
        coarse_ref, even_edge, odd_edge, even_rows, odd_rows = refs[number:]
        even_x = lax.rem(place[0], 2) == 0
        even_y = lax.rem(place[1], 2) == 0
        at = 0
        for index, depth in enumerate(FIELD_DEPTHS):
            ref = fields[index]
            start = own_x - depth
            even_start = jnp.where(even_x, start, 0)
            odd_start = jnp.where(even_x, 0, start)
            for x in range(depth):
                even_edge[at + x] = ref[even_start + x]
                odd_edge[at + x] = ref[odd_start + x]
            at += depth
            for x in range(own_x):
                first, last = ref[x, :depth, :], ref[x, own_y - depth :, :]
                row = starts[index, x + depth]
                even_rows[row : row + depth, :] = jnp.where(even_y, last, first)
                odd_rows[row : row + depth, :] = jnp.where(even_y, first, last)
        planes = [jnp.exp(fields[2][x]) for x in range(own_x)]
        coarse = restrict_rows(planes, 0, own_y)
        for x in range(coarse.shape[0]):
            coarse_ref[x] = coarse[x] * 0.125

    edge = (sum(FIELD_DEPTHS), own_y, lanes)
    return call(
        kernel,
        [(own_x // 2, own_y // 2, lanes // 2), edge, edge, (rows, lanes), (rows, lanes)],
        [],
        list(fields),
    )


def gathered_row(own):
    size = lax.axis_size("gy")
    return jnp.concatenate([own] + [rotate(own, "gy", t) for t in range(1, size)], axis=0)


def gathered_rows(row):
    return [row] + [rotate(row, "gx", s) for s in range(1, lax.axis_size("gx"))]


def gathered(own):
    return gathered_rows(gathered_row(own))


FIELD_DEPTHS = (DEEP, HALO, HALO, HALO, WIDE)


def reach(depth, own_x, x):
    return depth - max(0, depth - x, x - depth - own_x + 1)


def setup_rows(own_x, own):
    starts, at = {}, 0
    for index, depth in enumerate(FIELD_DEPTHS):
        for x in range(own_x + 2 * depth):
            near = reach(depth, own_x, x)
            if near and own == (near == depth):
                starts[index, x] = at
                at += near
    return starts, -(-at // 8) * 8


def field_plane(fields, even_edge, odd_edge, even, index, x):
    depth = FIELD_DEPTHS[index]
    start = sum(FIELD_DEPTHS[:index])
    own = fields[index].shape[0]
    if x < depth:
        return jnp.where(even, odd_edge[start + x], even_edge[start + x])
    if x < depth + own:
        return fields[index][x - depth]
    at = start + x - depth - own
    return jnp.where(even, even_edge[at], odd_edge[at])


def pack_corners(fields, even_edge, odd_edge):
    own_x, own_y, lanes = fields[0].shape
    starts, rows = setup_rows(own_x, False)

    def kernel(even_edge, odd_edge, even_ref, odd_ref):
        place = here()
        even_x = lax.rem(place[0], 2) == 0
        even_y = lax.rem(place[1], 2) == 0
        for (index, x), at in starts.items():
            near = reach(FIELD_DEPTHS[index], own_x, x)
            plane = field_plane(fields, even_edge, odd_edge, even_x, index, x)
            first, last = plane[:near], plane[own_y - near :]
            even_ref[at : at + near, :] = jnp.where(even_y, last, first)
            odd_ref[at : at + near, :] = jnp.where(even_y, first, last)

    return call(kernel, [(rows, lanes)] * 2, [], [even_edge, odd_edge])


def setup(sizes, fields, x_edges, y_edges, corners, own_cond):
    own_x, own_y, lanes = fields[0].shape
    frame = (own_x + 2 * HALO, own_y + 2 * HALO, lanes)
    own_starts, _ = setup_rows(own_x, True)
    corner_starts, _ = setup_rows(own_x, False)
    number = len(fields)
    coarse = (own_x // 2, own_y // 2, lanes // 2)

    def kernel(*refs):
        place = here()
        fields = refs[:number]
        even_edge, odd_edge, *y_rows = refs[number : 6 + number]
        own_cond = refs[6 + number]
        even_x = lax.rem(place[0], 2) == 0
        even_y = lax.rem(place[1], 2) == 0
        outs = refs[7 + number : 20 + number]
        cond, hux, huy, huz, nbu, fx, fy, fz, rd, weight, source, z_out, b1 = outs
        prior, state, grad = refs[20 + number :]

        def assemble(index, ref, x_skip, first_row):
            depth = FIELD_DEPTHS[index]
            for x in range(own_x + 2 * depth):
                near = reach(depth, own_x, x)
                own_row = first_row + depth
                if near < depth or x_skip:
                    ref[x + x_skip] = jnp.zeros(ref.shape[1:], jnp.float32)
                ref[x + x_skip, own_row : own_row + own_y, :] = field_plane(
                    fields, even_edge, odd_edge, even_x, index, x
                )
                if near == 0:
                    continue
                if near == depth:
                    at, (even_rows, odd_rows) = own_starts[index, x], y_rows[:2]
                else:
                    at, (even_rows, odd_rows) = corner_starts[index, x], y_rows[2:]
                even_part, odd_part = even_rows[at : at + near, :], odd_rows[at : at + near, :]
                ref[x + x_skip, own_row - near : own_row, :] = jnp.where(
                    even_y, odd_part, even_part
                )
                end = own_row + own_y
                ref[x + x_skip, end : end + near, :] = jnp.where(even_y, even_part, odd_part)

        zero = jnp.zeros(frame[1:], jnp.float32)
        for x in range(HALO - WIDE):
            weight[x] = zero
            weight[frame[0] - 1 - x] = zero
        assemble(0, prior, 0, 0)
        assemble(1, grad, 0, 0)
        assemble(2, cond, 0, 0)
        assemble(3, state, 0, 0)
        assemble(4, weight, HALO - WIDE, HALO - WIDE)
        x_mask, y_mask, z_mask, outside = frame_masks(place, frame, HALO, sizes)
        planes, rows = frame[:2]
        for x in range(planes):
            center = prior[x + 1, 1 : 1 + rows, :]
            value = prior_rows(
                center,
                prior[x, 1 : 1 + rows, :],
                prior[x + 2, 1 : 1 + rows, :],
                prior[x + 1, 0:rows, :],
                prior[x + 1, 2 : 2 + rows, :],
                x_mask(x),
                x_mask(x + 1),
                y_mask,
                z_mask,
                outside(x),
            )
            source[x] = value - grad[x]
        for x in range(planes):
            cond[x] = jnp.exp(cond[x])
        for x in range(planes):
            u = state[x]
            if x > 0:
                hux[x] = (0.5 * x_mask(x)) * (u - state[x - 1])
            else:
                hux[x] = zero
            huy[x] = (0.5 * y_mask) * (u - shifted(u, 1, 0))
            huz[x] = (0.5 * z_mask) * (u - shifted(u, 1, 1))
            nbu[x] = outside(x) * u
        found = coefficients(
            [cond[x] for x in range(planes)], 1.0, 1, x_mask, y_mask, z_mask, outside
        )
        for x in range(planes):
            fx[x], fy[x], fz[x], rd[x] = found[x]
        z = sensitivity_planes(
            lambda x: cond[x] * source[x], hux, huy, huz, nbu, 1, planes - 1
        )
        z_out[0] = zero
        z_out[planes - 1] = zero
        first_residual_stage(z, fx, fy, fz, rd, z_out, b1, planes)
        for x in range(coarse[0]):
            b1[coarse[0] + x] = own_cond[x]

    deep = (own_x + 2 * DEEP, -(-(own_y + 2 * DEEP) // 8) * 8, lanes)
    return call(
        kernel,
        [frame] * 12 + [(2 * coarse[0],) + coarse[1:]],
        [deep, frame, frame],
        list(fields) + list(x_edges) + list(y_edges) + list(corners) + [own_cond],
    )


def coarse_setup(sizes, blocks, shape):
    planes, own_rows, lanes = shape
    count, rows = planes * sizes[0], own_rows * sizes[1]
    half = count // 2

    def kernel(*refs):
        blocks = refs[: sizes[0]]
        outs = refs[sizes[0] : 8 + sizes[0]]
        cond, pairs = refs[8 + sizes[0] :]
        placed_whole(blocks, here(), sizes, shape, 2 * planes, planes, cond)

        def level(values, scale, step, refs):
            number, extent = len(values), values[0].shape[0]
            at_y = iota((extent, lanes), 0)
            at_z = iota((extent, lanes), 1)
            edges = (
                flag(at_y == 0) + flag(at_y == extent - 1)
                + flag(at_z < step) + flag(at_z >= lanes - step)
            )

            def x_mask(x):
                return 1.0 if x > 0 else 0.0

            def outside(x):
                return edges + float((x == 0) + (x == number - 1))

            found = coefficients(
                values, scale, step, x_mask, flag(at_y >= 1), flag(at_z >= step), outside
            )
            for x in range(number):
                for ref, value in zip(refs, found[x]):
                    ref[x, :extent, :] = value

        level([cond[x] for x in range(count)], 2.0, 1, outs[:4])
        blank = jnp.zeros((own_rows, lanes), jnp.float32)
        for x in range(count):
            for ref in outs[:4]:
                ref[x, rows:, :] = blank
        outs[0][count] = jnp.zeros((rows + own_rows, lanes), jnp.float32)
        for x in range(half):
            pairs[x] = swap_sum(cond[2 * x] + cond[2 * x + 1], 1, 1)
        coarse = [0.125 * row_pairs(pairs, x, rows) for x in range(half)]
        level(coarse, 4.0, 2, outs[4:])

    padded = (count, rows + own_rows, lanes)
    return call(
        kernel,
        [(count + 1,) + padded[1:]] + [padded] * 3 + [(half, rows // 2, lanes)] * 4,
        [(count, rows, lanes), (half, rows, lanes)],
        list(blocks),
    )


def prior_part(sizes, direction):
    planes, rows, lanes = direction.shape

    def kernel(direction, out_ref):
        x_mask, y_mask, z_mask, outside = frame_masks(here(), direction.shape, HALO, sizes)
        for x in range(HALO, planes - HALO):
            center = direction[x]
            out_ref[x - HALO] = prior_rows(
                center,
                direction[x - 1],
                direction[x + 1],
                shifted(center, 1, 0),
                shifted(center, -1, 0),
                x_mask(x),
                x_mask(x + 1),
                y_mask,
                z_mask,
                outside(x),
            )

    size = planes * rows * lanes
    return call(
        kernel, [(planes - 2 * HALO, rows, lanes)], [], [direction],
        cost=pl.CostEstimate(flops=20 * size, bytes_accessed=8 * size, transcendentals=0),
    )[0]


def middle(sizes, blocks, per, levels, fine, z, direction, curved, weight, earlier):
    planes, rows, lanes = z.shape
    own_x = planes - 2 * HALO
    coarse = (own_x // 2, (rows - 2 * HALO) // 2, lanes // 2)
    first_time = earlier is None
    extra = [] if first_time else list(earlier)
    inputs = list(blocks) + list(levels) + list(fine) + [z, direction, curved, weight] + extra

    def kernel(*refs):
        at = 0

        def take(number):
            nonlocal at
            at += number
            return refs[at - number : at]

        place = here()
        blocks = take(sizes[0])
        levels = take(8)
        fx, fy, fz, rd = take(4)
        z, direction, curved, weight = take(4)
        old = take(len(extra))
        b1, second = take(2)
        if first_time:
            (kept,) = take(1)
        else:
            combined, curved_out, norm_ref = take(3)
        source, whole_mid, pairs, mid, *room = refs[at:]
        frame_rows = iota((rows, lanes), 0)
        own_rows = (frame_rows >= HALO) & (frame_rows < rows - HALO)
        if first_time:
            placed_whole(blocks, place, sizes, coarse, per, 0, source)
        else:
            placed_overlapping(blocks, place, sizes, coarse, per, room[0], source)
        correction = coarse_correction(
            place, coarse, source, whole_mid, pairs, levels[:4], levels[4:]
        )
        zero = jnp.zeros((rows, lanes), jnp.float32)
        forms = zero
        squares = zero
        if first_time:
            for x in range(own_x):
                d = direction[x + HALO]
                forms = forms + d * curved[x]
                squares = squares + d * d
        else:
            tile = summed_tiles(blocks, sizes, per, per - 1)
            norm = total(jnp.where(iota(tile.shape, 0) >= 4, tile, 0.0))
            ratio = norm / old[2][0:1, 0:1]
            for x in range(own_x):
                d = direction[x + HALO] + ratio * old[1][x + HALO]
                image = curved[x] + ratio * old[3][x]
                combined[x] = d
                curved_out[x] = image
                forms = forms + d * image
            norm_ref[...] = jnp.broadcast_to(norm, (8, 128))
        for x in range(1, planes - 1):
            mid[x] = rd[x] * z[x] + correction[x // 2]
        rights = {}
        for x in range(2, planes - 2):
            off = off_diagonal(mid[x], mid[x - 1], mid[x + 1], fx[x], fx[x + 1], fy[x], fz[x])
            change = KEPT * mid[x] + rd[x] * (z[x] + off)
            if first_time:
                kept[x] = change
            else:
                change = change + ratio * old[0][x]
            right = weight[x] * change
            second[x] = right
            rights[x] = right
            if HALO <= x < planes - HALO:
                forms = forms + right * change
        for x in (0, 1, planes - 2, planes - 1):
            second[x] = zero
            if first_time:
                kept[x] = zero
        iterate = {x: rd[x] * rights[x] for x in range(HALO - 1, planes - HALO + 1)}
        fine_restricted(rights, iterate, fx, fy, fz, b1, HALO, own_x)
        tile = fold(jnp.where(own_rows, forms, 0.0))
        if first_time:
            tile = halved(tile, fold(jnp.where(own_rows, squares, 0.0)))
        b1[coarse[0]] = tile

    frame = (planes, rows, lanes)
    own = (own_x, rows, lanes)
    margin = (coarse[0] * sizes[0] + 2, coarse[1] * (sizes[1] + 2), coarse[2])
    return call(
        kernel,
        [(coarse[0] + 1,) + coarse[1:], frame] + ([frame] if first_time else [own, own, (8, 128)]),
        coarse_scratch(coarse, sizes) + [frame] + ([] if first_time else [margin]),
        inputs,
    )


def image_planes(levels, fine, sizes, blocks, per, second, curved, cond, faces, scratch):
    fx, fy, fz, rd = fine
    hux, huy, huz, nbu = faces
    source, whole_mid, pairs, mid = scratch
    place = here()
    planes, rows, lanes = second.shape
    own = ((planes - 2 * HALO) // 2, (rows - 2 * HALO) // 2, lanes // 2)
    placed_whole(blocks, place, sizes, own, per, 0, source)
    correction = coarse_correction(
        place, own, source, whole_mid, pairs, levels[:4], levels[4:]
    )
    for x in range(2, planes - 2):
        mid[x] = rd[x] * second[x] + correction[x // 2]
    adjoint = {}
    for x in range(3, planes - 3):
        off = off_diagonal(mid[x], mid[x - 1], mid[x + 1], fx[x], fx[x + 1], fy[x], fz[x])
        adjoint[x] = KEPT * mid[x] + rd[x] * (second[x] + off)
    out = {}
    along_x = {
        x: hux[x] * (adjoint[x] - adjoint[x - 1]) for x in range(HALO, planes - HALO + 1)
    }
    for x in range(HALO, planes - HALO):
        p = adjoint[x]
        along_y = huy[x] * (p - shifted(p, 1, 0))
        along_z = huz[x] * (p - shifted(p, 1, 1))
        value = along_x[x] + along_x[x + 1] + nbu[x] * p
        value = value + (along_y + shifted(along_y, -1, 0))
        value = value + (along_z + shifted(along_z, -1, 1))
        out[x] = cond[x] * value + curved[x - HALO]
    return out


def own_restricted(direction, cond, faces, fine, squares, out_ref):
    fx, fy, fz, rd = fine
    hux, huy, huz, nbu = faces
    first, last = min(direction), max(direction)
    own_x = last - first + 1
    rows, lanes = direction[first].shape
    q = {x: cond[x] * direction[x] for x in direction}
    along_x = {first: hux[first] * q[first], last + 1: hux[last + 1] * q[last]}
    for x in range(first + 1, last + 1):
        along_x[x] = hux[x] * (q[x] + q[x - 1])
    z = {first - 1: -along_x[first], last + 1: along_x[last + 1]}
    for x in direction:
        mid = q[x]
        along_y = huy[x] * (mid + shifted(mid, 1, 0))
        along_z = huz[x] * (mid + shifted(mid, 1, 1))
        value = along_x[x] - along_x[x + 1] + nbu[x] * mid
        value = value + (along_y - shifted(along_y, -1, 0))
        z[x] = value + (along_z - shifted(along_z, -1, 1))
    iterate = {x: rd[x] * z[x] for x in z}
    planes = [fx[first - 1] * iterate[first - 1]]
    for x in range(first - 1, last + 2):
        off = off_diagonal(
            iterate[x], iterate.get(x - 1), iterate.get(x + 1),
            fx[x], fx[x + 1], fy[x], fz[x],
        )
        planes.append(KEPT * z[x] + off)
    planes[0] = fx[first - 1] * iterate[first - 1]
    planes.append(fx[last + 2] * iterate[last + 1])
    margin = HALO - 2
    block_rows = (rows - 2 * HALO) // 2
    target = iota((2 * block_rows, rows), 0)
    home = jnp.where(target < block_rows, target + 1, jnp.where(target == block_rows, 0, -9))
    home = jnp.where(target == block_rows + 1, block_rows + 1, home)
    here_row = iota((2 * block_rows, rows), 1)
    pick = flag((here_row >= margin + 2 * home) & (here_row < margin + 2 * home + 2))
    frame_rows = iota((rows, lanes), 0)
    inside = (frame_rows >= margin) & (frame_rows < rows - margin)
    halves = [
        dot(pick, jnp.where(inside, planes[x] + planes[x + 1], 0.0))
        for x in range(0, len(planes), 2)
    ]
    packed = dot(jnp.concatenate(halves, axis=0), z_pairs(lanes))
    tops, borders = [], []
    for x in range(len(halves)):
        at = 2 * block_rows * x
        tops.append(packed[at : at + block_rows])
        borders.append(packed[at + block_rows : at + 2 * block_rows])
    number = own_x // 2
    for x in range(number):
        out_ref[x] = tops[x + 1]
    out_ref[number] = tops[0]
    out_ref[number + 1] = tops[-1]
    pairs = borders[1]
    for x in range(1, number):
        pairs = pairs + shifted(borders[x + 1], 2 * x, 0)
    out_ref[number + 2] = pairs
    tile = fold(squares)
    tile = tile + shifted(tile, 4, 0)
    corners = borders[0] + shifted(borders[-1], 2, 0)
    out_ref[number + 3] = jnp.where(iota(tile.shape, 0) >= 4, tile, corners)


def end_first(sizes, blocks, per, levels, fine, second, curved, cond, faces, source):
    planes, rows, lanes = second.shape
    own_x, own_y = planes - 2 * HALO, rows - 2 * HALO
    coarse = own_x // 2
    scratch_shapes = coarse_scratch((coarse, own_y // 2, lanes // 2), sizes)
    inputs = (
        list(blocks) + list(levels) + list(fine)
        + [second, curved, cond] + list(faces) + [source]
    )

    def kernel(*refs):
        n = sizes[0]
        blocks = refs[:n]
        levels = refs[n : 8 + n]
        fine = refs[8 + n : 12 + n]
        second, curved, cond = refs[12 + n : 15 + n]
        faces = refs[15 + n : 19 + n]
        source = refs[19 + n]
        first_ref, last_ref, own_ref, b1, norm_ref, step_ref = refs[20 + n : 26 + n]
        *scratch, hold = refs[26 + n :]
        image = image_planes(
            levels, fine, sizes, blocks, per, second, curved, cond, faces, scratch
        )
        tile = summed_tiles(blocks, sizes, per, coarse)
        lower = iota(tile.shape, 1) < tile.shape[1] // 2
        form = total(jnp.where(lower, tile, 0.0))
        norm = total(jnp.where(lower, 0.0, tile))
        step = norm / form
        norm_ref[...] = jnp.broadcast_to(norm, (8, 128))
        step_ref[...] = jnp.broadcast_to(step, (8, 128))
        frame_rows = iota((rows, lanes), 0)
        own_rows = (frame_rows >= HALO) & (frame_rows < rows - HALO)
        squares = jnp.zeros((rows, lanes), jnp.float32)
        remaining = {}
        for x in range(HALO, planes - HALO):
            value = jnp.where(own_rows, source[x] - step * image[x], 0.0)
            hold[x - HALO] = value
            remaining[x] = value
            squares = squares + value * value
        own_restricted(remaining, cond, faces, fine, squares, b1)
        for x in range(own_x):
            value = hold[x, HALO : HALO + own_y, :]
            own_ref[x] = value
            if x < HALO:
                first_ref[x] = value
            if x >= own_x - HALO:
                last_ref[x - own_x + HALO] = value

    strip = (HALO, own_y, lanes)
    return call(
        kernel,
        [strip, strip, (own_x, own_y, lanes), (coarse + 4, own_y // 2, lanes // 2)]
        + [(8, 128), (8, 128)],
        scratch_shapes + [(planes, rows, lanes), (own_x, rows, lanes)],
        inputs,
    )


def end_second(
    sizes, blocks, per, levels, fine, second, curved, cond, faces,
    source, remaining, combined, norm, step
):
    planes, rows, lanes = second.shape
    own_x, own_y = planes - 2 * HALO, rows - 2 * HALO
    coarse = own_x // 2
    scratch_shapes = coarse_scratch((coarse, own_y // 2, lanes // 2), sizes)
    inputs = (
        list(blocks) + list(levels) + list(fine)
        + [second, curved, cond] + list(faces) + [source, remaining, combined, norm, step]
    )

    def kernel(*refs):
        n = sizes[0]
        blocks = refs[:n]
        levels = refs[n : 8 + n]
        fine = refs[8 + n : 12 + n]
        second, curved, cond = refs[12 + n : 15 + n]
        faces = refs[15 + n : 19 + n]
        source, remaining, combined, norm, step = refs[19 + n : 24 + n]
        step_out, residual_out = refs[24 + n : 26 + n]
        *scratch, hold, hold_step = refs[26 + n :]
        image = image_planes(
            levels, fine, sizes, blocks, per, second, curved, cond, faces, scratch
        )
        form = total(summed_tiles(blocks, sizes, per, coarse))
        now = norm[0:1, 0:1] / form
        before = step[0:1, 0:1]
        for x in range(HALO, planes - HALO):
            hold[x - HALO] = now * image[x]
            hold_step[x - HALO] = before * source[x] + now * combined[x - HALO]
        for x in range(own_x):
            residual_out[x] = remaining[x] - hold[x, HALO : HALO + own_y, :]
            step_out[x] = hold_step[x, HALO : HALO + own_y, :]

    own = (own_x, own_y, lanes)
    hold = (own_x, rows, lanes)
    return call(
        kernel,
        [own, own],
        scratch_shapes + [(planes, rows, lanes), hold, hold],
        inputs,
    )


def edge_rows(own_x):
    starts, at = [], 0
    for x in range(own_x + 2 * HALO):
        starts.append(at)
        at += reach(HALO, own_x, x)
    return starts, -(-at // 8) * 8


def pack_edges(own, low, high):
    own_x, own_y, lanes = own.shape
    planes = own_x + 2 * HALO
    starts, rows = edge_rows(own_x)

    def kernel(own, low, high, first_ref, last_ref):
        for x in range(planes):
            near = reach(HALO, own_x, x)
            if near == 0:
                continue
            if x < HALO:
                ref, at = low, x
            elif x < HALO + own_x:
                ref, at = own, x - HALO
            else:
                ref, at = high, x - HALO - own_x
            row = starts[x]
            first_ref[row : row + near, :] = ref[at, :near, :]
            last_ref[row : row + near, :] = ref[at, own_y - near :, :]

    return call(kernel, [(rows, lanes)] * 2, [], [own, low, high])


def begin(own, low, high, before, after, cond, faces):
    own_x, own_y, lanes = own.shape
    planes, rows = own_x + 2 * HALO, own_y + 2 * HALO
    frame = (planes, rows, lanes)
    starts, _ = edge_rows(own_x)

    def kernel(
        own, low, high, before, after, cond, hux, huy, huz, nbu, direction, z_out
    ):
        for x in range(planes):
            if x < HALO:
                value = low[x]
            elif x < HALO + own_x:
                value = own[x - HALO]
            else:
                value = high[x - HALO - own_x]
            near = reach(HALO, own_x, x)
            if near < HALO:
                direction[x] = jnp.zeros((rows, lanes), jnp.float32)
            direction[x, HALO : HALO + own_y, :] = value
            if near:
                row = starts[x]
                direction[x, HALO - near : HALO, :] = before[row : row + near, :]
                end = HALO + own_y
                direction[x, end : end + near, :] = after[row : row + near, :]
        z = sensitivity_planes(
            lambda x: cond[x] * direction[x], hux, huy, huz, nbu, 1, planes - 1
        )
        zero = jnp.zeros((rows, lanes), jnp.float32)
        z_out[0] = zero
        z_out[planes - 1] = zero
        for x in z:
            z_out[x] = z[x]

    size = planes * rows * lanes
    return call(
        kernel,
        [frame, frame],
        [],
        [own, low, high, before, after, cond] + list(faces),
        cost=pl.CostEstimate(flops=20 * size, bytes_accessed=28 * size, transcendentals=0),
    )


def on_device(log_conductivity, state, gradient, prior_sample, sensor_cells, noise_precision):
    sizes = (lax.axis_size("gx"), lax.axis_size("gy"))
    cells_x, cells_y, cells_z = log_conductivity.shape
    coarse = (cells_x // 2, cells_y // 2, cells_z // 2)
    per = coarse[0] + 1

    weight = scattered(
        sizes, log_conductivity.shape, sensor_cells[None], noise_precision[None]
    )
    fields = (prior_sample, gradient, log_conductivity, state, weight)
    own_cond, even_edge, odd_edge, even_rows, odd_rows = prepare(fields)
    x_edges = exchange(even_edge, odd_edge, "gx")
    y_edges = exchange(even_rows, odd_rows, "gy")
    corners = exchange(*pack_corners(fields, *x_edges), "gy")
    (cond, hux, huy, huz, nbu, fx, fy, fz, rd, weight, source, z, b1) = setup(
        sizes, fields, x_edges, y_edges, corners, own_cond
    )
    faces = (hux, huy, huz, nbu)
    fine = (fx, fy, fz, rd)

    blocks = gathered(b1)
    curved = prior_part(sizes, source)
    levels = coarse_setup(sizes, blocks, coarse)
    b1, second, kept = middle(
        sizes, blocks, 2 * coarse[0], levels, fine, z, source, curved, weight, None
    )
    first, last, remaining, b1, norm, step = end_first(
        sizes, gathered(b1), per, levels, fine, second, curved, cond, faces, source
    )
    row = gathered_row(b1)
    low, high = rotate(last, "gx", 1), rotate(first, "gx", -1)
    first, last = pack_edges(remaining, low, high)
    row, first, last = lax.optimization_barrier((row, first, last))
    blocks = gathered_rows(row)
    before, after = rotate(last, "gy", 1), rotate(first, "gy", -1)
    direction, z = begin(remaining, low, high, before, after, cond, faces)
    b1, second, combined, curved, norm = middle(
        sizes, blocks, per + 3, levels, fine, z, direction, prior_part(sizes, direction), weight,
        (kept, source, norm, curved),
    )
    return tuple(
        end_second(
            sizes, gathered(b1), per, levels, fine, second, curved, cond,
            faces, source, remaining, combined, norm, step,
        )
    )


def solution(mesh):
    field = P(("ens", "gx"), "gy", None)
    sensors = P(("ens", "gx", "gy"))
    return jax.shard_map(
        on_device,
        mesh=mesh,
        in_specs=(field, field, field, field, sensors, sensors),
        out_specs=(field, field),
        check_vma=False,
    )
```

```python
import jax
import jax.numpy as jnp
from jax import lax
from jax.experimental import pallas as pl
from jax.experimental.pallas import tpu as pltpu
from jax.sharding import PartitionSpec as P


DAMPING = 0.8
KEPT = 0.2
PRIOR_MASS = 0.5
COARSE_SWEEPS = 6
HALO = 4
DEEP = 5
WIDE = 2
VMEM_LIMIT = 24 * 1024 * 1024
EXACT = lax.Precision.HIGHEST


def rotate(x, axis, shift):
    size = lax.axis_size(axis)
    return lax.ppermute(x, axis, [(i, (i + shift) % size) for i in range(size)])


def exchange(even_pairs, odd_pairs, axis):
    size = lax.axis_size(axis)
    inner = [(i, i) for i in (0, size - 1)]
    for i in range(1, size - 1, 2):
        inner += [(i, i + 1), (i + 1, i)]
    outer = [(i, i ^ 1) for i in range(size)]
    return lax.ppermute(even_pairs, axis, outer), lax.ppermute(odd_pairs, axis, inner)


def here():
    return lax.axis_index("gx"), lax.axis_index("gy")


def shifted(v, step, dim):
    size = v.shape[dim]
    return pltpu.roll(v, step % size, dim)


def dot(a, b):
    return lax.dot_general(
        a, b, (((1,), (0,)), ((), ())), precision=EXACT, preferred_element_type=jnp.float32
    )


def iota(shape, dim):
    return lax.broadcasted_iota(jnp.int32, shape, dim)


def total(tile):
    return jnp.sum(jnp.sum(tile, axis=1, keepdims=True), axis=0, keepdims=True)


def fold(plane):
    rows, lanes = plane.shape
    parts = [
        plane[r : r + 8, c : c + 128] for r in range(0, rows, 8) for c in range(0, lanes, 128)
    ]
    out = parts[0]
    for part in parts[1:]:
        out = out + part
    return out


def z_pairs(lanes):
    half = lanes // 2
    return (iota((lanes, half), 0) // 2 == iota((lanes, half), 1)).astype(jnp.float32)


def z_copies(lanes):
    return (iota((lanes, 2 * lanes), 0) == iota((lanes, 2 * lanes), 1) // 2).astype(jnp.float32)


def restrict_rows(planes, first_row, rows):
    extent = planes[0].shape[0]
    here = iota(planes[0].shape, 0)
    inside = (here >= first_row) & (here < first_row + rows)
    pick = (
        (iota((rows // 2, extent), 1) - first_row + 2) // 2 - 1 == iota((rows // 2, extent), 0)
    ).astype(jnp.float32)
    halves = []
    for x in range(0, len(planes), 2):
        pair = jnp.where(inside, planes[x] + planes[x + 1], 0.0)
        halves.append(dot(pick, pair))
    packed = dot(jnp.concatenate(halves, axis=0), z_pairs(planes[0].shape[1]))
    return packed.reshape(len(planes) // 2, rows // 2, packed.shape[1])


def swap_sum(v, dim, stride):
    even = (iota(v.shape, dim) // stride) % 2 == 0
    return v + jnp.where(even, shifted(v, -stride, dim), shifted(v, stride, dim))


def off_diagonal(v, low, high, fx, fx_high, fy, fz, step=1):
    out = fy * shifted(v, 1, 0) + shifted(fy * v, -1, 0)
    out = out + (fz * shifted(v, step, 1) + shifted(fz * v, -step, 1))
    if low is not None:
        out = out + fx * low
    if high is not None:
        out = out + fx_high * high
    return out


def coefficients(planes, scale, step, x_mask, y_mask, z_mask, outside):
    count = len(planes)
    faces = [None] * count
    for x in range(count):
        low = planes[x] if x == 0 else planes[x - 1]
        faces[x] = (scale * x_mask(x)) * (0.5 * (planes[x] + low))
    out = []
    for x in range(count):
        k = planes[x]
        fy = (scale * y_mask) * (0.5 * (k + shifted(k, 1, 0)))
        fz = (scale * z_mask) * (0.5 * (k + shifted(k, step, 1)))
        diag = (scale * outside(x)) * k + fy + shifted(fy, -1, 0) + fz + shifted(fz, -step, 1)
        diag = diag + faces[x]
        if x + 1 < count:
            diag = diag + faces[x + 1]
        out.append((faces[x], fy, fz, DAMPING / diag))
    return out


def flag(condition):
    return jnp.where(condition, 1.0, 0.0).astype(jnp.float32)


def placed_whole(refs, place, sizes, shape, per, first, whole_ref):
    planes, block_rows, _ = shape
    for s in range(sizes[0]):
        at_x = lax.rem(place[0] - s + sizes[0], sizes[0]) * planes
        for t in range(sizes[1]):
            at_y = lax.rem(place[1] - t + sizes[1], sizes[1])
            row = pl.multiple_of(at_y * block_rows, block_rows)
            for x in range(planes):
                block = refs[s][t * per + first + x]
                whole_ref[at_x + x, pl.ds(row, block_rows), :] = block


def placed_overlapping(refs, place, sizes, shape, per, room, whole_ref):
    planes, block_rows, lanes = shape
    sub = iota((block_rows, lanes), 0)
    last, first = sub == block_rows - 1, sub == 0

    def spots():
        for s in range(sizes[0]):
            at_x = lax.rem(place[0] - s + sizes[0], sizes[0]) * planes
            for t in range(sizes[1]):
                at_y = lax.rem(place[1] - t + sizes[1], sizes[1])
                row = pl.multiple_of(at_y * block_rows, block_rows)
                yield refs[s], t * per, at_x, row

    for ref, tile, at_x, row in spots():
        for x in range(planes):
            room[at_x + x + 1, pl.ds(row + block_rows, block_rows), :] = ref[tile + x]
    for ref, tile, at_x, row in spots():
        adds = [(0, 1, ref[tile + planes]), (planes + 1, 1, ref[tile + planes + 1])]
        pairs = [(x + 1, ref[tile + planes + 2], 2 * x) for x in range(planes)]
        pairs += [(0, ref[tile + planes + 3], 0), (planes + 1, ref[tile + planes + 3], 2)]
        for x, borders, at in pairs:
            before = shifted(borders, block_rows - 1 - at, 0)
            after = shifted(borders, -(at + 1), 0)
            adds.append((x, 0, jnp.where(last, before, 0.0)))
            adds.append((x, 2, jnp.where(first, after, 0.0)))
        spans = [
            (at_x + x, pl.ds(row + step * block_rows, block_rows)) for x, step, _ in adds
        ]
        values = [room[x, span, :] + add for (x, span), (_, _, add) in zip(spans, adds)]
        for (x, span), value in zip(spans, values):
            room[x, span, :] = value
    rows = block_rows * sizes[1]
    for x in range(planes * sizes[0]):
        whole_ref[x, :rows, :] = room[x + 1, block_rows : block_rows + rows, :]


def summed_tiles(refs, sizes, per, index):
    tile = None
    for s in range(sizes[0]):
        for t in range(sizes[1]):
            part = refs[s][t * per + index]
            tile = part if tile is None else tile + part
    return tile


def halved(one, two):
    lower = iota(one.shape, 1) < one.shape[1] // 2
    middle = one.shape[1] // 2
    return jnp.where(lower, one + shifted(one, middle, 1), two + shifted(two, middle, 1))


def row_pairs(ref, x, rows):
    return ref[x, pl.ds(0, rows // 2, stride=2), :] + ref[x, pl.ds(1, rows // 2, stride=2), :]


def coarse_correction(place, own, source, mid, pairs, level1, level2):
    fx1, fy1, fz1, rd1 = level1
    fx2, fy2, fz2, rd2 = level2
    planes, own_rows, lanes = own
    count = source.shape[0]
    rows = source.shape[1] - own_rows
    half = count // 2
    blank = jnp.zeros((own_rows, lanes), jnp.float32)
    for x in range(count):
        source[x, rows:, :] = blank
        mid[x, rows:, :] = blank
        mid[x, :rows, :] = rd1[x, :rows, :] * source[x, :rows, :]

    def off1(x):
        low = mid[x - 1, :rows, :] if x > 0 else None
        high = mid[x + 1, :rows, :] if x + 1 < count else None
        fx_high = fx1[x + 1, :rows, :] if x + 1 < count else None
        return off_diagonal(
            mid[x, :rows, :], low, high, fx1[x, :rows, :], fx_high,
            fy1[x, :rows, :], fz1[x, :rows, :],
        )

    for x in range(half):
        pair = KEPT * (source[2 * x, :rows, :] + source[2 * x + 1, :rows, :])
        pairs[x, :rows, :] = swap_sum(pair + (off1(2 * x) + off1(2 * x + 1)), 1, 1)
    coarse = [row_pairs(pairs, x, rows) for x in range(half)]
    iterate = [rd2[x] * coarse[x] for x in range(half)]
    for _ in range(COARSE_SWEEPS - 1):
        new = []
        for x in range(half):
            low = iterate[x - 1] if x > 0 else None
            high = iterate[x + 1] if x + 1 < half else None
            fx_high = fx2[x + 1] if x + 1 < half else None
            off = off_diagonal(iterate[x], low, high, fx2[x], fx_high, fy2[x], fz2[x], 2)
            new.append(KEPT * iterate[x] + rd2[x] * (coarse[x] + off))
        iterate = new
    for x in range(half):
        pairs[x, rows:, :] = blank
        pairs[x, pl.ds(0, rows // 2, stride=2), :] = iterate[x]
        pairs[x, pl.ds(1, rows // 2, stride=2), :] = iterate[x]

    start = jnp.clip((place[1] - 1) * own_rows, 0, max(rows - 2 * own_rows, 0))
    window = pl.ds(pl.multiple_of(start, own_rows), min(3 * own_rows, rows + own_rows))
    ends = HALO // 2
    at = [
        jnp.clip(place[0] * planes - ends + x, 0, count - 1) for x in range(-1, planes + 2 * ends + 1)
    ]
    value = [mid[a, window, :] + pairs[lax.div(a, 2), window, :] for a in at]
    first = place[1] * own_rows - ends - start
    frame_rows = 2 * (own_rows + 2 * ends)
    extent = value[0].shape[0]
    pick = flag(
        iota((frame_rows, extent), 1) == first + iota((frame_rows, extent), 0) // 2
    )
    parts = []
    for x in range(1, len(at) - 1):
        a = at[x]
        off = off_diagonal(
            value[x], value[x - 1], value[x + 1], fx1[a, window, :], fx1[a + 1, window, :],
            fy1[a, window, :], fz1[a, window, :],
        )
        smooth = KEPT * value[x] + rd1[a, window, :] * (source[a, window, :] + off)
        parts.append(dot(pick, smooth))
    wide = dot(jnp.concatenate(parts, axis=0), z_copies(lanes))
    return [wide[x * frame_rows : (x + 1) * frame_rows] for x in range(len(parts))]


def coarse_scratch(own, sizes):
    whole = (own[0] * sizes[0], own[1] * (sizes[1] + 1), own[2])
    return [whole, whole, (whole[0] // 2,) + whole[1:]]


def frame_masks(place, shape, pad, sizes):
    planes, rows, lanes = shape
    own_x, own_y = planes - 2 * pad, rows - 2 * pad
    all_x, all_y = own_x * sizes[0], own_y * sizes[1]
    base_x, base_y = place[0] * own_x - pad, place[1] * own_y - pad
    at_y = base_y + iota((rows, lanes), 0)
    at_z = iota((rows, lanes), 1)
    y_mask = flag((at_y >= 1) & (at_y < all_y))
    z_mask = flag(at_z >= 1)
    edges = flag(at_y == 0) + flag(at_y == all_y - 1) + flag(at_z == 0) + flag(at_z == lanes - 1)

    def x_mask(x):
        at = base_x + x
        return flag((at >= 1) & (at < all_x))

    def outside(x):
        at = base_x + x
        return edges + (flag(at == 0) + flag(at == all_x - 1))

    return x_mask, y_mask, z_mask, outside


def prior_rows(center, low, high, up, down, x_low, x_high, y_mask, z_mask, outside):
    y_next = shifted(y_mask, -1, 0)
    z_next = shifted(z_mask, -1, 1)
    out = (PRIOR_MASS + outside) * center + x_low * (center - low) + x_high * (center - high)
    out = out + y_mask * (center - up) + y_next * (center - down)
    out = out + z_mask * (center - shifted(center, 1, 1))
    return out + z_next * (center - shifted(center, -1, 1))


def fine_restricted(base, fields, fx, fy, fz, out_ref, first, own):
    planes = []
    for x in range(first, first + own):
        off = off_diagonal(
            fields[x], fields[x - 1], fields[x + 1], fx[x], fx[x + 1], fy[x], fz[x]
        )
        planes.append(KEPT * base[x] + off)
    rows = planes[0].shape[0]
    coarse = restrict_rows(planes, first, rows - 2 * first)
    for x in range(coarse.shape[0]):
        out_ref[x] = coarse[x]


def sensitivity_planes(q, hux, huy, huz, nbu, first, last):
    faces = {x: hux[x] * (q(x) + q(x - 1)) for x in range(first, last + 1)}
    out = {}
    for x in range(first, last):
        mid = q(x)
        along_y = huy[x] * (mid + shifted(mid, 1, 0))
        along_z = huz[x] * (mid + shifted(mid, 1, 1))
        z = faces[x] - faces[x + 1] + nbu[x] * mid
        z = z + (along_y - shifted(along_y, -1, 0))
        out[x] = z + (along_z - shifted(along_z, -1, 1))
    return out


def first_residual_stage(z, fx, fy, fz, rd, z_ref, out_ref, planes):
    for x in z:
        z_ref[x] = z[x]
    iterate = {x: rd[x] * z[x] for x in range(HALO - 1, planes - HALO + 1)}
    fine_restricted(z, iterate, fx, fy, fz, out_ref, HALO, planes - 2 * HALO)


def call(kernel, outs, scratch, inputs, limit=VMEM_LIMIT, cost=None):
    vmem = pl.BlockSpec(memory_space=pltpu.VMEM)
    return pl.pallas_call(
        kernel,
        out_shape=[jax.ShapeDtypeStruct(shape, jnp.float32) for shape in outs],
        in_specs=[vmem] * len(inputs),
        out_specs=[vmem] * len(outs),
        scratch_shapes=[pltpu.VMEM(shape, jnp.float32) for shape in scratch],
        compiler_params=pltpu.CompilerParams(vmem_limit_bytes=limit),
        cost_estimate=cost,
    )(*inputs)


def scattered(sizes, shape, cells, precision):
    own_x, own_y, lanes = shape
    all_rows = own_y * sizes[1]

    def kernel(cells, precision, out_ref):
        place = here()
        cell = cells[...]
        column = lax.div(cell, lanes)
        at_z = cell - column * lanes
        at_x = lax.div(column, all_rows)
        at_y = column - at_x * all_rows
        row = (at_x - place[0] * own_x) * own_y + (at_y - place[1] * own_y)
        count = cell.shape[1]
        picks = flag(iota((own_x * own_y, count), 0) == row)
        values = jnp.where(iota((lanes, count), 0) == at_z, precision[...], 0.0)
        weight = lax.dot_general(
            picks, values, (((1,), (1,)), ((), ())),
            precision=EXACT, preferred_element_type=jnp.float32,
        )
        for x in range(own_x):
            out_ref[x] = weight[x * own_y : (x + 1) * own_y]

    cost = pl.CostEstimate(flops=10**9, bytes_accessed=4096, transcendentals=0)
    return call(kernel, [shape], [], [cells, precision], cost=cost)[0]


def prepare(fields):
    own_x, own_y, lanes = fields[0].shape
    number = len(fields)
    starts, rows = setup_rows(own_x, True)

    def kernel(*refs):
        place = here()
        fields = refs[:number]
        coarse_ref, even_edge, odd_edge, even_rows, odd_rows = refs[number:]
        even_x = lax.rem(place[0], 2) == 0
        even_y = lax.rem(place[1], 2) == 0
        at = 0
        for index, depth in enumerate(FIELD_DEPTHS):
            ref = fields[index]
            start = own_x - depth
            even_start = jnp.where(even_x, start, 0)
            odd_start = jnp.where(even_x, 0, start)
            for x in range(depth):
                even_edge[at + x] = ref[even_start + x]
                odd_edge[at + x] = ref[odd_start + x]
            at += depth
            for x in range(own_x):
                first, last = ref[x, :depth, :], ref[x, own_y - depth :, :]
                row = starts[index, x + depth]
                even_rows[row : row + depth, :] = jnp.where(even_y, last, first)
                odd_rows[row : row + depth, :] = jnp.where(even_y, first, last)
        planes = [jnp.exp(fields[2][x]) for x in range(own_x)]
        coarse = restrict_rows(planes, 0, own_y)
        for x in range(coarse.shape[0]):
            coarse_ref[x] = coarse[x] * 0.125

    edge = (sum(FIELD_DEPTHS), own_y, lanes)
    return call(
        kernel,
        [(own_x // 2, own_y // 2, lanes // 2), edge, edge, (rows, lanes), (rows, lanes)],
        [],
        list(fields),
    )


def gathered_row(own):
    parts = [rotate(own, "gy", t) for t in range(1, lax.axis_size("gy"))]
    return jnp.concatenate([own] + parts, axis=0)


def gathered_rows(row):
    return [row] + [rotate(row, "gx", s) for s in range(1, lax.axis_size("gx"))]


def gathered(own):
    return gathered_rows(gathered_row(own))


FIELD_DEPTHS = (DEEP, HALO, HALO, HALO, WIDE)


def reach(depth, own_x, x):
    return depth - max(0, depth - x, x - depth - own_x + 1)


def setup_rows(own_x, own):
    starts, at = {}, 0
    for index, depth in enumerate(FIELD_DEPTHS):
        for x in range(own_x + 2 * depth):
            near = reach(depth, own_x, x)
            if near and own == (near == depth):
                starts[index, x] = at
                at += near
    return starts, -(-at // 8) * 8


def field_plane(fields, even_edge, odd_edge, even, index, x):
    depth = FIELD_DEPTHS[index]
    start = sum(FIELD_DEPTHS[:index])
    own = fields[index].shape[0]
    if x < depth:
        return jnp.where(even, odd_edge[start + x], even_edge[start + x])
    if x < depth + own:
        return fields[index][x - depth]
    at = start + x - depth - own
    return jnp.where(even, even_edge[at], odd_edge[at])


def pack_corners(fields, even_edge, odd_edge):
    own_x, own_y, lanes = fields[0].shape
    starts, rows = setup_rows(own_x, False)

    def kernel(even_edge, odd_edge, even_ref, odd_ref):
        place = here()
        even_x = lax.rem(place[0], 2) == 0
        even_y = lax.rem(place[1], 2) == 0
        for (index, x), at in starts.items():
            near = reach(FIELD_DEPTHS[index], own_x, x)
            plane = field_plane(fields, even_edge, odd_edge, even_x, index, x)
            first, last = plane[:near], plane[own_y - near :]
            even_ref[at : at + near, :] = jnp.where(even_y, last, first)
            odd_ref[at : at + near, :] = jnp.where(even_y, first, last)

    return call(kernel, [(rows, lanes)] * 2, [], [even_edge, odd_edge])


def setup(sizes, fields, x_edges, y_edges, corners, own_cond):
    own_x, own_y, lanes = fields[0].shape
    frame = (own_x + 2 * HALO, own_y + 2 * HALO, lanes)
    own_starts, _ = setup_rows(own_x, True)
    corner_starts, _ = setup_rows(own_x, False)
    number = len(fields)
    coarse = (own_x // 2, own_y // 2, lanes // 2)

    def kernel(*refs):
        place = here()
        fields = refs[:number]
        even_edge, odd_edge, *y_rows = refs[number : 6 + number]
        own_cond = refs[6 + number]
        even_x = lax.rem(place[0], 2) == 0
        even_y = lax.rem(place[1], 2) == 0
        outs = refs[7 + number : 20 + number]
        cond, hux, huy, huz, nbu, fx, fy, fz, rd, weight, source, z_out, b1 = outs
        prior, state, grad = refs[20 + number :]

        def assemble(index, ref, x_skip, first_row):
            depth = FIELD_DEPTHS[index]
            for x in range(own_x + 2 * depth):
                near = reach(depth, own_x, x)
                own_row = first_row + depth
                if near < depth or x_skip:
                    ref[x + x_skip] = jnp.zeros(ref.shape[1:], jnp.float32)
                ref[x + x_skip, own_row : own_row + own_y, :] = field_plane(
                    fields, even_edge, odd_edge, even_x, index, x
                )
                if near == 0:
                    continue
                if near == depth:
                    at, (even_rows, odd_rows) = own_starts[index, x], y_rows[:2]
                else:
                    at, (even_rows, odd_rows) = corner_starts[index, x], y_rows[2:]
                even_part, odd_part = even_rows[at : at + near, :], odd_rows[at : at + near, :]
                ref[x + x_skip, own_row - near : own_row, :] = jnp.where(
                    even_y, odd_part, even_part
                )
                end = own_row + own_y
                ref[x + x_skip, end : end + near, :] = jnp.where(even_y, even_part, odd_part)

        zero = jnp.zeros(frame[1:], jnp.float32)
        for x in range(HALO - WIDE):
            weight[x] = zero
            weight[frame[0] - 1 - x] = zero
        assemble(0, prior, 0, 0)
        assemble(1, grad, 0, 0)
        assemble(2, cond, 0, 0)
        assemble(3, state, 0, 0)
        assemble(4, weight, HALO - WIDE, HALO - WIDE)
        x_mask, y_mask, z_mask, outside = frame_masks(place, frame, HALO, sizes)
        planes, rows = frame[:2]
        for x in range(planes):
            center = prior[x + 1, 1 : 1 + rows, :]
            value = prior_rows(
                center,
                prior[x, 1 : 1 + rows, :],
                prior[x + 2, 1 : 1 + rows, :],
                prior[x + 1, 0:rows, :],
                prior[x + 1, 2 : 2 + rows, :],
                x_mask(x),
                x_mask(x + 1),
                y_mask,
                z_mask,
                outside(x),
            )
            source[x] = value - grad[x]
        for x in range(planes):
            cond[x] = jnp.exp(cond[x])
        for x in range(planes):
            u = state[x]
            if x > 0:
                hux[x] = (0.5 * x_mask(x)) * (u - state[x - 1])
            else:
                hux[x] = zero
            huy[x] = (0.5 * y_mask) * (u - shifted(u, 1, 0))
            huz[x] = (0.5 * z_mask) * (u - shifted(u, 1, 1))
            nbu[x] = outside(x) * u
        found = coefficients(
            [cond[x] for x in range(planes)], 1.0, 1, x_mask, y_mask, z_mask, outside
        )
        for x in range(planes):
            fx[x], fy[x], fz[x], rd[x] = found[x]
        z = sensitivity_planes(
            lambda x: cond[x] * source[x], hux, huy, huz, nbu, 1, planes - 1
        )
        z_out[0] = zero
        z_out[planes - 1] = zero
        first_residual_stage(z, fx, fy, fz, rd, z_out, b1, planes)
        for x in range(coarse[0]):
            b1[coarse[0] + x] = own_cond[x]

    deep = (own_x + 2 * DEEP, -(-(own_y + 2 * DEEP) // 8) * 8, lanes)
    return call(
        kernel,
        [frame] * 12 + [(2 * coarse[0],) + coarse[1:]],
        [deep, frame, frame],
        list(fields) + list(x_edges) + list(y_edges) + list(corners) + [own_cond],
    )


def coarse_setup(sizes, blocks, shape):
    planes, own_rows, lanes = shape
    count, rows = planes * sizes[0], own_rows * sizes[1]
    half = count // 2

    def kernel(*refs):
        blocks = refs[: sizes[0]]
        outs = refs[sizes[0] : 8 + sizes[0]]
        cond, pairs = refs[8 + sizes[0] :]
        placed_whole(blocks, here(), sizes, shape, 2 * planes, planes, cond)

        def level(values, scale, step, refs):
            number, extent = len(values), values[0].shape[0]
            at_y = iota((extent, lanes), 0)
            at_z = iota((extent, lanes), 1)
            edges = (
                flag(at_y == 0) + flag(at_y == extent - 1)
                + flag(at_z < step) + flag(at_z >= lanes - step)
            )

            def x_mask(x):
                return 1.0 if x > 0 else 0.0

            def outside(x):
                return edges + float((x == 0) + (x == number - 1))

            found = coefficients(
                values, scale, step, x_mask, flag(at_y >= 1), flag(at_z >= step), outside
            )
            for x in range(number):
                for ref, value in zip(refs, found[x]):
                    ref[x, :extent, :] = value

        level([cond[x] for x in range(count)], 2.0, 1, outs[:4])
        blank = jnp.zeros((own_rows, lanes), jnp.float32)
        for x in range(count):
            for ref in outs[:4]:
                ref[x, rows:, :] = blank
        outs[0][count] = jnp.zeros((rows + own_rows, lanes), jnp.float32)
        for x in range(half):
            pairs[x] = swap_sum(cond[2 * x] + cond[2 * x + 1], 1, 1)
        coarse = [0.125 * row_pairs(pairs, x, rows) for x in range(half)]
        level(coarse, 4.0, 2, outs[4:])

    padded = (count, rows + own_rows, lanes)
    return call(
        kernel,
        [(count + 1,) + padded[1:]] + [padded] * 3 + [(half, rows // 2, lanes)] * 4,
        [(count, rows, lanes), (half, rows, lanes)],
        list(blocks),
    )


def prior_part(sizes, direction):
    planes, rows, lanes = direction.shape

    def kernel(direction, out_ref):
        x_mask, y_mask, z_mask, outside = frame_masks(here(), direction.shape, HALO, sizes)
        for x in range(HALO, planes - HALO):
            center = direction[x]
            out_ref[x - HALO] = prior_rows(
                center,
                direction[x - 1],
                direction[x + 1],
                shifted(center, 1, 0),
                shifted(center, -1, 0),
                x_mask(x),
                x_mask(x + 1),
                y_mask,
                z_mask,
                outside(x),
            )

    size = planes * rows * lanes
    return call(
        kernel, [(planes - 2 * HALO, rows, lanes)], [], [direction],
        cost=pl.CostEstimate(flops=20 * size, bytes_accessed=8 * size, transcendentals=0),
    )[0]


def middle(sizes, blocks, per, levels, fine, z, direction, curved, weight, earlier):
    planes, rows, lanes = z.shape
    own_x = planes - 2 * HALO
    coarse = (own_x // 2, (rows - 2 * HALO) // 2, lanes // 2)
    first_time = earlier is None
    extra = [] if first_time else list(earlier)
    inputs = list(blocks) + list(levels) + list(fine) + [z, direction, curved, weight] + extra

    def kernel(*refs):
        at = 0

        def take(number):
            nonlocal at
            at += number
            return refs[at - number : at]

        place = here()
        blocks = take(sizes[0])
        levels = take(8)
        fx, fy, fz, rd = take(4)
        z, direction, curved, weight = take(4)
        old = take(len(extra))
        b1, second = take(2)
        if first_time:
            (kept,) = take(1)
        else:
            combined, curved_out, norm_ref = take(3)
        source, whole_mid, pairs, mid, *room = refs[at:]
        frame_rows = iota((rows, lanes), 0)
        own_rows = (frame_rows >= HALO) & (frame_rows < rows - HALO)
        if first_time:
            placed_whole(blocks, place, sizes, coarse, per, 0, source)
        else:
            placed_overlapping(blocks, place, sizes, coarse, per, room[0], source)
        correction = coarse_correction(
            place, coarse, source, whole_mid, pairs, levels[:4], levels[4:]
        )
        zero = jnp.zeros((rows, lanes), jnp.float32)
        forms = zero
        squares = zero
        if first_time:
            for x in range(own_x):
                d = direction[x + HALO]
                forms = forms + d * curved[x]
                squares = squares + d * d
        else:
            tile = summed_tiles(blocks, sizes, per, per - 1)
            norm = total(jnp.where(iota(tile.shape, 0) >= 4, tile, 0.0))
            ratio = norm / old[2][0:1, 0:1]
            for x in range(own_x):
                d = direction[x + HALO] + ratio * old[1][x + HALO]
                image = curved[x] + ratio * old[3][x]
                combined[x] = d
                curved_out[x] = image
                forms = forms + d * image
            norm_ref[...] = jnp.broadcast_to(norm, (8, 128))
        for x in range(1, planes - 1):
            mid[x] = rd[x] * z[x] + correction[x // 2]
        rights = {}
        for x in range(2, planes - 2):
            off = off_diagonal(mid[x], mid[x - 1], mid[x + 1], fx[x], fx[x + 1], fy[x], fz[x])
            change = KEPT * mid[x] + rd[x] * (z[x] + off)
            if first_time:
                kept[x] = change
            else:
                change = change + ratio * old[0][x]
            right = weight[x] * change
            second[x] = right
            rights[x] = right
            if HALO <= x < planes - HALO:
                forms = forms + right * change
        for x in (0, 1, planes - 2, planes - 1):
            second[x] = zero
            if first_time:
                kept[x] = zero
        iterate = {x: rd[x] * rights[x] for x in range(HALO - 1, planes - HALO + 1)}
        fine_restricted(rights, iterate, fx, fy, fz, b1, HALO, own_x)
        tile = fold(jnp.where(own_rows, forms, 0.0))
        if first_time:
            tile = halved(tile, fold(jnp.where(own_rows, squares, 0.0)))
        b1[coarse[0]] = tile

    frame = (planes, rows, lanes)
    own = (own_x, rows, lanes)
    margin = (coarse[0] * sizes[0] + 2, coarse[1] * (sizes[1] + 2), coarse[2])
    return call(
        kernel,
        [(coarse[0] + 1,) + coarse[1:], frame] + ([frame] if first_time else [own, own, (8, 128)]),
        coarse_scratch(coarse, sizes) + [frame] + ([] if first_time else [margin]),
        inputs,
    )


def image_planes(levels, fine, sizes, blocks, per, second, curved, cond, faces, scratch):
    fx, fy, fz, rd = fine
    hux, huy, huz, nbu = faces
    source, whole_mid, pairs, mid = scratch
    place = here()
    planes, rows, lanes = second.shape
    own = ((planes - 2 * HALO) // 2, (rows - 2 * HALO) // 2, lanes // 2)
    placed_whole(blocks, place, sizes, own, per, 0, source)
    correction = coarse_correction(
        place, own, source, whole_mid, pairs, levels[:4], levels[4:]
    )
    for x in range(2, planes - 2):
        mid[x] = rd[x] * second[x] + correction[x // 2]
    adjoint = {}
    for x in range(3, planes - 3):
        off = off_diagonal(mid[x], mid[x - 1], mid[x + 1], fx[x], fx[x + 1], fy[x], fz[x])
        adjoint[x] = KEPT * mid[x] + rd[x] * (second[x] + off)
    out = {}
    along_x = {
        x: hux[x] * (adjoint[x] - adjoint[x - 1]) for x in range(HALO, planes - HALO + 1)
    }
    for x in range(HALO, planes - HALO):
        p = adjoint[x]
        along_y = huy[x] * (p - shifted(p, 1, 0))
        along_z = huz[x] * (p - shifted(p, 1, 1))
        value = along_x[x] + along_x[x + 1] + nbu[x] * p
        value = value + (along_y + shifted(along_y, -1, 0))
        value = value + (along_z + shifted(along_z, -1, 1))
        out[x] = cond[x] * value + curved[x - HALO]
    return out


def own_restricted(direction, cond, faces, fine, squares, out_ref):
    fx, fy, fz, rd = fine
    hux, huy, huz, nbu = faces
    first, last = min(direction), max(direction)
    own_x = last - first + 1
    rows, lanes = direction[first].shape
    q = {x: cond[x] * direction[x] for x in direction}
    along_x = {first: hux[first] * q[first], last + 1: hux[last + 1] * q[last]}
    for x in range(first + 1, last + 1):
        along_x[x] = hux[x] * (q[x] + q[x - 1])
    z = {first - 1: -along_x[first], last + 1: along_x[last + 1]}
    for x in direction:
        mid = q[x]
        along_y = huy[x] * (mid + shifted(mid, 1, 0))
        along_z = huz[x] * (mid + shifted(mid, 1, 1))
        value = along_x[x] - along_x[x + 1] + nbu[x] * mid
        value = value + (along_y - shifted(along_y, -1, 0))
        z[x] = value + (along_z - shifted(along_z, -1, 1))
    iterate = {x: rd[x] * z[x] for x in z}
    planes = [fx[first - 1] * iterate[first - 1]]
    for x in range(first - 1, last + 2):
        off = off_diagonal(
            iterate[x], iterate.get(x - 1), iterate.get(x + 1),
            fx[x], fx[x + 1], fy[x], fz[x],
        )
        planes.append(KEPT * z[x] + off)
    planes[0] = fx[first - 1] * iterate[first - 1]
    planes.append(fx[last + 2] * iterate[last + 1])
    margin = HALO - 2
    block_rows = (rows - 2 * HALO) // 2
    target = iota((2 * block_rows, rows), 0)
    home = jnp.where(target < block_rows, target + 1, jnp.where(target == block_rows, 0, -9))
    home = jnp.where(target == block_rows + 1, block_rows + 1, home)
    here_row = iota((2 * block_rows, rows), 1)
    pick = flag((here_row >= margin + 2 * home) & (here_row < margin + 2 * home + 2))
    frame_rows = iota((rows, lanes), 0)
    inside = (frame_rows >= margin) & (frame_rows < rows - margin)
    halves = [
        dot(pick, jnp.where(inside, planes[x] + planes[x + 1], 0.0))
        for x in range(0, len(planes), 2)
    ]
    packed = dot(jnp.concatenate(halves, axis=0), z_pairs(lanes))
    tops, borders = [], []
    for x in range(len(halves)):
        at = 2 * block_rows * x
        tops.append(packed[at : at + block_rows])
        borders.append(packed[at + block_rows : at + 2 * block_rows])
    number = own_x // 2
    for x in range(number):
        out_ref[x] = tops[x + 1]
    out_ref[number] = tops[0]
    out_ref[number + 1] = tops[-1]
    pairs = borders[1]
    for x in range(1, number):
        pairs = pairs + shifted(borders[x + 1], 2 * x, 0)
    out_ref[number + 2] = pairs
    tile = fold(squares)
    tile = tile + shifted(tile, 4, 0)
    corners = borders[0] + shifted(borders[-1], 2, 0)
    out_ref[number + 3] = jnp.where(iota(tile.shape, 0) >= 4, tile, corners)


def end_first(sizes, blocks, per, levels, fine, second, curved, cond, faces, source):
    planes, rows, lanes = second.shape
    own_x, own_y = planes - 2 * HALO, rows - 2 * HALO
    coarse = own_x // 2
    scratch_shapes = coarse_scratch((coarse, own_y // 2, lanes // 2), sizes)
    inputs = (
        list(blocks) + list(levels) + list(fine)
        + [second, curved, cond] + list(faces) + [source]
    )

    def kernel(*refs):
        n = sizes[0]
        blocks = refs[:n]
        levels = refs[n : 8 + n]
        fine = refs[8 + n : 12 + n]
        second, curved, cond = refs[12 + n : 15 + n]
        faces = refs[15 + n : 19 + n]
        source = refs[19 + n]
        first_ref, last_ref, own_ref, b1, norm_ref, step_ref = refs[20 + n : 26 + n]
        *scratch, hold = refs[26 + n :]
        image = image_planes(
            levels, fine, sizes, blocks, per, second, curved, cond, faces, scratch
        )
        tile = summed_tiles(blocks, sizes, per, coarse)
        lower = iota(tile.shape, 1) < tile.shape[1] // 2
        form = total(jnp.where(lower, tile, 0.0))
        norm = total(jnp.where(lower, 0.0, tile))
        step = norm / form
        norm_ref[...] = jnp.broadcast_to(norm, (8, 128))
        step_ref[...] = jnp.broadcast_to(step, (8, 128))
        frame_rows = iota((rows, lanes), 0)
        own_rows = (frame_rows >= HALO) & (frame_rows < rows - HALO)
        squares = jnp.zeros((rows, lanes), jnp.float32)
        remaining = {}
        for x in range(HALO, planes - HALO):
            value = jnp.where(own_rows, source[x] - step * image[x], 0.0)
            hold[x - HALO] = value
            remaining[x] = value
            squares = squares + value * value
        own_restricted(remaining, cond, faces, fine, squares, b1)
        for x in range(own_x):
            value = hold[x, HALO : HALO + own_y, :]
            own_ref[x] = value
            if x < HALO:
                first_ref[x] = value
            if x >= own_x - HALO:
                last_ref[x - own_x + HALO] = value

    strip = (HALO, own_y, lanes)
    return call(
        kernel,
        [strip, strip, (own_x, own_y, lanes), (coarse + 4, own_y // 2, lanes // 2)]
        + [(8, 128), (8, 128)],
        scratch_shapes + [(planes, rows, lanes), (own_x, rows, lanes)],
        inputs,
    )


def end_second(
    sizes, blocks, per, levels, fine, second, curved, cond, faces,
    source, remaining, combined, norm, step
):
    planes, rows, lanes = second.shape
    own_x, own_y = planes - 2 * HALO, rows - 2 * HALO
    coarse = own_x // 2
    scratch_shapes = coarse_scratch((coarse, own_y // 2, lanes // 2), sizes)
    inputs = (
        list(blocks) + list(levels) + list(fine)
        + [second, curved, cond] + list(faces) + [source, remaining, combined, norm, step]
    )

    def kernel(*refs):
        n = sizes[0]
        blocks = refs[:n]
        levels = refs[n : 8 + n]
        fine = refs[8 + n : 12 + n]
        second, curved, cond = refs[12 + n : 15 + n]
        faces = refs[15 + n : 19 + n]
        source, remaining, combined, norm, step = refs[19 + n : 24 + n]
        step_out, residual_out = refs[24 + n : 26 + n]
        *scratch, hold, hold_step = refs[26 + n :]
        image = image_planes(
            levels, fine, sizes, blocks, per, second, curved, cond, faces, scratch
        )
        form = total(summed_tiles(blocks, sizes, per, coarse))
        now = norm[0:1, 0:1] / form
        before = step[0:1, 0:1]
        for x in range(HALO, planes - HALO):
            hold[x - HALO] = now * image[x]
            hold_step[x - HALO] = before * source[x] + now * combined[x - HALO]
        for x in range(own_x):
            residual_out[x] = remaining[x] - hold[x, HALO : HALO + own_y, :]
            step_out[x] = hold_step[x, HALO : HALO + own_y, :]

    own = (own_x, own_y, lanes)
    hold = (own_x, rows, lanes)
    return call(
        kernel,
        [own, own],
        scratch_shapes + [(planes, rows, lanes), hold, hold],
        inputs,
    )


def edge_rows(own_x):
    starts, at = [], 0
    for x in range(own_x + 2 * HALO):
        starts.append(at)
        at += reach(HALO, own_x, x)
    return starts, -(-at // 8) * 8


def pack_edges(own, low, high):
    own_x, own_y, lanes = own.shape
    planes = own_x + 2 * HALO
    starts, rows = edge_rows(own_x)

    def kernel(own, low, high, first_ref, last_ref):
        for x in range(planes):
            near = reach(HALO, own_x, x)
            if near == 0:
                continue
            if x < HALO:
                ref, at = low, x
            elif x < HALO + own_x:
                ref, at = own, x - HALO
            else:
                ref, at = high, x - HALO - own_x
            row = starts[x]
            first_ref[row : row + near, :] = ref[at, :near, :]
            last_ref[row : row + near, :] = ref[at, own_y - near :, :]

    return call(kernel, [(rows, lanes)] * 2, [], [own, low, high])


def begin(own, low, high, before, after, cond, faces):
    own_x, own_y, lanes = own.shape
    planes, rows = own_x + 2 * HALO, own_y + 2 * HALO
    frame = (planes, rows, lanes)
    starts, _ = edge_rows(own_x)

    def kernel(
        own, low, high, before, after, cond, hux, huy, huz, nbu, direction, z_out
    ):
        for x in range(planes):
            if x < HALO:
                value = low[x]
            elif x < HALO + own_x:
                value = own[x - HALO]
            else:
                value = high[x - HALO - own_x]
            near = reach(HALO, own_x, x)
            if near < HALO:
                direction[x] = jnp.zeros((rows, lanes), jnp.float32)
            direction[x, HALO : HALO + own_y, :] = value
            if near:
                row = starts[x]
                direction[x, HALO - near : HALO, :] = before[row : row + near, :]
                end = HALO + own_y
                direction[x, end : end + near, :] = after[row : row + near, :]
        z = sensitivity_planes(
            lambda x: cond[x] * direction[x], hux, huy, huz, nbu, 1, planes - 1
        )
        zero = jnp.zeros((rows, lanes), jnp.float32)
        z_out[0] = zero
        z_out[planes - 1] = zero
        for x in z:
            z_out[x] = z[x]

    size = planes * rows * lanes
    return call(
        kernel,
        [frame, frame],
        [],
        [own, low, high, before, after, cond] + list(faces),
        cost=pl.CostEstimate(flops=20 * size, bytes_accessed=28 * size, transcendentals=0),
    )


def on_device(log_conductivity, state, gradient, prior_sample, sensor_cells, noise_precision):
    sizes = (lax.axis_size("gx"), lax.axis_size("gy"))
    cells_x, cells_y, cells_z = log_conductivity.shape
    coarse = (cells_x // 2, cells_y // 2, cells_z // 2)
    per = coarse[0] + 1

    weight = scattered(
        sizes, log_conductivity.shape, sensor_cells[None], noise_precision[None]
    )
    fields = (prior_sample, gradient, log_conductivity, state, weight)
    own_cond, even_edge, odd_edge, even_rows, odd_rows = prepare(fields)
    x_edges = exchange(even_edge, odd_edge, "gx")
    y_edges = exchange(even_rows, odd_rows, "gy")
    corners = exchange(*pack_corners(fields, *x_edges), "gy")
    (cond, hux, huy, huz, nbu, fx, fy, fz, rd, weight, source, z, b1) = setup(
        sizes, fields, x_edges, y_edges, corners, own_cond
    )
    faces = (hux, huy, huz, nbu)
    fine = (fx, fy, fz, rd)

    blocks = gathered(b1)
    curved = prior_part(sizes, source)
    levels = coarse_setup(sizes, blocks, coarse)
    b1, second, kept = middle(
        sizes, blocks, 2 * coarse[0], levels, fine, z, source, curved, weight, None
    )
    first, last, remaining, b1, norm, step = end_first(
        sizes, gathered(b1), per, levels, fine, second, curved, cond, faces, source
    )
    row = gathered_row(b1)
    low = rotate(last, "gx", 1)
    high = rotate(first, "gx", -1)
    first, last = pack_edges(remaining, low, high)
    row, first, last = lax.optimization_barrier((row, first, last))
    blocks = gathered_rows(row)
    before = rotate(last, "gy", 1)
    after = rotate(first, "gy", -1)
    direction, z = begin(remaining, low, high, before, after, cond, faces)
    b1, second, combined, curved, norm = middle(
        sizes, blocks, per + 3, levels, fine, z, direction, prior_part(sizes, direction), weight,
        (kept, source, norm, curved),
    )
    return tuple(
        end_second(
            sizes, gathered(b1), per, levels, fine, second, curved, cond,
            faces, source, remaining, combined, norm, step,
        )
    )


def solution(mesh):
    field = P(("ens", "gx"), "gy", None)
    sensors = P(("ens", "gx", "gy"))

    return jax.shard_map(
        on_device,
        mesh=mesh,
        in_specs=(field, field, field, field, sensors, sensors),
        out_specs=(field, field),
        check_vma=False,
    )
```

```python
import jax
import jax.numpy as jnp
from jax import lax
from jax.experimental import pallas as pl
from jax.experimental.pallas import tpu as pltpu
from jax.sharding import PartitionSpec as P


DAMPING = 0.8
KEPT = 0.2
PRIOR_MASS = 0.5
COARSE_SWEEPS = 6
HALO = 4
DEEP = 5
WIDE = 2
VMEM_LIMIT = 24 * 1024 * 1024


def rotate(x, axis, shift):
    size = lax.axis_size(axis)
    return lax.ppermute(x, axis, [(i, (i + shift) % size) for i in range(size)])


def exchange(even_pairs, odd_pairs, axis):
    size = lax.axis_size(axis)
    inner = [(i, i) for i in (0, size - 1)]
    for i in range(1, size - 1, 2):
        inner += [(i, i + 1), (i + 1, i)]
    outer = [(i, i ^ 1) for i in range(size)]
    return lax.ppermute(even_pairs, axis, outer), lax.ppermute(odd_pairs, axis, inner)


def here():
    return lax.axis_index("gx"), lax.axis_index("gy")


def shifted(v, step, dim):
    size = v.shape[dim]
    return pltpu.roll(v, step % size, dim)


def pieces(v):
    high = v.astype(jnp.bfloat16)
    rest = v - high.astype(jnp.float32)
    middle = rest.astype(jnp.bfloat16)
    return high, middle, (rest - middle.astype(jnp.float32)).astype(jnp.bfloat16)


def product(a, b, contract):
    dims = ((contract[:1], contract[1:]), ((), ()))
    return lax.dot_general(a, b, dims, preferred_element_type=jnp.float32)


def pick_rows(picks, v, contract=(1, 0)):
    picks = picks.astype(jnp.bfloat16)
    high, middle, low = (product(picks, part, contract) for part in pieces(v))
    return high + (middle + low)


def pick_lanes(v, picks):
    picks = picks.astype(jnp.bfloat16)
    joined = jnp.concatenate(pieces(v), axis=1)
    return product(joined, jnp.concatenate([picks] * 3, axis=0), (1, 0))


def iota(shape, dim):
    return lax.broadcasted_iota(jnp.int32, shape, dim)


def total(tile):
    return jnp.sum(jnp.sum(tile, axis=1, keepdims=True), axis=0, keepdims=True)


def fold(plane):
    rows, lanes = plane.shape
    parts = [
        plane[r : r + 8, c : c + 128] for r in range(0, rows, 8) for c in range(0, lanes, 128)
    ]
    out = parts[0]
    for part in parts[1:]:
        out = out + part
    return out


def z_pairs(lanes):
    half = lanes // 2
    return (iota((lanes, half), 0) // 2 == iota((lanes, half), 1)).astype(jnp.float32)


def z_copies(lanes):
    return (iota((lanes, 2 * lanes), 0) == iota((lanes, 2 * lanes), 1) // 2).astype(jnp.float32)


def restrict_rows(planes, first_row, rows):
    extent = planes[0].shape[0]
    here = iota(planes[0].shape, 0)
    inside = (here >= first_row) & (here < first_row + rows)
    pick = (
        (iota((rows // 2, extent), 1) - first_row + 2) // 2 - 1 == iota((rows // 2, extent), 0)
    ).astype(jnp.float32)
    halves = []
    for x in range(0, len(planes), 2):
        pair = jnp.where(inside, planes[x] + planes[x + 1], 0.0)
        halves.append(pick_rows(pick, pair))
    packed = pick_lanes(jnp.concatenate(halves, axis=0), z_pairs(planes[0].shape[1]))
    return packed.reshape(len(planes) // 2, rows // 2, packed.shape[1])


def swap_sum(v, dim, stride):
    even = (iota(v.shape, dim) // stride) % 2 == 0
    return v + jnp.where(even, shifted(v, -stride, dim), shifted(v, stride, dim))


def off_diagonal(v, low, high, fx, fx_high, fy, fz, step=1):
    out = fy * shifted(v, 1, 0) + shifted(fy * v, -1, 0)
    out = out + (fz * shifted(v, step, 1) + shifted(fz * v, -step, 1))
    if low is not None:
        out = out + fx * low
    if high is not None:
        out = out + fx_high * high
    return out


def coefficients(planes, scale, step, x_mask, y_mask, z_mask, outside):
    count = len(planes)
    faces = [None] * count
    for x in range(count):
        low = planes[x] if x == 0 else planes[x - 1]
        faces[x] = (scale * x_mask(x)) * (0.5 * (planes[x] + low))
    out = []
    for x in range(count):
        k = planes[x]
        fy = (scale * y_mask) * (0.5 * (k + shifted(k, 1, 0)))
        fz = (scale * z_mask) * (0.5 * (k + shifted(k, step, 1)))
        diag = (scale * outside(x)) * k + fy + shifted(fy, -1, 0) + fz + shifted(fz, -step, 1)
        diag = diag + faces[x]
        if x + 1 < count:
            diag = diag + faces[x + 1]
        out.append((faces[x], fy, fz, DAMPING / diag))
    return out


def flag(condition):
    return jnp.where(condition, 1.0, 0.0).astype(jnp.float32)


def placed_whole(refs, place, sizes, shape, per, first, whole_ref):
    planes, block_rows, _ = shape
    for s in range(sizes[0]):
        at_x = lax.rem(place[0] - s + sizes[0], sizes[0]) * planes
        for t in range(sizes[1]):
            at_y = lax.rem(place[1] - t + sizes[1], sizes[1])
            row = pl.multiple_of(at_y * block_rows, block_rows)
            for x in range(planes):
                block = refs[s][t * per + first + x]
                whole_ref[at_x + x, pl.ds(row, block_rows), :] = block


def placed_overlapping(refs, place, sizes, shape, per, room, whole_ref):
    planes, block_rows, lanes = shape
    sub = iota((block_rows, lanes), 0)
    last, first = sub == block_rows - 1, sub == 0

    def spots():
        for s in range(sizes[0]):
            at_x = lax.rem(place[0] - s + sizes[0], sizes[0]) * planes
            for t in range(sizes[1]):
                at_y = lax.rem(place[1] - t + sizes[1], sizes[1])
                row = pl.multiple_of(at_y * block_rows, block_rows)
                yield refs[s], t * per, at_x, row

    for ref, tile, at_x, row in spots():
        for x in range(planes):
            room[at_x + x + 1, pl.ds(row + block_rows, block_rows), :] = ref[tile + x]
    for ref, tile, at_x, row in spots():
        adds = [(0, 1, ref[tile + planes]), (planes + 1, 1, ref[tile + planes + 1])]
        pairs = [(x + 1, ref[tile + planes + 2], 2 * x) for x in range(planes)]
        pairs += [(0, ref[tile + planes + 3], 0), (planes + 1, ref[tile + planes + 3], 2)]
        for x, borders, at in pairs:
            before = shifted(borders, block_rows - 1 - at, 0)
            after = shifted(borders, -(at + 1), 0)
            adds.append((x, 0, jnp.where(last, before, 0.0)))
            adds.append((x, 2, jnp.where(first, after, 0.0)))
        spans = [
            (at_x + x, pl.ds(row + step * block_rows, block_rows)) for x, step, _ in adds
        ]
        values = [room[x, span, :] + add for (x, span), (_, _, add) in zip(spans, adds)]
        for (x, span), value in zip(spans, values):
            room[x, span, :] = value
    rows = block_rows * sizes[1]
    for x in range(planes * sizes[0]):
        whole_ref[x, :rows, :] = room[x + 1, block_rows : block_rows + rows, :]


def summed_tiles(refs, sizes, per, index):
    tile = None
    for s in range(sizes[0]):
        for t in range(sizes[1]):
            part = refs[s][t * per + index]
            tile = part if tile is None else tile + part
    return tile


def halved(one, two):
    lower = iota(one.shape, 1) < one.shape[1] // 2
    middle = one.shape[1] // 2
    return jnp.where(lower, one + shifted(one, middle, 1), two + shifted(two, middle, 1))


def row_pairs(ref, x, rows):
    return ref[x, pl.ds(0, rows // 2, stride=2), :] + ref[x, pl.ds(1, rows // 2, stride=2), :]


def coarse_correction(place, own, source, mid, pairs, level1, level2):
    fx1, fy1, fz1, rd1 = level1
    fx2, fy2, fz2, rd2 = level2
    planes, own_rows, lanes = own
    count = source.shape[0]
    rows = source.shape[1] - own_rows
    half = count // 2
    blank = jnp.zeros((own_rows, lanes), jnp.float32)
    for x in range(count):
        source[x, rows:, :] = blank
        mid[x, rows:, :] = blank
        mid[x, :rows, :] = rd1[x, :rows, :] * source[x, :rows, :]

    def off1(x):
        low = mid[x - 1, :rows, :] if x > 0 else None
        high = mid[x + 1, :rows, :] if x + 1 < count else None
        fx_high = fx1[x + 1, :rows, :] if x + 1 < count else None
        return off_diagonal(
            mid[x, :rows, :], low, high, fx1[x, :rows, :], fx_high,
            fy1[x, :rows, :], fz1[x, :rows, :],
        )

    for x in range(half):
        pair = KEPT * (source[2 * x, :rows, :] + source[2 * x + 1, :rows, :])
        pairs[x, :rows, :] = swap_sum(pair + (off1(2 * x) + off1(2 * x + 1)), 1, 1)
    coarse = [row_pairs(pairs, x, rows) for x in range(half)]
    iterate = [rd2[x] * coarse[x] for x in range(half)]
    for _ in range(COARSE_SWEEPS - 1):
        new = []
        for x in range(half):
            low = iterate[x - 1] if x > 0 else None
            high = iterate[x + 1] if x + 1 < half else None
            fx_high = fx2[x + 1] if x + 1 < half else None
            off = off_diagonal(iterate[x], low, high, fx2[x], fx_high, fy2[x], fz2[x], 2)
            new.append(KEPT * iterate[x] + rd2[x] * (coarse[x] + off))
        iterate = new
    for x in range(half):
        pairs[x, rows:, :] = blank
        pairs[x, pl.ds(0, rows // 2, stride=2), :] = iterate[x]
        pairs[x, pl.ds(1, rows // 2, stride=2), :] = iterate[x]

    start = jnp.clip((place[1] - 1) * own_rows, 0, max(rows - 2 * own_rows, 0))
    window = pl.ds(pl.multiple_of(start, own_rows), min(3 * own_rows, rows + own_rows))
    ends = HALO // 2
    at = [
        jnp.clip(place[0] * planes - ends + x, 0, count - 1) for x in range(-1, planes + 2 * ends + 1)
    ]
    value = [mid[a, window, :] + pairs[lax.div(a, 2), window, :] for a in at]
    first = place[1] * own_rows - ends - start
    frame_rows = 2 * (own_rows + 2 * ends)
    extent = value[0].shape[0]
    pick = flag(
        iota((frame_rows, extent), 1) == first + iota((frame_rows, extent), 0) // 2
    )
    parts = []
    for x in range(1, len(at) - 1):
        a = at[x]
        off = off_diagonal(
            value[x], value[x - 1], value[x + 1], fx1[a, window, :], fx1[a + 1, window, :],
            fy1[a, window, :], fz1[a, window, :],
        )
        smooth = KEPT * value[x] + rd1[a, window, :] * (source[a, window, :] + off)
        parts.append(pick_rows(pick, smooth))
    wide = pick_lanes(jnp.concatenate(parts, axis=0), z_copies(lanes))
    return [wide[x * frame_rows : (x + 1) * frame_rows] for x in range(len(parts))]


def pairs_room(frame):
    return (frame[2] // 128, frame[0] // 2 - HALO, frame[1], 128)


def coarse_scratch(own, sizes):
    whole = (own[0] * sizes[0], own[1] * (sizes[1] + 1), own[2])
    return [whole, whole, (whole[0] // 2,) + whole[1:]]


def frame_masks(place, shape, pad, sizes):
    planes, rows, lanes = shape
    own_x, own_y = planes - 2 * pad, rows - 2 * pad
    all_x, all_y = own_x * sizes[0], own_y * sizes[1]
    base_x, base_y = place[0] * own_x - pad, place[1] * own_y - pad
    at_y = base_y + iota((rows, lanes), 0)
    at_z = iota((rows, lanes), 1)
    y_mask = flag((at_y >= 1) & (at_y < all_y))
    z_mask = flag(at_z >= 1)
    edges = flag(at_y == 0) + flag(at_y == all_y - 1) + flag(at_z == 0) + flag(at_z == lanes - 1)

    def x_mask(x):
        at = base_x + x
        return flag((at >= 1) & (at < all_x))

    def outside(x):
        at = base_x + x
        return edges + (flag(at == 0) + flag(at == all_x - 1))

    return x_mask, y_mask, z_mask, outside


def prior_rows(center, low, high, up, down, x_low, x_high, y_mask, z_mask, outside):
    y_next = shifted(y_mask, -1, 0)
    z_next = shifted(z_mask, -1, 1)
    out = (PRIOR_MASS + outside) * center + x_low * (center - low) + x_high * (center - high)
    out = out + y_mask * (center - up) + y_next * (center - down)
    out = out + z_mask * (center - shifted(center, 1, 1))
    return out + z_next * (center - shifted(center, -1, 1))


def fine_restricted(base, fields, fx, fy, fz, out_ref, first, own):
    planes = []
    for x in range(first, first + own):
        off = off_diagonal(
            fields[x], fields[x - 1], fields[x + 1], fx[x], fx[x + 1], fy[x], fz[x]
        )
        planes.append(KEPT * base[x] + off)
    rows = planes[0].shape[0]
    coarse = restrict_rows(planes, first, rows - 2 * first)
    for x in range(coarse.shape[0]):
        out_ref[x] = coarse[x]


def fine_restricted_by_rows(base, fields, fx, fy, fz, out_ref, room, first, own):
    halves = []
    for x in range(first, first + own, 2):
        pair = 0.0
        for at in (x, x + 1):
            off = off_diagonal(
                fields[at], fields[at - 1], fields[at + 1],
                fx[at], fx[at + 1], fy[at], fz[at],
            )
            pair = pair + (KEPT * base[at] + off)
        rows, lanes = pair.shape
        for part in range(0, lanes, 128):
            room[part // 128, (x - first) // 2] = pair[:, part : part + 128]
        number = rows // 2 - first
        halves.append(
            jnp.concatenate(
                [
                    room[part, (x - first) // 2, pl.ds(first, number, stride=2), :]
                    + room[part, (x - first) // 2, pl.ds(first + 1, number, stride=2), :]
                    for part in range(lanes // 128)
                ],
                axis=1,
            )
        )
    packed = pick_lanes(jnp.concatenate(halves, axis=0), z_pairs(lanes))
    for x in range(len(halves)):
        out_ref[x] = packed[x * number : (x + 1) * number]


def sensitivity_planes(q, hux, huy, huz, nbu, first, last):
    faces = {x: hux[x] * (q(x) + q(x - 1)) for x in range(first, last + 1)}
    out = {}
    for x in range(first, last):
        mid = q(x)
        along_y = huy[x] * (mid + shifted(mid, 1, 0))
        along_z = huz[x] * (mid + shifted(mid, 1, 1))
        z = faces[x] - faces[x + 1] + nbu[x] * mid
        z = z + (along_y - shifted(along_y, -1, 0))
        out[x] = z + (along_z - shifted(along_z, -1, 1))
    return out


def first_residual_stage(z, fx, fy, fz, rd, z_ref, out_ref, planes):
    for x in z:
        z_ref[x] = z[x]
    iterate = {x: rd[x] * z[x] for x in range(HALO - 1, planes - HALO + 1)}
    fine_restricted(z, iterate, fx, fy, fz, out_ref, HALO, planes - 2 * HALO)


def call(kernel, outs, scratch, inputs, limit=VMEM_LIMIT, cost=None):
    vmem = pl.BlockSpec(memory_space=pltpu.VMEM)
    return pl.pallas_call(
        kernel,
        out_shape=[jax.ShapeDtypeStruct(shape, jnp.float32) for shape in outs],
        in_specs=[vmem] * len(inputs),
        out_specs=[vmem] * len(outs),
        scratch_shapes=[pltpu.VMEM(shape, jnp.float32) for shape in scratch],
        compiler_params=pltpu.CompilerParams(vmem_limit_bytes=limit),
        cost_estimate=cost,
    )(*inputs)


def scattered(sizes, shape, cells, precision):
    own_x, own_y, lanes = shape
    all_rows = own_y * sizes[1]

    def kernel(cells, precision, out_ref):
        place = here()
        cell = cells[...]
        column = lax.div(cell, lanes)
        at_z = cell - column * lanes
        at_x = lax.div(column, all_rows)
        at_y = column - at_x * all_rows
        row = (at_x - place[0] * own_x) * own_y + (at_y - place[1] * own_y)
        count = cell.shape[1]
        picks = flag(iota((own_x * own_y, count), 0) == row)
        values = jnp.where(iota((lanes, count), 0) == at_z, precision[...], 0.0)
        weight = pick_rows(picks, values, (1, 1))
        for x in range(own_x):
            out_ref[x] = weight[x * own_y : (x + 1) * own_y]

    cost = pl.CostEstimate(flops=10**9, bytes_accessed=4096, transcendentals=0)
    return call(kernel, [shape], [], [cells, precision], cost=cost)[0]


def prepare(fields):
    own_x, own_y, lanes = fields[0].shape
    number = len(fields)
    starts, rows = setup_rows(own_x, True)

    def kernel(*refs):
        place = here()
        fields = refs[:number]
        coarse_ref, even_edge, odd_edge, even_rows, odd_rows = refs[number:]
        even_x = lax.rem(place[0], 2) == 0
        even_y = lax.rem(place[1], 2) == 0
        at = 0
        for index, depth in enumerate(FIELD_DEPTHS):
            ref = fields[index]
            start = own_x - depth
            even_start = jnp.where(even_x, start, 0)
            odd_start = jnp.where(even_x, 0, start)
            for x in range(depth):
                even_edge[at + x] = ref[even_start + x]
                odd_edge[at + x] = ref[odd_start + x]
            at += depth
            for x in range(own_x):
                first, last = ref[x, :depth, :], ref[x, own_y - depth :, :]
                row = starts[index, x + depth]
                even_rows[row : row + depth, :] = jnp.where(even_y, last, first)
                odd_rows[row : row + depth, :] = jnp.where(even_y, first, last)
        planes = [jnp.exp(fields[2][x]) for x in range(own_x)]
        coarse = restrict_rows(planes, 0, own_y)
        for x in range(coarse.shape[0]):
            coarse_ref[x] = coarse[x] * 0.125

    edge = (sum(FIELD_DEPTHS), own_y, lanes)
    return call(
        kernel,
        [(own_x // 2, own_y // 2, lanes // 2), edge, edge, (rows, lanes), (rows, lanes)],
        [],
        list(fields),
    )


def gathered_row(own):
    parts = [rotate(own, "gy", t) for t in range(1, lax.axis_size("gy"))]
    return jnp.concatenate([own] + parts, axis=0)


def gathered_rows(row):
    return [row] + [rotate(row, "gx", s) for s in range(1, lax.axis_size("gx"))]


def gathered(own):
    return gathered_rows(gathered_row(own))


FIELD_DEPTHS = (DEEP, HALO, HALO, HALO, WIDE)


def reach(depth, own_x, x):
    return depth - max(0, depth - x, x - depth - own_x + 1)


def setup_rows(own_x, own):
    starts, at = {}, 0
    for index, depth in enumerate(FIELD_DEPTHS):
        for x in range(own_x + 2 * depth):
            near = reach(depth, own_x, x)
            if near and own == (near == depth):
                starts[index, x] = at
                at += near
    return starts, -(-at // 8) * 8


def field_plane(fields, even_edge, odd_edge, even, index, x):
    depth = FIELD_DEPTHS[index]
    start = sum(FIELD_DEPTHS[:index])
    own = fields[index].shape[0]
    if x < depth:
        return jnp.where(even, odd_edge[start + x], even_edge[start + x])
    if x < depth + own:
        return fields[index][x - depth]
    at = start + x - depth - own
    return jnp.where(even, even_edge[at], odd_edge[at])


def pack_corners(fields, even_edge, odd_edge):
    own_x, own_y, lanes = fields[0].shape
    starts, rows = setup_rows(own_x, False)

    def kernel(even_edge, odd_edge, even_ref, odd_ref):
        place = here()
        even_x = lax.rem(place[0], 2) == 0
        even_y = lax.rem(place[1], 2) == 0
        for (index, x), at in starts.items():
            near = reach(FIELD_DEPTHS[index], own_x, x)
            plane = field_plane(fields, even_edge, odd_edge, even_x, index, x)
            first, last = plane[:near], plane[own_y - near :]
            even_ref[at : at + near, :] = jnp.where(even_y, last, first)
            odd_ref[at : at + near, :] = jnp.where(even_y, first, last)

    return call(kernel, [(rows, lanes)] * 2, [], [even_edge, odd_edge])


def setup(sizes, fields, x_edges, y_edges, corners, own_cond):
    own_x, own_y, lanes = fields[0].shape
    frame = (own_x + 2 * HALO, own_y + 2 * HALO, lanes)
    own_starts, _ = setup_rows(own_x, True)
    corner_starts, _ = setup_rows(own_x, False)
    number = len(fields)
    coarse = (own_x // 2, own_y // 2, lanes // 2)

    def kernel(*refs):
        place = here()
        fields = refs[:number]
        even_edge, odd_edge, *y_rows = refs[number : 6 + number]
        own_cond = refs[6 + number]
        even_x = lax.rem(place[0], 2) == 0
        even_y = lax.rem(place[1], 2) == 0
        outs = refs[7 + number : 20 + number]
        cond, hux, huy, huz, nbu, fx, fy, fz, rd, weight, source, z_out, b1 = outs
        prior, state, grad = refs[20 + number :]

        def assemble(index, ref, x_skip, first_row):
            depth = FIELD_DEPTHS[index]
            for x in range(own_x + 2 * depth):
                near = reach(depth, own_x, x)
                own_row = first_row + depth
                if near < depth or x_skip:
                    ref[x + x_skip] = jnp.zeros(ref.shape[1:], jnp.float32)
                ref[x + x_skip, own_row : own_row + own_y, :] = field_plane(
                    fields, even_edge, odd_edge, even_x, index, x
                )
                if near == 0:
                    continue
                if near == depth:
                    at, (even_rows, odd_rows) = own_starts[index, x], y_rows[:2]
                else:
                    at, (even_rows, odd_rows) = corner_starts[index, x], y_rows[2:]
                even_part, odd_part = even_rows[at : at + near, :], odd_rows[at : at + near, :]
                ref[x + x_skip, own_row - near : own_row, :] = jnp.where(
                    even_y, odd_part, even_part
                )
                end = own_row + own_y
                ref[x + x_skip, end : end + near, :] = jnp.where(even_y, even_part, odd_part)

        zero = jnp.zeros(frame[1:], jnp.float32)
        for x in range(HALO - WIDE):
            weight[x] = zero
            weight[frame[0] - 1 - x] = zero
        assemble(0, prior, 0, 0)
        assemble(1, grad, 0, 0)
        assemble(2, cond, 0, 0)
        assemble(3, state, 0, 0)
        assemble(4, weight, HALO - WIDE, HALO - WIDE)
        x_mask, y_mask, z_mask, outside = frame_masks(place, frame, HALO, sizes)
        planes, rows = frame[:2]
        for x in range(planes):
            center = prior[x + 1, 1 : 1 + rows, :]
            value = prior_rows(
                center,
                prior[x, 1 : 1 + rows, :],
                prior[x + 2, 1 : 1 + rows, :],
                prior[x + 1, 0:rows, :],
                prior[x + 1, 2 : 2 + rows, :],
                x_mask(x),
                x_mask(x + 1),
                y_mask,
                z_mask,
                outside(x),
            )
            source[x] = value - grad[x]
        for x in range(planes):
            cond[x] = jnp.exp(cond[x])
        for x in range(planes):
            u = state[x]
            if x > 0:
                hux[x] = (0.5 * x_mask(x)) * (u - state[x - 1])
            else:
                hux[x] = zero
            huy[x] = (0.5 * y_mask) * (u - shifted(u, 1, 0))
            huz[x] = (0.5 * z_mask) * (u - shifted(u, 1, 1))
            nbu[x] = outside(x) * u
        found = coefficients(
            [cond[x] for x in range(planes)], 1.0, 1, x_mask, y_mask, z_mask, outside
        )
        for x in range(planes):
            fx[x], fy[x], fz[x], rd[x] = found[x]
        z = sensitivity_planes(
            lambda x: cond[x] * source[x], hux, huy, huz, nbu, 1, planes - 1
        )
        z_out[0] = zero
        z_out[planes - 1] = zero
        first_residual_stage(z, fx, fy, fz, rd, z_out, b1, planes)
        for x in range(coarse[0]):
            b1[coarse[0] + x] = own_cond[x]

    deep = (own_x + 2 * DEEP, -(-(own_y + 2 * DEEP) // 8) * 8, lanes)
    return call(
        kernel,
        [frame] * 12 + [(2 * coarse[0],) + coarse[1:]],
        [deep, frame, frame],
        list(fields) + list(x_edges) + list(y_edges) + list(corners) + [own_cond],
    )


def coarse_setup(sizes, blocks, shape):
    planes, own_rows, lanes = shape
    count, rows = planes * sizes[0], own_rows * sizes[1]
    half = count // 2

    def kernel(*refs):
        blocks = refs[: sizes[0]]
        outs = refs[sizes[0] : 8 + sizes[0]]
        cond, pairs = refs[8 + sizes[0] :]
        placed_whole(blocks, here(), sizes, shape, 2 * planes, planes, cond)

        def level(values, scale, step, refs):
            number, extent = len(values), values[0].shape[0]
            at_y = iota((extent, lanes), 0)
            at_z = iota((extent, lanes), 1)
            edges = (
                flag(at_y == 0) + flag(at_y == extent - 1)
                + flag(at_z < step) + flag(at_z >= lanes - step)
            )

            def x_mask(x):
                return 1.0 if x > 0 else 0.0

            def outside(x):
                return edges + float((x == 0) + (x == number - 1))

            found = coefficients(
                values, scale, step, x_mask, flag(at_y >= 1), flag(at_z >= step), outside
            )
            for x in range(number):
                for ref, value in zip(refs, found[x]):
                    ref[x, :extent, :] = value

        level([cond[x] for x in range(count)], 2.0, 1, outs[:4])
        blank = jnp.zeros((own_rows, lanes), jnp.float32)
        for x in range(count):
            for ref in outs[:4]:
                ref[x, rows:, :] = blank
        outs[0][count] = jnp.zeros((rows + own_rows, lanes), jnp.float32)
        for x in range(half):
            pairs[x] = swap_sum(cond[2 * x] + cond[2 * x + 1], 1, 1)
        coarse = [0.125 * row_pairs(pairs, x, rows) for x in range(half)]
        level(coarse, 4.0, 2, outs[4:])

    padded = (count, rows + own_rows, lanes)
    return call(
        kernel,
        [(count + 1,) + padded[1:]] + [padded] * 3 + [(half, rows // 2, lanes)] * 4,
        [(count, rows, lanes), (half, rows, lanes)],
        list(blocks),
    )


def prior_part(sizes, direction):
    planes, rows, lanes = direction.shape

    def kernel(direction, out_ref):
        x_mask, y_mask, z_mask, outside = frame_masks(here(), direction.shape, HALO, sizes)
        for x in range(HALO, planes - HALO):
            center = direction[x]
            out_ref[x - HALO] = prior_rows(
                center,
                direction[x - 1],
                direction[x + 1],
                shifted(center, 1, 0),
                shifted(center, -1, 0),
                x_mask(x),
                x_mask(x + 1),
                y_mask,
                z_mask,
                outside(x),
            )

    size = planes * rows * lanes
    return call(
        kernel, [(planes - 2 * HALO, rows, lanes)], [], [direction],
        cost=pl.CostEstimate(flops=20 * size, bytes_accessed=8 * size, transcendentals=0),
    )[0]


def middle(sizes, blocks, per, levels, fine, z, direction, curved, weight, earlier):
    planes, rows, lanes = z.shape
    own_x = planes - 2 * HALO
    coarse = (own_x // 2, (rows - 2 * HALO) // 2, lanes // 2)
    first_time = earlier is None
    extra = [] if first_time else list(earlier)
    inputs = list(blocks) + list(levels) + list(fine) + [z, direction, curved, weight] + extra

    def kernel(*refs):
        at = 0

        def take(number):
            nonlocal at
            at += number
            return refs[at - number : at]

        place = here()
        blocks = take(sizes[0])
        levels = take(8)
        fx, fy, fz, rd = take(4)
        z, direction, curved, weight = take(4)
        old = take(len(extra))
        b1, second = take(2)
        if first_time:
            (kept,) = take(1)
        else:
            combined, curved_out, norm_ref = take(3)
        source, whole_mid, pairs, mid, pair_rows, *room = refs[at:]
        frame_rows = iota((rows, lanes), 0)
        own_rows = (frame_rows >= HALO) & (frame_rows < rows - HALO)
        if first_time:
            placed_whole(blocks, place, sizes, coarse, per, 0, source)
        else:
            placed_overlapping(blocks, place, sizes, coarse, per, room[0], source)
        correction = coarse_correction(
            place, coarse, source, whole_mid, pairs, levels[:4], levels[4:]
        )
        zero = jnp.zeros((rows, lanes), jnp.float32)
        forms = zero
        squares = zero
        if first_time:
            for x in range(own_x):
                d = direction[x + HALO]
                forms = forms + d * curved[x]
                squares = squares + d * d
        else:
            tile = summed_tiles(blocks, sizes, per, per - 1)
            norm = total(jnp.where(iota(tile.shape, 0) >= 4, tile, 0.0))
            ratio = norm / old[2][0:1, 0:1]
            for x in range(own_x):
                d = direction[x + HALO] + ratio * old[1][x + HALO]
                image = curved[x] + ratio * old[3][x]
                combined[x] = d
                curved_out[x] = image
                forms = forms + d * image
            norm_ref[...] = jnp.broadcast_to(norm, (8, 128))
        for x in range(1, planes - 1):
            mid[x] = rd[x] * z[x] + correction[x // 2]
        rights = {}
        for x in range(2, planes - 2):
            off = off_diagonal(mid[x], mid[x - 1], mid[x + 1], fx[x], fx[x + 1], fy[x], fz[x])
            change = KEPT * mid[x] + rd[x] * (z[x] + off)
            if first_time:
                kept[x] = change
            else:
                change = change + ratio * old[0][x]
            right = weight[x] * change
            second[x] = right
            rights[x] = right
            if HALO <= x < planes - HALO:
                forms = forms + right * change
        for x in (0, 1, planes - 2, planes - 1):
            second[x] = zero
            if first_time:
                kept[x] = zero
        iterate = {x: rd[x] * rights[x] for x in range(HALO - 1, planes - HALO + 1)}
        fine_restricted_by_rows(rights, iterate, fx, fy, fz, b1, pair_rows, HALO, own_x)
        tile = fold(jnp.where(own_rows, forms, 0.0))
        if first_time:
            tile = halved(tile, fold(jnp.where(own_rows, squares, 0.0)))
        b1[coarse[0]] = tile

    frame = (planes, rows, lanes)
    own = (own_x, rows, lanes)
    margin = (coarse[0] * sizes[0] + 2, coarse[1] * (sizes[1] + 2), coarse[2])
    return call(
        kernel,
        [(coarse[0] + 1,) + coarse[1:], frame] + ([frame] if first_time else [own, own, (8, 128)]),
        coarse_scratch(coarse, sizes)
        + [frame, pairs_room(frame)]
        + ([] if first_time else [margin]),
        inputs,
    )


def image_planes(levels, fine, sizes, blocks, per, second, curved, cond, faces, scratch):
    fx, fy, fz, rd = fine
    hux, huy, huz, nbu = faces
    source, whole_mid, pairs, mid = scratch
    place = here()
    planes, rows, lanes = second.shape
    own = ((planes - 2 * HALO) // 2, (rows - 2 * HALO) // 2, lanes // 2)
    placed_whole(blocks, place, sizes, own, per, 0, source)
    correction = coarse_correction(
        place, own, source, whole_mid, pairs, levels[:4], levels[4:]
    )
    for x in range(2, planes - 2):
        mid[x] = rd[x] * second[x] + correction[x // 2]
    adjoint = {}
    for x in range(3, planes - 3):
        off = off_diagonal(mid[x], mid[x - 1], mid[x + 1], fx[x], fx[x + 1], fy[x], fz[x])
        adjoint[x] = KEPT * mid[x] + rd[x] * (second[x] + off)
    out = {}
    along_x = {
        x: hux[x] * (adjoint[x] - adjoint[x - 1]) for x in range(HALO, planes - HALO + 1)
    }
    for x in range(HALO, planes - HALO):
        p = adjoint[x]
        along_y = huy[x] * (p - shifted(p, 1, 0))
        along_z = huz[x] * (p - shifted(p, 1, 1))
        value = along_x[x] + along_x[x + 1] + nbu[x] * p
        value = value + (along_y + shifted(along_y, -1, 0))
        value = value + (along_z + shifted(along_z, -1, 1))
        out[x] = cond[x] * value + curved[x - HALO]
    return out


def own_restricted(direction, cond, faces, fine, squares, out_ref):
    fx, fy, fz, rd = fine
    hux, huy, huz, nbu = faces
    first, last = min(direction), max(direction)
    own_x = last - first + 1
    rows, lanes = direction[first].shape
    q = {x: cond[x] * direction[x] for x in direction}
    along_x = {first: hux[first] * q[first], last + 1: hux[last + 1] * q[last]}
    for x in range(first + 1, last + 1):
        along_x[x] = hux[x] * (q[x] + q[x - 1])
    z = {first - 1: -along_x[first], last + 1: along_x[last + 1]}
    for x in direction:
        mid = q[x]
        along_y = huy[x] * (mid + shifted(mid, 1, 0))
        along_z = huz[x] * (mid + shifted(mid, 1, 1))
        value = along_x[x] - along_x[x + 1] + nbu[x] * mid
        value = value + (along_y - shifted(along_y, -1, 0))
        z[x] = value + (along_z - shifted(along_z, -1, 1))
    iterate = {x: rd[x] * z[x] for x in z}
    planes = [fx[first - 1] * iterate[first - 1]]
    for x in range(first - 1, last + 2):
        off = off_diagonal(
            iterate[x], iterate.get(x - 1), iterate.get(x + 1),
            fx[x], fx[x + 1], fy[x], fz[x],
        )
        planes.append(KEPT * z[x] + off)
    planes[0] = fx[first - 1] * iterate[first - 1]
    planes.append(fx[last + 2] * iterate[last + 1])
    margin = HALO - 2
    block_rows = (rows - 2 * HALO) // 2
    target = iota((2 * block_rows, rows), 0)
    home = jnp.where(target < block_rows, target + 1, jnp.where(target == block_rows, 0, -9))
    home = jnp.where(target == block_rows + 1, block_rows + 1, home)
    here_row = iota((2 * block_rows, rows), 1)
    pick = flag((here_row >= margin + 2 * home) & (here_row < margin + 2 * home + 2))
    frame_rows = iota((rows, lanes), 0)
    inside = (frame_rows >= margin) & (frame_rows < rows - margin)
    halves = [
        pick_rows(pick, jnp.where(inside, planes[x] + planes[x + 1], 0.0))
        for x in range(0, len(planes), 2)
    ]
    packed = pick_lanes(jnp.concatenate(halves, axis=0), z_pairs(lanes))
    tops, borders = [], []
    for x in range(len(halves)):
        at = 2 * block_rows * x
        tops.append(packed[at : at + block_rows])
        borders.append(packed[at + block_rows : at + 2 * block_rows])
    number = own_x // 2
    for x in range(number):
        out_ref[x] = tops[x + 1]
    out_ref[number] = tops[0]
    out_ref[number + 1] = tops[-1]
    pairs = borders[1]
    for x in range(1, number):
        pairs = pairs + shifted(borders[x + 1], 2 * x, 0)
    out_ref[number + 2] = pairs
    tile = fold(squares)
    tile = tile + shifted(tile, 4, 0)
    corners = borders[0] + shifted(borders[-1], 2, 0)
    out_ref[number + 3] = jnp.where(iota(tile.shape, 0) >= 4, tile, corners)


def end_first(sizes, blocks, per, levels, fine, second, curved, cond, faces, source):
    planes, rows, lanes = second.shape
    own_x, own_y = planes - 2 * HALO, rows - 2 * HALO
    coarse = own_x // 2
    scratch_shapes = coarse_scratch((coarse, own_y // 2, lanes // 2), sizes)
    inputs = (
        list(blocks) + list(levels) + list(fine)
        + [second, curved, cond] + list(faces) + [source]
    )

    def kernel(*refs):
        n = sizes[0]
        blocks = refs[:n]
        levels = refs[n : 8 + n]
        fine = refs[8 + n : 12 + n]
        second, curved, cond = refs[12 + n : 15 + n]
        faces = refs[15 + n : 19 + n]
        source = refs[19 + n]
        first_ref, last_ref, own_ref, b1, norm_ref, step_ref = refs[20 + n : 26 + n]
        *scratch, hold = refs[26 + n :]
        image = image_planes(
            levels, fine, sizes, blocks, per, second, curved, cond, faces, scratch
        )
        tile = summed_tiles(blocks, sizes, per, coarse)
        lower = iota(tile.shape, 1) < tile.shape[1] // 2
        form = total(jnp.where(lower, tile, 0.0))
        norm = total(jnp.where(lower, 0.0, tile))
        step = norm / form
        norm_ref[...] = jnp.broadcast_to(norm, (8, 128))
        step_ref[...] = jnp.broadcast_to(step, (8, 128))
        frame_rows = iota((rows, lanes), 0)
        own_rows = (frame_rows >= HALO) & (frame_rows < rows - HALO)
        squares = jnp.zeros((rows, lanes), jnp.float32)
        remaining = {}
        for x in range(HALO, planes - HALO):
            value = jnp.where(own_rows, source[x] - step * image[x], 0.0)
            hold[x - HALO] = value
            remaining[x] = value
            squares = squares + value * value
        own_restricted(remaining, cond, faces, fine, squares, b1)
        for x in range(own_x):
            value = hold[x, HALO : HALO + own_y, :]
            own_ref[x] = value
            if x < HALO:
                first_ref[x] = value
            if x >= own_x - HALO:
                last_ref[x - own_x + HALO] = value

    strip = (HALO, own_y, lanes)
    return call(
        kernel,
        [strip, strip, (own_x, own_y, lanes), (coarse + 4, own_y // 2, lanes // 2)]
        + [(8, 128), (8, 128)],
        scratch_shapes + [(planes, rows, lanes), (own_x, rows, lanes)],
        inputs,
    )


def end_second(
    sizes, blocks, per, levels, fine, second, curved, cond, faces,
    source, remaining, combined, norm, step
):
    planes, rows, lanes = second.shape
    own_x, own_y = planes - 2 * HALO, rows - 2 * HALO
    coarse = own_x // 2
    scratch_shapes = coarse_scratch((coarse, own_y // 2, lanes // 2), sizes)
    inputs = (
        list(blocks) + list(levels) + list(fine)
        + [second, curved, cond] + list(faces) + [source, remaining, combined, norm, step]
    )

    def kernel(*refs):
        n = sizes[0]
        blocks = refs[:n]
        levels = refs[n : 8 + n]
        fine = refs[8 + n : 12 + n]
        second, curved, cond = refs[12 + n : 15 + n]
        faces = refs[15 + n : 19 + n]
        source, remaining, combined, norm, step = refs[19 + n : 24 + n]
        step_out, residual_out = refs[24 + n : 26 + n]
        *scratch, hold, hold_step = refs[26 + n :]
        image = image_planes(
            levels, fine, sizes, blocks, per, second, curved, cond, faces, scratch
        )
        form = total(summed_tiles(blocks, sizes, per, coarse))
        now = norm[0:1, 0:1] / form
        before = step[0:1, 0:1]
        for x in range(HALO, planes - HALO):
            hold[x - HALO] = now * image[x]
            hold_step[x - HALO] = before * source[x] + now * combined[x - HALO]
        for x in range(own_x):
            residual_out[x] = remaining[x] - hold[x, HALO : HALO + own_y, :]
            step_out[x] = hold_step[x, HALO : HALO + own_y, :]

    own = (own_x, own_y, lanes)
    hold = (own_x, rows, lanes)
    return call(
        kernel,
        [own, own],
        scratch_shapes + [(planes, rows, lanes), hold, hold],
        inputs,
    )


def edge_rows(own_x):
    starts, at = [], 0
    for x in range(own_x + 2 * HALO):
        starts.append(at)
        at += reach(HALO, own_x, x)
    return starts, -(-at // 8) * 8


def pack_edges(own, low, high):
    own_x, own_y, lanes = own.shape
    planes = own_x + 2 * HALO
    starts, rows = edge_rows(own_x)

    def kernel(own, low, high, first_ref, last_ref):
        for x in range(planes):
            near = reach(HALO, own_x, x)
            if near == 0:
                continue
            if x < HALO:
                ref, at = low, x
            elif x < HALO + own_x:
                ref, at = own, x - HALO
            else:
                ref, at = high, x - HALO - own_x
            row = starts[x]
            first_ref[row : row + near, :] = ref[at, :near, :]
            last_ref[row : row + near, :] = ref[at, own_y - near :, :]

    return call(kernel, [(rows, lanes)] * 2, [], [own, low, high])


def begin(own, low, high, before, after, cond, faces):
    own_x, own_y, lanes = own.shape
    planes, rows = own_x + 2 * HALO, own_y + 2 * HALO
    frame = (planes, rows, lanes)
    starts, _ = edge_rows(own_x)

    def kernel(
        own, low, high, before, after, cond, hux, huy, huz, nbu, direction, z_out
    ):
        for x in range(planes):
            if x < HALO:
                value = low[x]
            elif x < HALO + own_x:
                value = own[x - HALO]
            else:
                value = high[x - HALO - own_x]
            near = reach(HALO, own_x, x)
            if near < HALO:
                direction[x] = jnp.zeros((rows, lanes), jnp.float32)
            direction[x, HALO : HALO + own_y, :] = value
            if near:
                row = starts[x]
                direction[x, HALO - near : HALO, :] = before[row : row + near, :]
                end = HALO + own_y
                direction[x, end : end + near, :] = after[row : row + near, :]
        z = sensitivity_planes(
            lambda x: cond[x] * direction[x], hux, huy, huz, nbu, 1, planes - 1
        )
        zero = jnp.zeros((rows, lanes), jnp.float32)
        z_out[0] = zero
        z_out[planes - 1] = zero
        for x in z:
            z_out[x] = z[x]

    size = planes * rows * lanes
    return call(
        kernel,
        [frame, frame],
        [],
        [own, low, high, before, after, cond] + list(faces),
        cost=pl.CostEstimate(flops=20 * size, bytes_accessed=28 * size, transcendentals=0),
    )


def on_device(log_conductivity, state, gradient, prior_sample, sensor_cells, noise_precision):
    sizes = (lax.axis_size("gx"), lax.axis_size("gy"))
    cells_x, cells_y, cells_z = log_conductivity.shape
    coarse = (cells_x // 2, cells_y // 2, cells_z // 2)
    per = coarse[0] + 1

    weight = scattered(
        sizes, log_conductivity.shape, sensor_cells[None], noise_precision[None]
    )
    fields = (prior_sample, gradient, log_conductivity, state, weight)
    own_cond, even_edge, odd_edge, even_rows, odd_rows = prepare(fields)
    x_edges = exchange(even_edge, odd_edge, "gx")
    y_edges = exchange(even_rows, odd_rows, "gy")
    corners = exchange(*pack_corners(fields, *x_edges), "gy")
    (cond, hux, huy, huz, nbu, fx, fy, fz, rd, weight, source, z, b1) = setup(
        sizes, fields, x_edges, y_edges, corners, own_cond
    )
    faces = (hux, huy, huz, nbu)
    fine = (fx, fy, fz, rd)

    blocks = gathered(b1)
    curved = prior_part(sizes, source)
    levels = coarse_setup(sizes, blocks, coarse)
    b1, second, kept = middle(
        sizes, blocks, 2 * coarse[0], levels, fine, z, source, curved, weight, None
    )
    first, last, remaining, b1, norm, step = end_first(
        sizes, gathered(b1), per, levels, fine, second, curved, cond, faces, source
    )
    row = gathered_row(b1)
    low = rotate(last, "gx", 1)
    high = rotate(first, "gx", -1)
    first, last = pack_edges(remaining, low, high)
    row, first, last = lax.optimization_barrier((row, first, last))
    blocks = gathered_rows(row)
    before = rotate(last, "gy", 1)
    after = rotate(first, "gy", -1)
    direction, z = begin(remaining, low, high, before, after, cond, faces)
    b1, second, combined, curved, norm = middle(
        sizes, blocks, per + 3, levels, fine, z, direction, prior_part(sizes, direction), weight,
        (kept, source, norm, curved),
    )
    return tuple(
        end_second(
            sizes, gathered(b1), per, levels, fine, second, curved, cond,
            faces, source, remaining, combined, norm, step,
        )
    )


def solution(mesh):
    field = P(("ens", "gx"), "gy", None)
    sensors = P(("ens", "gx", "gy"))

    return jax.shard_map(
        on_device,
        mesh=mesh,
        in_specs=(field, field, field, field, sensors, sensors),
        out_specs=(field, field),
        check_vma=False,
    )
```
